32 devices in a mesh: chain: 8 (over y, x, core), lane: 4 (over z).
Axes of the slice: x: 2, y: 2, z: 4, core: 2. Of those that a mesh axis runs over, the one named last changes fastest.
Arguments:
- fiedler: float32 [16, 96, 128, 128], P(None, 'chain', 'lane'), may hold values from -6 to 6
- side_labels: int32 [96, 128, 128], P('chain', 'lane'), may hold values from 0 to 1, as said below
Outputs:
- squared_image: float32 [16, 120, 128, 128], P(None, 'chain', 'lane')
- gram_blocks: float32 [2, 16, 16], replicated
The draws below stay inside these ranges and needn't reach their ends.
Inputs may be any that keep to these rules, and one draw needn't show every extreme that they name: `side_labels`: along every line of the first dimension (fixed second and third index) the vertices of side 0 form one run of planes [a, b) with 18 <= a <= 30 and 66 <= b <= 78; all other vertices are of side 1.
All inputs are finite; a program needn't handle non-finite values.
Results may differ from the reference program's by a relative error of at most 0.0001.
Values sent between devices are 32-bit elements; how exact they have to be, the bound alone decides.
A program may use at most 128 MiB of HBM per device.

```python
import jax
import jax.numpy as jnp
from jax import lax

K = 16
NZ = 128
MARGIN = 6
NX = 96
NY = 128
BAND = 60


def draw_side_labels(key, part):
    key_low = jax.random.fold_in(key, 11)
    key_high = jax.random.fold_in(key, 23)
    shift_low = jax.random.randint(key_low, (NY, NZ), -MARGIN, MARGIN + 1)
    shift_high = jax.random.randint(key_high, (NY, NZ), -MARGIN, MARGIN + 1)
    planes = jnp.arange(NX, dtype=jnp.int32)[:, None, None]
    lower_edge = NX // 4 + shift_low
    upper_edge = 3 * NX // 4 + shift_high
    inside = (planes >= lower_edge[None]) & (planes < upper_edge[None])
    return jnp.where(inside, 0, 1).astype(jnp.int32)


def block_levels(key, extent, split, smallest, largest):
    def one(dim, blocks):
        draws = jax.random.uniform(jax.random.fold_in(jax.random.fold_in(key, 6), dim), (blocks,), jnp.float32, smallest / len(split), largest / len(split))
        return jnp.repeat(jnp.exp(draws), extent[dim] // blocks).reshape((-1,) + (1,) * (len(extent) - dim - 1))

    factor_of = one(*split[0])
    for cut in split[1:]:
        factor_of = factor_of * one(*cut)
    return factor_of


def bell_draw(stream_key, extent, spread, reach, split=(), held_as=jnp.bfloat16):
    array = spread * jax.random.normal(stream_key, extent, jnp.float32)
    if split:
        array = array * block_levels(stream_key, extent, split, -0.22, 0.18)
    return jnp.clip(array, -reach, reach).astype(held_as)


def setup_inputs(seed: int = 0) -> dict:
    key_of = jax.random.split(jax.random.key(seed), 3)
    fiedler = bell_draw(key_of[0], (K, NX, NY, NZ), 1.0, 6.0, ((1, 8), (2, 4)), jnp.float32)
    side_labels = draw_side_labels(jax.random.fold_in(key_of[2], 71), 0)
    return dict(fiedler=fiedler, side_labels=side_labels)


def neighbour_sum(field):
    padded = jnp.pad(field, ((0, 0), (1, 1), (0, 0), (0, 0)))
    total = padded[:, :-2] + padded[:, 2:]
    total = total + jnp.roll(field, 1, 2) + jnp.roll(field, -1, 2)
    total = total + jnp.roll(field, 1, 3) + jnp.roll(field, -1, 3)
    return total


def reference(fiedler, side_labels):
    images = []
    grams = []
    for half_idx in range(2):
        start_plane = NX // 4 - MARGIN + half_idx * (NX // 2)
        rolled = jnp.roll(fiedler, -start_plane, axis=1)[:, :BAND]
        labels_band = jnp.roll(side_labels, -start_plane, axis=0)[:BAND]
        keep = labels_band == half_idx
        member = keep.astype(jnp.float32)[None]
        moved = jnp.where(keep[None], rolled, jnp.float32(0.0))
        degree = neighbour_sum(member)
        once_applied = member * (degree * moved - neighbour_sum(moved)) / 6.0
        twice_applied = member * (degree * once_applied - neighbour_sum(once_applied)) / 6.0
        gram = jnp.einsum("kpyz,lpyz->kl", once_applied, once_applied, precision=lax.Precision.HIGHEST)
        images.append(twice_applied)
        grams.append(gram / (BAND * NY * NZ))
    joined = jnp.concatenate(images, axis=1)
    return jnp.roll(joined, BAND // 2, axis=1), jnp.stack(grams)
```

```python
import functools

import jax
import jax.numpy as jnp
from jax import lax
from jax.experimental import pallas as pl
from jax.experimental.pallas import tpu as pltpu
from jax.sharding import PartitionSpec as P

REACH = 2
MESH = pl.DeviceIdType.MESH


def two_sided(field):
    return (
        pltpu.roll(field, 1, 0) + pltpu.roll(field, field.shape[0] - 1, 0)
        + pltpu.roll(field, 1, 1) + pltpu.roll(field, field.shape[1] - 1, 1)
    )


class Plan:
    def __init__(self, chain, lanes, vectors, planes, lines, width):
        self.chain, self.lanes, self.vectors, self.planes, self.lines, self.width = (
            chain, lanes, vectors, planes, lines, width)
        self.half = chain // 2
        self.band = planes + planes // 4
        self.grow = self.band - planes
        self.margin = self.grow * self.half // 2
        self.window = self.band + 2 * REACH
        spots = [self.spot(w, max_of=max) for w in range(self.half)]
        self.most = max(max(below, above) for _, below, above in spots)
        assert self.most <= planes and 8 * vectors == width
        assert spots[0][1] == spots[-1][2] > 0 and spots[0][2] == spots[-1][1] == 0
        self.pad = 1 + max(max(0, -slot) for slot, _, _ in spots)
        tail = 1 + max(max(0, slot + planes - self.window) for slot, _, _ in spots)
        self.frames = self.pad + self.window + tail

    def spot(self, w, max_of=jnp.maximum):
        first, last = (w == 0), (w == self.half - 1)
        if not isinstance(w, int):
            first, last = first.astype(jnp.int32), last.astype(jnp.int32)
        slot = self.margin + REACH - self.grow * w
        below = max_of(0, slot - REACH * first)
        above = max_of(0, self.window - REACH * last - slot - self.planes)
        return slot, below, above

    def place(self, c):
        relative = lax.rem(c + (self.chain - self.chain // 4), self.chain)
        side = lax.div(relative, self.half)
        within = relative - side * self.half
        return side, within


def kernel(plan, scale_of, fiedler, labels, image, gram, field, moved, once, mark, label, count, counted, spare, acc,
           packed, got, local_sem, lab_s, lab_r, own_s, own_r, plane_s, plane_r, edge_s, edge_r, cnt_s, cnt_r,
           gram_s, gram_r):
    chain, lanes, vectors, planes, lines, width = (
        plan.chain, plan.lanes, plan.vectors, plan.planes, plan.lines, plan.width)
    window, pad, most = plan.window, plan.pad, plan.most
    c, l = lax.axis_index("chain"), lax.axis_index("lane")
    up_c, down_c = lax.rem(c + 1, chain), lax.rem(c + chain - 1, chain)
    up_l, down_l = lax.rem(l + 1, lanes), lax.rem(l + lanes - 1, lanes)
    side, within = plan.place(c)
    slot, below, above = plan.spot(within)
    up_side, up_within = plan.place(up_c)
    down_side, down_within = plan.place(down_c)
    up_slot, up_count, _ = plan.spot(up_within)
    down_slot, _, down_count = plan.spot(down_within)
    tall = lines + 8
    lo, hi = slice(0, REACH), slice(lines - REACH, lines)
    nxt, prv = slice(lines, lines + REACH), slice(tall - REACH, tall)

    def remote(src, dst, send, recv, device):
        return pltpu.make_async_remote_copy(
            src_ref=src, dst_ref=dst, send_sem=send, recv_sem=recv, device_id=device, device_id_type=MESH)

    base = pad + slot
    load_field = pltpu.make_async_copy(fiedler, field.at[:, pl.ds(base, planes), 0:lines], local_sem.at[0])
    load_label = pltpu.make_async_copy(labels, label.at[:, 0:lines], local_sem.at[1])
    load_label.start()
    load_field.start()

    barrier = pltpu.get_barrier_semaphore()
    for dc in range(chain):
        for dl in range(lanes):
            if dc or dl:
                pl.semaphore_signal(barrier, inc=1, device_id=(lax.rem(c + dc, chain), lax.rem(l + dl, lanes)),
                                    device_id_type=MESH)
    pl.semaphore_wait(barrier, chain * lanes - 1)

    lab_copies = [
        remote(labels.at[:, lo], label.at[:, nxt], lab_s.at[0], lab_r.at[0], (c, down_l)),
        remote(labels.at[:, hi], label.at[:, prv], lab_s.at[1], lab_r.at[1], (c, up_l)),
    ]
    own = pl.ds(base, planes)
    own_copies = [
        remote(fiedler.at[:, :, lo], field.at[:, own, nxt], own_s.at[0], own_r.at[0], (c, down_l)),
        remote(fiedler.at[:, :, hi], field.at[:, own, prv], own_s.at[1], own_r.at[1], (c, up_l)),
    ]

    def plane_copies(way, j):
        if way == 0:
            source, at, to = planes - j, pad + up_slot - j, up_c
        else:
            source, at, to = j - 1, pad + down_slot + planes - 1 + j, down_c
        return [
            remote(fiedler.at[:, source], field.at[:, at, 0:lines], plane_s.at[way, j - 1], plane_r.at[way, j - 1],
                   (to, l)),
            remote(fiedler.at[:, source, lo], field.at[:, at, nxt], edge_s.at[way, j - 1, 0],
                   edge_r.at[way, j - 1, 0], (to, down_l)),
            remote(fiedler.at[:, source, hi], field.at[:, at, prv], edge_s.at[way, j - 1, 1],
                   edge_r.at[way, j - 1, 1], (to, up_l)),
        ]

    for copy in lab_copies:
        copy.start()
    for j in range(1, most + 1):
        for way, total in ((0, up_count), (1, down_count)):
            @pl.when(j <= total)
            def _():
                for copy in plane_copies(way, j):
                    copy.start()
        if j == 1:
            for copy in own_copies:
                copy.start()

    load_label.wait()
    for copy in lab_copies:
        copy.wait_recv()

    def count_copy(way):
        return remote(count.at[way], counted.at[way], cnt_s.at[way], cnt_r.at[way], ((up_c, down_c)[way], l))

    totals = [jnp.zeros((tall, width), jnp.float32) for _ in range(2)]
    for p in range(planes):
        here = label[p]
        totals[0] += jnp.where((here == up_side) & (p >= planes - up_count), 1.0, 0.0)
        totals[1] += jnp.where((here == down_side) & (p < down_count), 1.0, 0.0)
    for way, total in ((0, up_count), (1, down_count)):
        count[way] = totals[way]

        @pl.when(total > 0)
        def _():
            count_copy(way).start()

    acc[...] = jnp.zeros(acc.shape, jnp.float32)
    for p in range(planes):
        mark[base + p] = jnp.where(label[p] == side, 1.0, 0.0)

    is_end = (within == 0) | (within == plan.half - 1)
    lower = within < plan.half // 2
    d = jnp.where(lower, -1, 1)
    near_way, far_way = jnp.where(lower, 0, 1), jnp.where(lower, 1, 0)
    near, far = jnp.where(lower, below, above), jnp.where(lower, above, below)
    near_edge = jnp.where(lower, base, base + planes - 1)
    far_edge = jnp.where(lower, base + planes - 1, base)

    @pl.when(is_end)
    def _():
        at = near_edge + d * (near + 1)
        mark[at] = jnp.zeros((tall, width), jnp.float32)

        def clear(k, _):
            moved[k, at] = jnp.zeros((tall, width), jnp.float32)
            once[k, at] = jnp.zeros((tall, width), jnp.float32)
            return 0

        lax.fori_loop(0, vectors, clear, 0)

    def take(at):
        keep = mark[at] > 0.5

        def one(k, _):
            moved[k, at] = jnp.where(keep, field[k, at], 0.0)
            return 0

        lax.fori_loop(0, vectors, one, 0, unroll=4)

    def weights(before, here, after):
        scale = here * jnp.float32(1.0 / 6.0)
        return scale * (before + after + two_sided(here)), scale

    def apply_once(s):
        degree, scale = weights(mark[s - 1], mark[s], mark[s + 1])

        def one(k, _):
            here = moved[k, s]
            once[k, s] = degree * here - scale * (moved[k, s - 1] + moved[k, s + 1] + two_sided(here))
            return 0

        lax.fori_loop(0, vectors, one, 0, unroll=4)

    def apply_twice(s):
        degree, scale = weights(mark[s - 1], mark[s], mark[s + 1])

        def one(k, _):
            here = once[k, s]
            value = degree * here - scale * (once[k, s - 1] + once[k, s + 1] + two_sided(here))
            image[k, s - pad - REACH] = value[0:lines]
            return 0

        @pl.when((s >= pad + REACH) & (s < pad + window - REACH))
        def _():
            lax.fori_loop(0, vectors, one, 0, unroll=4)

    def add_gram(read, which):
        block = jnp.concatenate(
            [read(g).reshape(8 * vectors, width) for g in range(lines // 8)], axis=1)
        high = block.astype(jnp.bfloat16)
        low = (block - high.astype(jnp.float32)).astype(jnp.bfloat16)
        dot = functools.partial(
            lax.dot_general, dimension_numbers=(((1,), (1,)), ((), ())), preferred_element_type=jnp.float32)
        acc[which, 0] += dot(high, high)
        acc[which, 1] += dot(high, low)

    def gram_of(s):
        add_gram(lambda g: once[:, s, 8 * g : 8 * g + 8, :], 0)

    load_field.wait()
    for copy in own_copies:
        copy.wait_recv()

    def take_own(p, _):
        take(base + p)
        return 0

    lax.fori_loop(0, planes, take_own, 0)

    def inner_once(s, _):
        apply_once(s)

        @pl.when((s >= pad + REACH) & (s < pad + window - REACH))
        def _():
            gram_of(s)
        return 0

    def inner_twice(s, _):
        apply_twice(s)
        return 0

    first, last = jnp.maximum(base, pad), jnp.minimum(base + planes, pad + window)
    lax.fori_loop(first + 1, last - 1, inner_once, 0)
    lax.fori_loop(first + 2, last - 2, inner_twice, 0)

    for way, total in ((0, below), (1, above)):
        @pl.when(total > 0)
        def _():
            count_copy(way).wait_recv()

    def wait_plane(way, j, at):
        remote(fiedler.at[:, 0], field.at[:, at, 0:lines], plane_s.at[way, j - 1], plane_r.at[way, j - 1],
               (c, l)).wait_recv()
        remote(fiedler.at[:, 0, lo], field.at[:, at, nxt], edge_s.at[way, j - 1, 0], edge_r.at[way, j - 1, 0],
               (c, l)).wait_recv()
        remote(fiedler.at[:, 0, hi], field.at[:, at, prv], edge_s.at[way, j - 1, 1], edge_r.at[way, j - 1, 1],
               (c, l)).wait_recv()

    def near_step(j, _):
        at = near_edge + d * j

        @pl.when(j <= near)
        def _():
            wait_plane(near_way, j, at)
            mark[at] = jnp.where(counted[near_way] >= j.astype(jnp.float32) - 0.5, 1.0, 0.0)
            take(at)

        @pl.when(j <= near + 1)
        def _():
            apply_once(at - d)

        @pl.when((at - d >= pad + REACH) & (at - d < pad + window - REACH) & (jnp.logical_not(is_end) | (j == 1)))
        def _():
            gram_of(at - d)

        apply_twice(at - 2 * d)
        return 0

    def far_step(j, _):
        at = far_edge - d * j
        wait_plane(far_way, j, at)
        mark[at] = jnp.where(counted[far_way] >= (far - j + 1).astype(jnp.float32) - 0.5, 1.0, 0.0)
        take(at)
        apply_once(at + d)

        @pl.when((at + d >= pad + REACH) & (at + d < pad + window - REACH))
        def _():
            gram_of(at + d)

        apply_twice(at + 2 * d)
        return 0

    def other_step(j, _):
        at = near_edge - d * (j - 1)
        toward, away = 1.0 - mark[at + d], jnp.where(j < near, 1.0 - mark[at - d], 0.0)
        here = 1.0 - mark[at]
        degree, scale = weights(toward, here, away)

        def one(k, _):
            def part(keep, index):
                return jnp.where(keep > 0.5, field[k, index], 0.0)

            value = part(here, at)
            value = degree * value - scale * (part(toward, at + d) + part(away, at - d) + two_sided(value))
            spare[k] = value[0:lines]
            return 0

        lax.fori_loop(0, vectors, one, 0, unroll=4)
        add_gram(lambda g: spare[:, 8 * g : 8 * g + 8, :], 1)
        return 0

    early = jnp.where(is_end, jnp.minimum(near, 1), near) + 1
    lax.fori_loop(1, early, near_step, 0)

    @pl.when(is_end)
    def _():
        lax.fori_loop(1, near + 1, other_step, 0)

    lax.fori_loop(1, far + 1, far_step, 0)

    me = c * lanes + l
    lane_of = functools.partial(lax.broadcasted_iota, jnp.int32)
    for which in range(2):
        total = acc[which, 0] + (acc[which, 1] + acc[which, 1].T)
        shape = (vectors, 8, width)
        diagonal = lane_of(shape, 1) == lax.rem(lane_of(shape, 2), 8)
        rows = jnp.sum(jnp.where(diagonal, total.reshape(shape), 0.0), axis=1)
        ones = jnp.where(lax.div(lane_of((width, width), 0), 8) == lax.div(lane_of((width, width), 1), 8), 1.0, 0.0)
        rows = jnp.dot(rows, ones, precision=lax.Precision.HIGHEST, preferred_element_type=jnp.float32)
        half = (8, width)
        pick = lane_of(half, 0) == lax.rem(lane_of(half, 1), 8)
        for h in range(vectors // 8):
            row = jnp.sum(jnp.where(pick, rows[8 * h : 8 * h + 8], 0.0), axis=0, keepdims=True)
            for place in range(2):
                @pl.when((side if which == 0 else 1 - side) == place)
                def _():
                    packed[place * (vectors // 8) + h : place * (vectors // 8) + h + 1, :] = row
    count_rows = 2 * (vectors // 8)
    body = packed.at[0:count_rows]
    for dc in range(chain):
        for dl in range(lanes):
            if dc or dl:
                remote(body, got.at[me, 0:count_rows], gram_s.at[0], gram_r.at[0],
                       (lax.rem(c + dc, chain), lax.rem(l + dl, lanes))).start()
    got[me, 0:count_rows] = packed[0:count_rows]

    lax.fori_loop(early, near, near_step, 0)

    everyone = got.at[0 : chain * lanes - 1, 0:count_rows]
    remote(everyone, everyone, gram_s.at[0], gram_r.at[0], (c, l)).wait_recv()

    def sum_one(i, total):
        return total + got[i, 0:count_rows]

    total = lax.fori_loop(1, chain * lanes, sum_one, got[0, 0:count_rows], unroll=True)
    tall_shape = (vectors, width)
    inside = lax.div(lane_of(tall_shape, 1), 8) == lane_of(tall_shape, 0)
    choose = jnp.where(
        lax.rem(lane_of((width, width), 0), 8) == lax.rem(lane_of((width, width), 1), 8), 1.0, 0.0)
    for place in range(2):
        result = jnp.zeros(tall_shape, jnp.float32)
        for h in range(vectors // 8):
            i = place * (vectors // 8) + h
            spread = jnp.where(inside, jnp.broadcast_to(total[i : i + 1], tall_shape), 0.0)
            spread = jnp.dot(spread, choose, precision=lax.Precision.HIGHEST, preferred_element_type=jnp.float32)
            result = jnp.where(lax.div(lane_of(tall_shape, 1), 8) == h, spread, result)
        gram[place] = result[:, 0:vectors] / scale_of

    lax.fori_loop(jnp.maximum(early, near), near + 1 + 2 * is_end.astype(jnp.int32), near_step, 0)

    remote(everyone, everyone, gram_s.at[0], gram_r.at[0], (c, l)).wait_send()
    for copy in lab_copies + own_copies:
        copy.wait_send()
    for way, total in ((0, up_count), (1, down_count)):
        @pl.when(total > 0)
        def _():
            count_copy(way).wait_send()
        for j in range(1, most + 1):
            @pl.when(j <= total)
            def _():
                for copy in plane_copies(way, j):
                    copy.wait_send()


def per_device(fiedler, side_labels):
    chain, lanes = lax.axis_size("chain"), lax.axis_size("lane")
    vectors, planes, lines, width = fiedler.shape
    plan = Plan(chain, lanes, vectors, planes, lines, width)
    slots = plan.band * plan.half * lines * lanes * width
    tall, frames, most = lines + 8, plan.frames, plan.most
    f32, dma = jnp.float32, pltpu.SemaphoreType.DMA
    anywhere, vmem = pl.BlockSpec(memory_space=pl.ANY), pl.BlockSpec(memory_space=pltpu.VMEM)
    return pl.pallas_call(
        functools.partial(kernel, plan, float(slots)),
        in_specs=[anywhere, anywhere],
        out_specs=[vmem, vmem],
        out_shape=[
            jax.ShapeDtypeStruct((vectors, plan.band, lines, width), f32),
            jax.ShapeDtypeStruct((2, vectors, vectors), f32),
        ],
        scratch_shapes=[
            pltpu.VMEM((vectors, frames, tall, width), f32),
            pltpu.VMEM((vectors, frames, tall, width), f32),
            pltpu.VMEM((vectors, frames, tall, width), f32),
            pltpu.VMEM((frames, tall, width), f32),
            pltpu.VMEM((planes, tall, width), jnp.int32),
            pltpu.VMEM((2, tall, width), f32),
            pltpu.VMEM((2, tall, width), f32),
            pltpu.VMEM((vectors, lines, width), f32),
            pltpu.VMEM((2, 2, 8 * vectors, 8 * vectors), f32),
            pltpu.VMEM((8, width), f32),
            pltpu.VMEM((chain * lanes, 8, width), f32),
            dma((2,)), dma((2,)), dma((2,)), dma((2,)), dma((2,)),
            dma((2, most)), dma((2, most)), dma((2, most, 2)), dma((2, most, 2)),
            dma((2,)), dma((2,)), dma((1,)), dma((1,)),
        ],
        compiler_params=pltpu.CompilerParams(
            collective_id=0, has_side_effects=True, vmem_limit_bytes=56 * 1024 * 1024),
        name="laplace",
    )(fiedler, side_labels)


def solution(mesh):
    return jax.shard_map(
        per_device,
        mesh=mesh,
        in_specs=(P(None, "chain", "lane", None), P("chain", "lane", None)),
        out_specs=(P(None, "chain", "lane", None), P()),
        check_vma=False,
    )
```

```python
import functools

import jax
import jax.numpy as jnp
from jax import lax
from jax.experimental import pallas as pl
from jax.experimental.pallas import tpu as pltpu
from jax.sharding import PartitionSpec as P

REACH = 2
MESH = pl.DeviceIdType.MESH


def two_sided(field):
    return (
        pltpu.roll(field, 1, 0) + pltpu.roll(field, field.shape[0] - 1, 0)
        + pltpu.roll(field, 1, 1) + pltpu.roll(field, field.shape[1] - 1, 1)
    )


class Plan:
    def __init__(self, chain, lanes, vectors, planes, lines, width):
        self.chain, self.lanes, self.vectors, self.planes, self.lines, self.width = (
            chain, lanes, vectors, planes, lines, width)
        self.half = chain // 2
        self.band = planes + planes // 4
        self.grow = self.band - planes
        self.margin = self.grow * self.half // 2
        self.window = self.band + 2 * REACH
        spots = [self.spot(w, max_of=max) for w in range(self.half)]
        self.most = max(max(below, above) for _, below, above in spots)
        assert self.most <= planes and 8 * vectors == width
        assert spots[0][1] == spots[-1][2] > 0 and spots[0][2] == spots[-1][1] == 0
        self.pad = 1 + max(max(0, -slot) for slot, _, _ in spots)
        tail = 1 + max(max(0, slot + planes - self.window) for slot, _, _ in spots)
        self.frames = self.pad + self.window + tail

    def spot(self, w, max_of=jnp.maximum):
        first, last = (w == 0), (w == self.half - 1)
        if not isinstance(w, int):
            first, last = first.astype(jnp.int32), last.astype(jnp.int32)
        slot = self.margin + REACH - self.grow * w
        below = max_of(0, slot - REACH * first)
        above = max_of(0, self.window - REACH * last - slot - self.planes)
        return slot, below, above

    def place(self, c):
        relative = lax.rem(c + (self.chain - self.chain // 4), self.chain)
        side = lax.div(relative, self.half)
        within = relative - side * self.half
        return side, within


def kernel(plan, scale_of, fiedler, labels, image, gram, field, moved, once, mark, label, count, counted, spare, acc,
           packed, got, local_sem, lab_s, lab_r, own_s, own_r, plane_s, plane_r, edge_s, edge_r, cnt_s, cnt_r,
           gram_s, gram_r):
    chain, lanes, vectors, planes, lines, width = (
        plan.chain, plan.lanes, plan.vectors, plan.planes, plan.lines, plan.width)
    window, pad, most = plan.window, plan.pad, plan.most
    c, l = lax.axis_index("chain"), lax.axis_index("lane")
    up_c, down_c = lax.rem(c + 1, chain), lax.rem(c + chain - 1, chain)
    up_l, down_l = lax.rem(l + 1, lanes), lax.rem(l + lanes - 1, lanes)
    side, within = plan.place(c)
    slot, below, above = plan.spot(within)
    up_side, up_within = plan.place(up_c)
    down_side, down_within = plan.place(down_c)
    up_slot, up_count, _ = plan.spot(up_within)
    down_slot, _, down_count = plan.spot(down_within)
    tall = lines + 8
    lo, hi = slice(0, REACH), slice(lines - REACH, lines)
    nxt, prv = slice(lines, lines + REACH), slice(tall - REACH, tall)

    def remote(src, dst, send, recv, device):
        return pltpu.make_async_remote_copy(
            src_ref=src, dst_ref=dst, send_sem=send, recv_sem=recv, device_id=device, device_id_type=MESH)

    base = pad + slot
    load_field = pltpu.make_async_copy(fiedler, field.at[:, pl.ds(base, planes), 0:lines], local_sem.at[0])
    load_label = pltpu.make_async_copy(labels, label.at[:, 0:lines], local_sem.at[1])
    load_label.start()
    load_field.start()

    barrier = pltpu.get_barrier_semaphore()
    for dc in range(chain):
        for dl in range(lanes):
            if dc or dl:
                pl.semaphore_signal(barrier, inc=1, device_id=(lax.rem(c + dc, chain), lax.rem(l + dl, lanes)),
                                    device_id_type=MESH)
    pl.semaphore_wait(barrier, chain * lanes - 1)

    lab_copies = [
        remote(labels.at[:, lo], label.at[:, nxt], lab_s.at[0], lab_r.at[0], (c, down_l)),
        remote(labels.at[:, hi], label.at[:, prv], lab_s.at[1], lab_r.at[1], (c, up_l)),
    ]
    own = pl.ds(base, planes)
    own_copies = [
        remote(fiedler.at[:, :, lo], field.at[:, own, nxt], own_s.at[0], own_r.at[0], (c, down_l)),
        remote(fiedler.at[:, :, hi], field.at[:, own, prv], own_s.at[1], own_r.at[1], (c, up_l)),
    ]

    def plane_copies(way, j):
        if way == 0:
            source, at, to = planes - j, pad + up_slot - j, up_c
        else:
            source, at, to = j - 1, pad + down_slot + planes - 1 + j, down_c
        return [
            remote(fiedler.at[:, source], field.at[:, at, 0:lines], plane_s.at[way, j - 1], plane_r.at[way, j - 1],
                   (to, l)),
            remote(fiedler.at[:, source, lo], field.at[:, at, nxt], edge_s.at[way, j - 1, 0],
                   edge_r.at[way, j - 1, 0], (to, down_l)),
            remote(fiedler.at[:, source, hi], field.at[:, at, prv], edge_s.at[way, j - 1, 1],
                   edge_r.at[way, j - 1, 1], (to, up_l)),
        ]

    for copy in lab_copies:
        copy.start()
    for j in range(1, most + 1):
        for way, total in ((0, up_count), (1, down_count)):
            @pl.when(j <= total)
            def _():
                for copy in plane_copies(way, j):
                    copy.start()
        if j == 1:
            for copy in own_copies:
                copy.start()

    load_label.wait()
    for copy in lab_copies:
        copy.wait_recv()

    def count_copy(way):
        return remote(count.at[way], counted.at[way], cnt_s.at[way], cnt_r.at[way], ((up_c, down_c)[way], l))

    totals = [jnp.zeros((tall, width), jnp.float32) for _ in range(2)]
    for p in range(planes):
        here = label[p]
        totals[0] += jnp.where((here == up_side) & (p >= planes - up_count), 1.0, 0.0)
        totals[1] += jnp.where((here == down_side) & (p < down_count), 1.0, 0.0)
    for way, total in ((0, up_count), (1, down_count)):
        count[way] = totals[way]

        @pl.when(total > 0)
        def _():
            count_copy(way).start()

    acc[...] = jnp.zeros(acc.shape, jnp.float32)
    for p in range(planes):
        mark[base + p] = jnp.where(label[p] == side, 1.0, 0.0)

    is_end = (within == 0) | (within == plan.half - 1)
    lower = within < plan.half // 2
    d = jnp.where(lower, -1, 1)
    near_way, far_way = jnp.where(lower, 0, 1), jnp.where(lower, 1, 0)
    near, far = jnp.where(lower, below, above), jnp.where(lower, above, below)
    near_edge = jnp.where(lower, base, base + planes - 1)
    far_edge = jnp.where(lower, base + planes - 1, base)

    @pl.when(is_end)
    def _():
        at = near_edge + d * (near + 1)
        mark[at] = jnp.zeros((tall, width), jnp.float32)

        def clear(k, _):
            moved[k, at] = jnp.zeros((tall, width), jnp.float32)
            once[k, at] = jnp.zeros((tall, width), jnp.float32)
            return 0

        lax.fori_loop(0, vectors, clear, 0)

    def take(at):
        keep = mark[at] > 0.5

        def one(k, _):
            moved[k, at] = jnp.where(keep, field[k, at], 0.0)
            return 0

        lax.fori_loop(0, vectors, one, 0, unroll=vectors)

    def weights(before, here, after):
        scale = here * jnp.float32(1.0 / 6.0)
        return scale * (before + after + two_sided(here)), scale

    def apply_once(s):
        degree, scale = weights(mark[s - 1], mark[s], mark[s + 1])

        def one(k, _):
            here = moved[k, s]
            once[k, s] = degree * here - scale * (moved[k, s - 1] + moved[k, s + 1] + two_sided(here))
            return 0

        lax.fori_loop(0, vectors, one, 0, unroll=vectors)

    def apply_twice(s):
        degree, scale = weights(mark[s - 1], mark[s], mark[s + 1])

        def one(k, _):
            here = once[k, s]
            value = degree * here - scale * (once[k, s - 1] + once[k, s + 1] + two_sided(here))
            image[k, s - pad - REACH] = value[0:lines]
            return 0

        @pl.when((s >= pad + REACH) & (s < pad + window - REACH))
        def _():
            lax.fori_loop(0, vectors, one, 0, unroll=vectors)

    def add_gram(read, which):
        block = jnp.concatenate(
            [read(g).reshape(8 * vectors, width) for g in range(lines // 8)], axis=1)
        high = block.astype(jnp.bfloat16)
        low = (block - high.astype(jnp.float32)).astype(jnp.bfloat16)
        dot = functools.partial(
            lax.dot_general, dimension_numbers=(((1,), (1,)), ((), ())), preferred_element_type=jnp.float32)
        acc[which, 0] += dot(high, high)
        acc[which, 1] += dot(high, low)

    def gram_of(s):
        add_gram(lambda g: once[:, s, 8 * g : 8 * g + 8, :], 0)

    load_field.wait()
    for copy in own_copies:
        copy.wait_recv()

    def take_own(p, _):
        take(base + p)
        return 0

    lax.fori_loop(0, planes, take_own, 0)

    def inner_once(s, _):
        apply_once(s)

        @pl.when((s >= pad + REACH) & (s < pad + window - REACH))
        def _():
            gram_of(s)
        return 0

    def inner_twice(s, _):
        apply_twice(s)
        return 0

    first, last = jnp.maximum(base, pad), jnp.minimum(base + planes, pad + window)
    lax.fori_loop(first + 1, last - 1, inner_once, 0)
    lax.fori_loop(first + 2, last - 2, inner_twice, 0)

    for way, total in ((0, below), (1, above)):
        @pl.when(total > 0)
        def _():
            count_copy(way).wait_recv()

    def wait_plane(way, j, at):
        remote(fiedler.at[:, 0], field.at[:, at, 0:lines], plane_s.at[way, j - 1], plane_r.at[way, j - 1],
               (c, l)).wait_recv()
        remote(fiedler.at[:, 0, lo], field.at[:, at, nxt], edge_s.at[way, j - 1, 0], edge_r.at[way, j - 1, 0],
               (c, l)).wait_recv()
        remote(fiedler.at[:, 0, hi], field.at[:, at, prv], edge_s.at[way, j - 1, 1], edge_r.at[way, j - 1, 1],
               (c, l)).wait_recv()

    def near_step(j, _):
        at = near_edge + d * j

        @pl.when(j <= near)
        def _():
            wait_plane(near_way, j, at)
            mark[at] = jnp.where(counted[near_way] >= j.astype(jnp.float32) - 0.5, 1.0, 0.0)
            take(at)

        @pl.when(j <= near + 1)
        def _():
            apply_once(at - d)

        @pl.when((at - d >= pad + REACH) & (at - d < pad + window - REACH) & (jnp.logical_not(is_end) | (j == 1)))
        def _():
            gram_of(at - d)

        apply_twice(at - 2 * d)
        return 0

    def far_step(j, _):
        at = far_edge - d * j
        wait_plane(far_way, j, at)
        mark[at] = jnp.where(counted[far_way] >= (far - j + 1).astype(jnp.float32) - 0.5, 1.0, 0.0)
        take(at)
        apply_once(at + d)

        @pl.when((at + d >= pad + REACH) & (at + d < pad + window - REACH))
        def _():
            gram_of(at + d)

        apply_twice(at + 2 * d)
        return 0

    def other_step(j, _):
        at = near_edge - d * (j - 1)
        toward, away = 1.0 - mark[at + d], jnp.where(j < near, 1.0 - mark[at - d], 0.0)
        here = 1.0 - mark[at]
        degree, scale = weights(toward, here, away)

        def one(k, _):
            def part(keep, index):
                return jnp.where(keep > 0.5, field[k, index], 0.0)

            value = part(here, at)
            value = degree * value - scale * (part(toward, at + d) + part(away, at - d) + two_sided(value))
            spare[k] = value[0:lines]
            return 0

        lax.fori_loop(0, vectors, one, 0, unroll=vectors)
        add_gram(lambda g: spare[:, 8 * g : 8 * g + 8, :], 1)
        return 0

    early = jnp.where(is_end, jnp.minimum(near, 1), near) + 1
    lax.fori_loop(1, early, near_step, 0)

    @pl.when(is_end)
    def _():
        lax.fori_loop(1, near + 1, other_step, 0)

    lax.fori_loop(1, far + 1, far_step, 0)

    me = c * lanes + l
    lane_of = functools.partial(lax.broadcasted_iota, jnp.int32)
    for which in range(2):
        total = acc[which, 0] + (acc[which, 1] + acc[which, 1].T)
        shape = (vectors, 8, width)
        diagonal = lane_of(shape, 1) == lax.rem(lane_of(shape, 2), 8)
        rows = jnp.sum(jnp.where(diagonal, total.reshape(shape), 0.0), axis=1)
        ones = jnp.where(lax.div(lane_of((width, width), 0), 8) == lax.div(lane_of((width, width), 1), 8), 1.0, 0.0)
        rows = jnp.dot(rows, ones, precision=lax.Precision.HIGHEST, preferred_element_type=jnp.float32)
        half = (8, width)
        pick = lane_of(half, 0) == lax.rem(lane_of(half, 1), 8)
        for h in range(vectors // 8):
            row = jnp.sum(jnp.where(pick, rows[8 * h : 8 * h + 8], 0.0), axis=0, keepdims=True)
            for place in range(2):
                @pl.when((side if which == 0 else 1 - side) == place)
                def _():
                    packed[place * (vectors // 8) + h : place * (vectors // 8) + h + 1, :] = row
    count_rows = 2 * (vectors // 8)
    body = packed.at[0:count_rows]
    for dc in range(chain):
        for dl in range(lanes):
            if dc or dl:
                remote(body, got.at[me, 0:count_rows], gram_s.at[0], gram_r.at[0],
                       (lax.rem(c + dc, chain), lax.rem(l + dl, lanes))).start()
    got[me, 0:count_rows] = packed[0:count_rows]

    lax.fori_loop(early, near, near_step, 0)

    everyone = got.at[0 : chain * lanes - 1, 0:count_rows]
    remote(everyone, everyone, gram_s.at[0], gram_r.at[0], (c, l)).wait_recv()

    def sum_one(i, total):
        return total + got[i, 0:count_rows]

    total = lax.fori_loop(1, chain * lanes, sum_one, got[0, 0:count_rows], unroll=True)
    tall_shape = (vectors, width)
    inside = lax.div(lane_of(tall_shape, 1), 8) == lane_of(tall_shape, 0)
    choose = jnp.where(
        lax.rem(lane_of((width, width), 0), 8) == lax.rem(lane_of((width, width), 1), 8), 1.0, 0.0)
    for place in range(2):
        result = jnp.zeros(tall_shape, jnp.float32)
        for h in range(vectors // 8):
            i = place * (vectors // 8) + h
            spread = jnp.where(inside, jnp.broadcast_to(total[i : i + 1], tall_shape), 0.0)
            spread = jnp.dot(spread, choose, precision=lax.Precision.HIGHEST, preferred_element_type=jnp.float32)
            result = jnp.where(lax.div(lane_of(tall_shape, 1), 8) == h, spread, result)
        gram[place] = result[:, 0:vectors] / scale_of

    lax.fori_loop(jnp.maximum(early, near), near + 1 + 2 * is_end.astype(jnp.int32), near_step, 0)

    remote(everyone, everyone, gram_s.at[0], gram_r.at[0], (c, l)).wait_send()
    for copy in lab_copies + own_copies:
        copy.wait_send()
    for way, total in ((0, up_count), (1, down_count)):
        @pl.when(total > 0)
        def _():
            count_copy(way).wait_send()
        for j in range(1, most + 1):
            @pl.when(j <= total)
            def _():
                for copy in plane_copies(way, j):
                    copy.wait_send()


def per_device(fiedler, side_labels):
    chain, lanes = lax.axis_size("chain"), lax.axis_size("lane")
    vectors, planes, lines, width = fiedler.shape
    plan = Plan(chain, lanes, vectors, planes, lines, width)
    slots = plan.band * plan.half * lines * lanes * width
    tall, frames, most = lines + 8, plan.frames, plan.most
    f32, dma = jnp.float32, pltpu.SemaphoreType.DMA
    anywhere, vmem = pl.BlockSpec(memory_space=pl.ANY), pl.BlockSpec(memory_space=pltpu.VMEM)
    return pl.pallas_call(
        functools.partial(kernel, plan, float(slots)),
        in_specs=[anywhere, anywhere],
        out_specs=[vmem, vmem],
        out_shape=[
            pltpu.VMEM((vectors, plan.band, lines, width), f32),
            jax.ShapeDtypeStruct((2, vectors, vectors), f32),
        ],
        scratch_shapes=[
            pltpu.VMEM((vectors, frames, tall, width), f32),
            pltpu.VMEM((vectors, frames, tall, width), f32),
            pltpu.VMEM((vectors, frames, tall, width), f32),
            pltpu.VMEM((frames, tall, width), f32),
            pltpu.VMEM((planes, tall, width), jnp.int32),
            pltpu.VMEM((2, tall, width), f32),
            pltpu.VMEM((2, tall, width), f32),
            pltpu.VMEM((vectors, lines, width), f32),
            pltpu.VMEM((2, 2, 8 * vectors, 8 * vectors), f32),
            pltpu.VMEM((8, width), f32),
            pltpu.VMEM((chain * lanes, 8, width), f32),
            dma((2,)), dma((2,)), dma((2,)), dma((2,)), dma((2,)),
            dma((2, most)), dma((2, most)), dma((2, most, 2)), dma((2, most, 2)),
            dma((2,)), dma((2,)), dma((1,)), dma((1,)),
        ],
        compiler_params=pltpu.CompilerParams(
            collective_id=0, has_side_effects=True, vmem_limit_bytes=56 * 1024 * 1024),
        name="laplace",
    )(fiedler, side_labels)


def solution(mesh):
    return jax.shard_map(
        per_device,
        mesh=mesh,
        in_specs=(P(None, "chain", "lane", None), P("chain", "lane", None)),
        out_specs=(P(None, "chain", "lane", None), P()),
        check_vma=False,
    )
```

```python
import functools

import jax
import jax.numpy as jnp
from jax import lax
from jax.experimental import pallas as pl
from jax.experimental.pallas import tpu as pltpu
from jax.sharding import PartitionSpec as P

REACH = 2
EARLY_PLANES = 3
CHUNKS = 3
MESH = pl.DeviceIdType.MESH


def two_sided(field):
    return (
        pltpu.roll(field, 1, 0) + pltpu.roll(field, field.shape[0] - 1, 0)
        + pltpu.roll(field, 1, 1) + pltpu.roll(field, field.shape[1] - 1, 1)
    )


class Plan:
    def __init__(self, chain, lanes, vectors, planes, lines, width):
        self.chain, self.lanes, self.vectors, self.planes, self.lines, self.width = (
            chain, lanes, vectors, planes, lines, width)
        self.half = chain // 2
        self.band = planes + planes // 4
        self.grow = self.band - planes
        self.margin = self.grow * self.half // 2
        self.window = self.band + 2 * REACH
        spots = [self.spot(w, max_of=max) for w in range(self.half)]
        self.most = max(max(below, above) for _, below, above in spots)
        assert self.most <= planes and 8 * vectors == width
        assert spots[0][1] == spots[-1][2] > 0 and spots[0][2] == spots[-1][1] == 0
        self.end_near = spots[0][1]
        self.chunk = planes // CHUNKS
        assert self.chunk * CHUNKS == planes and self.chunk > 2
        self.pad = 1 + max(max(0, -slot) for slot, _, _ in spots)
        tail = 1 + max(max(0, slot + planes - self.window) for slot, _, _ in spots)
        self.frames = self.pad + self.window + tail

    def spot(self, w, max_of=jnp.maximum):
        first, last = (w == 0), (w == self.half - 1)
        if not isinstance(w, int):
            first, last = first.astype(jnp.int32), last.astype(jnp.int32)
        slot = self.margin + REACH - self.grow * w
        below = max_of(0, slot - REACH * first)
        above = max_of(0, self.window - REACH * last - slot - self.planes)
        return slot, below, above

    def place(self, c):
        relative = lax.rem(c + (self.chain - self.chain // 4), self.chain)
        side = lax.div(relative, self.half)
        within = relative - side * self.half
        return side, within


def kernel(plan, scale_of, fiedler, labels, image, gram, field, moved, once, mark, label, count, counted, spare, acc,
           packed, got, local_sem, lab_s, lab_r, own_s, own_r, plane_s, plane_r, edge_s, edge_r, pass_s, cnt_s, cnt_r,
           gram_s, gram_r):
    chain, lanes, vectors, planes, lines, width = (
        plan.chain, plan.lanes, plan.vectors, plan.planes, plan.lines, plan.width)
    window, pad, most = plan.window, plan.pad, plan.most
    c, l = lax.axis_index("chain"), lax.axis_index("lane")
    up_c, down_c = lax.rem(c + 1, chain), lax.rem(c + chain - 1, chain)
    up_l, down_l = lax.rem(l + 1, lanes), lax.rem(l + lanes - 1, lanes)
    side, within = plan.place(c)
    slot, below, above = plan.spot(within)
    up_side, up_within = plan.place(up_c)
    down_side, down_within = plan.place(down_c)
    up_slot, up_count, _ = plan.spot(up_within)
    down_slot, _, down_count = plan.spot(down_within)
    tall = lines + 8
    lo, hi = slice(0, REACH), slice(lines - REACH, lines)
    nxt, prv = slice(lines, lines + REACH), slice(tall - REACH, tall)

    def remote(src, dst, send, recv, device):
        return pltpu.make_async_remote_copy(
            src_ref=src, dst_ref=dst, send_sem=send, recv_sem=recv, device_id=device, device_id_type=MESH)

    base = pad + slot
    is_end = (within == 0) | (within == plan.half - 1)
    lower = within < plan.half // 2
    d = jnp.where(lower, -1, 1)
    near_way, far_way = jnp.where(lower, 0, 1), jnp.where(lower, 1, 0)
    near, far = jnp.where(lower, below, above), jnp.where(lower, above, below)
    near_edge = jnp.where(lower, base, base + planes - 1)
    far_edge = jnp.where(lower, base + planes - 1, base)

    load_field = pltpu.make_async_copy(fiedler, field.at[:, pl.ds(base, planes), 0:lines], local_sem.at[0])
    load_label = pltpu.make_async_copy(labels, label.at[:, 0:lines], local_sem.at[1])
    load_label.start()
    load_field.start()

    barrier = pltpu.get_barrier_semaphore()
    for dc in range(chain):
        for dl in range(lanes):
            if dc or dl:
                pl.semaphore_signal(barrier, inc=1, device_id=(lax.rem(c + dc, chain), lax.rem(l + dl, lanes)),
                                    device_id_type=MESH)
    pl.semaphore_wait(barrier, chain * lanes - 1)

    lab_copies = [
        remote(labels.at[:, lo], label.at[:, nxt], lab_s.at[0], lab_r.at[0], (c, down_l)),
        remote(labels.at[:, hi], label.at[:, prv], lab_s.at[1], lab_r.at[1], (c, up_l)),
    ]
    chunk = plan.chunk

    def own_copies(i):
        start = jnp.where(lower, i * chunk, planes - (i + 1) * chunk)
        source, at = pl.ds(start, chunk), pl.ds(base + start, chunk)
        return [
            remote(fiedler.at[:, source, lo], field.at[:, at, nxt], own_s.at[i, 0], own_r.at[i, 0], (c, down_l)),
            remote(fiedler.at[:, source, hi], field.at[:, at, prv], own_s.at[i, 1], own_r.at[i, 1], (c, up_l)),
        ]

    sends = ((0, up_count, up_side != side), (1, down_count, down_side != side))

    def spot_of(way, j):
        if way == 0:
            return planes - j, pad + up_slot - j, up_c
        return j - 1, pad + down_slot + planes - 1 + j, down_c

    def plane_copy(way, j):
        source, at, to = spot_of(way, j)
        return remote(
            fiedler.at[:, source], field.at[:, at, 0:lines], plane_s.at[way, j - 1], plane_r.at[way, j - 1], (to, l))

    def corner_copies(way, j):
        source, at, to = spot_of(way, j)
        return [
            remote(fiedler.at[:, source, lo], field.at[:, at, nxt], edge_s.at[way, j - 1, 0],
                   edge_r.at[way, j - 1, 0], (to, down_l)),
            remote(fiedler.at[:, source, hi], field.at[:, at, prv], edge_s.at[way, j - 1, 1],
                   edge_r.at[way, j - 1, 1], (to, up_l)),
        ]

    def passed_on(j, total):
        return (j >= 2) & (j <= total - 2)

    def pass_copies(j):
        at = near_edge + d * j
        return [
            remote(field.at[:, at, lo], field.at[:, at, nxt], pass_s.at[j - 1, 0], edge_r.at[near_way, j - 1, 0],
                   (c, down_l)),
            remote(field.at[:, at, hi], field.at[:, at, prv], pass_s.at[j - 1, 1], edge_r.at[near_way, j - 1, 1],
                   (c, up_l)),
        ]

    def send_plane(j, late):
        for way, total, across in sends:
            @pl.when((j <= total) & (across if late else (jnp.logical_not(across) | (j <= EARLY_PLANES))))
            def _():
                plane_copy(way, j).start()

                @pl.when(jnp.logical_not(across & passed_on(j, total)))
                def _():
                    for copy in corner_copies(way, j):
                        copy.start()

    for copy in lab_copies:
        copy.start()
    send_plane(1, False)
    for i in range(CHUNKS):
        for copy in own_copies(i):
            copy.start()
    for j in range(2, most + 1):
        send_plane(j, False)

    load_label.wait()
    for copy in lab_copies:
        copy.wait_recv()

    def count_copy(way):
        return remote(count.at[way], counted.at[way], cnt_s.at[way], cnt_r.at[way], ((up_c, down_c)[way], l))

    totals = [jnp.zeros((tall, width), jnp.float32) for _ in range(2)]
    for p in range(planes):
        here = label[p]
        totals[0] += jnp.where((here == up_side) & (p >= planes - up_count), 1.0, 0.0)
        totals[1] += jnp.where((here == down_side) & (p < down_count), 1.0, 0.0)
    for way, total in ((0, up_count), (1, down_count)):
        count[way] = totals[way]

        @pl.when(total > 0)
        def _():
            count_copy(way).start()

    acc[...] = jnp.zeros(acc.shape, jnp.float32)
    for p in range(planes):
        mark[base + p] = jnp.where(label[p] == side, 1.0, 0.0)

    @pl.when(is_end)
    def _():
        at = near_edge + d * (near + 1)
        mark[at] = jnp.zeros((tall, width), jnp.float32)

        def clear(k, _):
            moved[k, at] = jnp.zeros((tall, width), jnp.float32)
            once[k, at] = jnp.zeros((tall, width), jnp.float32)
            return 0

        lax.fori_loop(0, vectors, clear, 0)

    def take(at):
        keep = mark[at] > 0.5

        def one(k, _):
            moved[k, at] = jnp.where(keep, field[k, at], 0.0)
            return 0

        lax.fori_loop(0, vectors, one, 0, unroll=vectors)

    def weights(before, here, after):
        scale = here * jnp.float32(1.0 / 6.0)
        return scale * (before + after + two_sided(here)), scale

    def apply_once(s):
        degree, scale = weights(mark[s - 1], mark[s], mark[s + 1])

        def one(k, _):
            here = moved[k, s]
            once[k, s] = degree * here - scale * (moved[k, s - 1] + moved[k, s + 1] + two_sided(here))
            return 0

        lax.fori_loop(0, vectors, one, 0, unroll=vectors)

    def apply_twice(s):
        degree, scale = weights(mark[s - 1], mark[s], mark[s + 1])

        def one(k, _):
            here = once[k, s]
            value = degree * here - scale * (once[k, s - 1] + once[k, s + 1] + two_sided(here))
            image[k, s - pad - REACH] = value[0:lines]
            return 0

        @pl.when(in_band(s))
        def _():
            lax.fori_loop(0, vectors, one, 0, unroll=vectors)

    def add_gram(read, which):
        block = jnp.concatenate(
            [read(g).reshape(8 * vectors, width) for g in range(lines // 8)], axis=1)
        high = block.astype(jnp.bfloat16)
        low = (block - high.astype(jnp.float32)).astype(jnp.bfloat16)
        dot = functools.partial(
            lax.dot_general, dimension_numbers=(((1,), (1,)), ((), ())), preferred_element_type=jnp.float32)
        acc[which, 0] += dot(high, high)
        acc[which, 1] += dot(high, low)

    def gram_of(s):
        add_gram(lambda g: once[:, s, 8 * g : 8 * g + 8, :], 0)

    def in_band(s):
        return (s >= pad + REACH) & (s < pad + window - REACH)

    def wait_plane(way, j, at):
        remote(fiedler.at[:, 0], field.at[:, at, 0:lines], plane_s.at[way, j - 1], plane_r.at[way, j - 1],
               (c, l)).wait_recv()

    def wait_edges(way, j, at):
        remote(fiedler.at[:, 0, lo], field.at[:, at, nxt], edge_s.at[way, j - 1, 0], edge_r.at[way, j - 1, 0],
               (c, l)).wait_recv()
        remote(fiedler.at[:, 0, hi], field.at[:, at, prv], edge_s.at[way, j - 1, 1], edge_r.at[way, j - 1, 1],
               (c, l)).wait_recv()

    def near_use(j, _):
        at = near_edge + d * j

        @pl.when(j <= near)
        def _():
            wait_edges(near_way, j, at)
            mark[at] = jnp.where(counted[near_way] >= j.astype(jnp.float32) - 0.5, 1.0, 0.0)
            take(at)

        @pl.when(j <= near + 1)
        def _():
            apply_once(at - d)

        @pl.when(in_band(at - d) & (jnp.logical_not(is_end) | (j == 1)))
        def _():
            gram_of(at - d)

        apply_twice(at - 2 * d)
        return 0

    def near_step(j, _):
        goes_on = is_end & passed_on(j, near)

        @pl.when(j <= near)
        def _():
            wait_plane(near_way, j, near_edge + d * j)

        @pl.when(goes_on)
        def _():
            for copy in pass_copies(j):
                copy.start()

        begin = jnp.where(is_end & passed_on(j - 1, near), j - 1, j)
        lax.fori_loop(begin, jnp.where(goes_on, j, j + 1), near_use, 0)
        return 0

    def far_step(j, _):
        at = far_edge - d * j
        wait_plane(far_way, j, at)
        wait_edges(far_way, j, at)
        mark[at] = jnp.where(counted[far_way] >= (far - j + 1).astype(jnp.float32) - 0.5, 1.0, 0.0)
        take(at)
        apply_once(at + d)

        @pl.when(in_band(at + d))
        def _():
            gram_of(at + d)

        apply_twice(at + 2 * d)
        return 0

    def other_step(j, _):
        at = near_edge - d * (j - 1)
        toward, away = 1.0 - mark[at + d], jnp.where(j < near, 1.0 - mark[at - d], 0.0)
        here = 1.0 - mark[at]
        degree, scale = weights(toward, here, away)

        def one(k, _):
            def part(keep, index):
                return jnp.where(keep > 0.5, field[k, index], 0.0)

            value = part(here, at)
            value = degree * value - scale * (part(toward, at + d) + part(away, at - d) + two_sided(value))
            spare[k] = value[0:lines]
            return 0

        lax.fori_loop(0, vectors, one, 0, unroll=vectors)
        add_gram(lambda g: spare[:, 8 * g : 8 * g + 8, :], 1)
        return 0

    def take_own(m, _):
        take(near_edge - d * m)
        return 0

    def inner_once(m, _):
        s = near_edge - d * m

        @pl.when((s > pad) & (s < pad + window - 1))
        def _():
            apply_once(s)

        @pl.when(in_band(s))
        def _():
            gram_of(s)
        return 0

    def inner_twice(m, _):
        apply_twice(near_edge - d * m)
        return 0

    def end_gram():
        @pl.when(is_end)
        def _():
            lax.fori_loop(1, 2, near_step, 0)
            lax.fori_loop(1, near + 1, other_step, 0)

    load_field.wait()
    ready = min(CHUNKS - 1, plan.end_near // chunk)
    for i in range(CHUNKS):
        for copy in own_copies(i):
            copy.wait_recv()
        lax.fori_loop(i * chunk, (i + 1) * chunk, take_own, 0)
        lax.fori_loop(max(1, i * chunk - 1), (i + 1) * chunk - 1, inner_once, 0)
        if i == 0:
            for way, total in ((0, below), (1, above)):
                @pl.when(total > 0)
                def _():
                    count_copy(way).wait_recv()
        if i == ready:
            end_gram()

    @pl.when(jnp.logical_not(is_end))
    def _():
        lax.fori_loop(2, planes - 2, inner_twice, 0)
        lax.fori_loop(1, near + 1, near_step, 0)

    lax.fori_loop(1, far + 1, far_step, 0)

    me = c * lanes + l
    lane_of = functools.partial(lax.broadcasted_iota, jnp.int32)
    for which in range(2):
        total = acc[which, 0] + (acc[which, 1] + acc[which, 1].T)
        shape = (vectors, 8, width)
        diagonal = lane_of(shape, 1) == lax.rem(lane_of(shape, 2), 8)
        rows = jnp.sum(jnp.where(diagonal, total.reshape(shape), 0.0), axis=1)
        ones = jnp.where(lax.div(lane_of((width, width), 0), 8) == lax.div(lane_of((width, width), 1), 8), 1.0, 0.0)
        rows = jnp.dot(rows, ones, precision=lax.Precision.HIGHEST, preferred_element_type=jnp.float32)
        half = (8, width)
        pick = lane_of(half, 0) == lax.rem(lane_of(half, 1), 8)
        for h in range(vectors // 8):
            row = jnp.sum(jnp.where(pick, rows[8 * h : 8 * h + 8], 0.0), axis=0, keepdims=True)
            for place in range(2):
                @pl.when((side if which == 0 else 1 - side) == place)
                def _():
                    packed[place * (vectors // 8) + h : place * (vectors // 8) + h + 1, :] = row
    count_rows = 2 * (vectors // 8)
    body = packed.at[0:count_rows]
    for dc in range(chain):
        for dl in range(lanes):
            if dc or dl:
                remote(body, got.at[me, 0:count_rows], gram_s.at[0], gram_r.at[0],
                       (lax.rem(c + dc, chain), lax.rem(l + dl, lanes))).start()
    got[me, 0:count_rows] = packed[0:count_rows]

    for j in range(EARLY_PLANES + 1, most + 1):
        send_plane(j, True)

    @pl.when(is_end)
    def _():
        lax.fori_loop(2, planes - 2, inner_twice, 0)
        lax.fori_loop(2, near, near_step, 0)

    everyone = got.at[0 : chain * lanes - 1, 0:count_rows]
    remote(everyone, everyone, gram_s.at[0], gram_r.at[0], (c, l)).wait_recv()

    def sum_one(i, total):
        return total + got[i, 0:count_rows]

    total = lax.fori_loop(1, chain * lanes, sum_one, got[0, 0:count_rows], unroll=True)
    tall_shape = (vectors, width)
    inside = lax.div(lane_of(tall_shape, 1), 8) == lane_of(tall_shape, 0)
    choose = jnp.where(
        lax.rem(lane_of((width, width), 0), 8) == lax.rem(lane_of((width, width), 1), 8), 1.0, 0.0)
    for place in range(2):
        result = jnp.zeros(tall_shape, jnp.float32)
        for h in range(vectors // 8):
            i = place * (vectors // 8) + h
            spread = jnp.where(inside, jnp.broadcast_to(total[i : i + 1], tall_shape), 0.0)
            spread = jnp.dot(spread, choose, precision=lax.Precision.HIGHEST, preferred_element_type=jnp.float32)
            result = jnp.where(lax.div(lane_of(tall_shape, 1), 8) == h, spread, result)
        gram[place] = result[:, 0:vectors] / scale_of

    @pl.when(is_end)
    def _():
        lax.fori_loop(near, near + 3, near_step, 0)

    remote(everyone, everyone, gram_s.at[0], gram_r.at[0], (c, l)).wait_send()
    for i in range(CHUNKS):
        for copy in own_copies(i):
            copy.wait_send()
    for copy in lab_copies:
        copy.wait_send()
    for way, total, across in sends:
        @pl.when(total > 0)
        def _():
            count_copy(way).wait_send()
        for j in range(1, most + 1):
            @pl.when(j <= total)
            def _():
                plane_copy(way, j).wait_send()

                @pl.when(jnp.logical_not(across & passed_on(j, total)))
                def _():
                    for copy in corner_copies(way, j):
                        copy.wait_send()
    for j in range(1, most + 1):
        @pl.when(is_end & passed_on(j, near))
        def _():
            for copy in pass_copies(j):
                copy.wait_send()


def per_device(fiedler, side_labels):
    chain, lanes = lax.axis_size("chain"), lax.axis_size("lane")
    vectors, planes, lines, width = fiedler.shape
    plan = Plan(chain, lanes, vectors, planes, lines, width)
    slots = plan.band * plan.half * lines * lanes * width
    tall, frames, most = lines + 8, plan.frames, plan.most
    f32, dma = jnp.float32, pltpu.SemaphoreType.DMA
    anywhere, vmem = pl.BlockSpec(memory_space=pl.ANY), pl.BlockSpec(memory_space=pltpu.VMEM)
    return pl.pallas_call(
        functools.partial(kernel, plan, float(slots)),
        in_specs=[anywhere, anywhere],
        out_specs=[vmem, vmem],
        out_shape=[
            pltpu.VMEM((vectors, plan.band, lines, width), f32),
            jax.ShapeDtypeStruct((2, vectors, vectors), f32),
        ],
        scratch_shapes=[
            pltpu.VMEM((vectors, frames, tall, width), f32),
            pltpu.VMEM((vectors, frames, tall, width), f32),
            pltpu.VMEM((vectors, frames, tall, width), f32),
            pltpu.VMEM((frames, tall, width), f32),
            pltpu.VMEM((planes, tall, width), jnp.int32),
            pltpu.VMEM((2, tall, width), f32),
            pltpu.VMEM((2, tall, width), f32),
            pltpu.VMEM((vectors, lines, width), f32),
            pltpu.VMEM((2, 2, 8 * vectors, 8 * vectors), f32),
            pltpu.VMEM((8, width), f32),
            pltpu.VMEM((chain * lanes, 8, width), f32),
            dma((2,)), dma((2,)), dma((2,)), dma((CHUNKS, 2)), dma((CHUNKS, 2)),
            dma((2, most)), dma((2, most)), dma((2, most, 2)), dma((2, most, 2)), dma((most, 2)),
            dma((2,)), dma((2,)), dma((1,)), dma((1,)),
        ],
        compiler_params=pltpu.CompilerParams(
            collective_id=0, has_side_effects=True, vmem_limit_bytes=56 * 1024 * 1024),
        name="laplace",
    )(fiedler, side_labels)


def solution(mesh):
    return jax.shard_map(
        per_device,
        mesh=mesh,
        in_specs=(P(None, "chain", "lane", None), P("chain", "lane", None)),
        out_specs=(P(None, "chain", "lane", None), P()),
        check_vma=False,
    )
```

```python
import functools

import jax
import jax.numpy as jnp
from jax import lax
from jax.experimental import pallas as pl
from jax.experimental.pallas import tpu as pltpu
from jax.sharding import PartitionSpec as P

REACH = 2
EARLY_PLANES = 4
CHUNKS = 3
STORES = 4
MESH = pl.DeviceIdType.MESH


def two_sided(field):
    return (
        pltpu.roll(field, 1, 0) + pltpu.roll(field, field.shape[0] - 1, 0)
        + pltpu.roll(field, 1, 1) + pltpu.roll(field, field.shape[1] - 1, 1)
    )


class Plan:
    def __init__(self, chain, lanes, vectors, planes, lines, width):
        self.chain, self.lanes, self.vectors, self.planes, self.lines, self.width = (
            chain, lanes, vectors, planes, lines, width)
        self.half = chain // 2
        self.band = planes + planes // 4
        self.grow = self.band - planes
        self.margin = self.grow * self.half // 2
        self.window = self.band + 2 * REACH
        spots = [self.spot(w, max_of=max) for w in range(self.half)]
        self.most = max(max(below, above) for _, below, above in spots)
        assert self.most <= planes and 8 * vectors == width
        assert spots[0][1] == spots[-1][2] > 0 and spots[0][2] == spots[-1][1] == 0
        self.end_near = spots[0][1]
        self.chunk = planes // CHUNKS
        assert self.chunk * CHUNKS == planes and self.chunk > 2
        self.pad = 1 + max(max(0, -slot) for slot, _, _ in spots)
        tail = 1 + max(max(0, slot + planes - self.window) for slot, _, _ in spots)
        self.frames = self.pad + self.window + tail

    def spot(self, w, max_of=jnp.maximum):
        first, last = (w == 0), (w == self.half - 1)
        if not isinstance(w, int):
            first, last = first.astype(jnp.int32), last.astype(jnp.int32)
        slot = self.margin + REACH - self.grow * w
        below = max_of(0, slot - REACH * first)
        above = max_of(0, self.window - REACH * last - slot - self.planes)
        return slot, below, above

    def place(self, c):
        relative = lax.rem(c + (self.chain - self.chain // 4), self.chain)
        side = lax.div(relative, self.half)
        within = relative - side * self.half
        return side, within


def kernel(plan, scale_of, fiedler, labels, image, gram, field, moved, once, mark, label, count, counted, spare, acc,
           packed, got, local_sem, lab_s, lab_r, own_s, own_r, plane_s, plane_r, edge_s, edge_r, pass_s, cnt_s, cnt_r,
           gram_s, gram_r):
    chain, lanes, vectors, planes, lines, width = (
        plan.chain, plan.lanes, plan.vectors, plan.planes, plan.lines, plan.width)
    window, pad, most = plan.window, plan.pad, plan.most
    c, l = lax.axis_index("chain"), lax.axis_index("lane")
    up_c, down_c = lax.rem(c + 1, chain), lax.rem(c + chain - 1, chain)
    up_l, down_l = lax.rem(l + 1, lanes), lax.rem(l + lanes - 1, lanes)
    side, within = plan.place(c)
    slot, below, above = plan.spot(within)
    up_side, up_within = plan.place(up_c)
    down_side, down_within = plan.place(down_c)
    up_slot, up_count, _ = plan.spot(up_within)
    down_slot, _, down_count = plan.spot(down_within)
    tall = lines + 8
    lo, hi = slice(0, REACH), slice(lines - REACH, lines)
    nxt, prv = slice(lines, lines + REACH), slice(tall - REACH, tall)

    def remote(src, dst, send, recv, device):
        return pltpu.make_async_remote_copy(
            src_ref=src, dst_ref=dst, send_sem=send, recv_sem=recv, device_id=device, device_id_type=MESH)

    base = pad + slot
    is_end = (within == 0) | (within == plan.half - 1)
    lower = within < plan.half // 2
    d = jnp.where(lower, -1, 1)
    near_way, far_way = jnp.where(lower, 0, 1), jnp.where(lower, 1, 0)
    near, far = jnp.where(lower, below, above), jnp.where(lower, above, below)
    near_edge = jnp.where(lower, base, base + planes - 1)
    far_edge = jnp.where(lower, base + planes - 1, base)

    load_field = pltpu.make_async_copy(fiedler, field.at[:, pl.ds(base, planes), 0:lines], local_sem.at[0])
    load_label = pltpu.make_async_copy(labels, label.at[:, 0:lines], local_sem.at[1])
    load_label.start()
    load_field.start()

    barrier = pltpu.get_barrier_semaphore()
    for dc in range(chain):
        for dl in range(lanes):
            if dc or dl:
                pl.semaphore_signal(barrier, inc=1, device_id=(lax.rem(c + dc, chain), lax.rem(l + dl, lanes)),
                                    device_id_type=MESH)
    load_label.wait()
    totals = [jnp.zeros((lines, width), jnp.float32) for _ in range(2)]
    for p in range(planes):
        here = label[p, 0:lines]
        totals[0] += jnp.where((here == up_side) & (p >= planes - up_count), 1.0, 0.0)
        totals[1] += jnp.where((here == down_side) & (p < down_count), 1.0, 0.0)
    for way in range(2):
        count[way] = totals[way]
    pl.semaphore_wait(barrier, chain * lanes - 1)

    lab_copies = [
        remote(labels.at[:, lo], label.at[:, nxt], lab_s.at[0], lab_r.at[0], (c, down_l)),
        remote(labels.at[:, hi], label.at[:, prv], lab_s.at[1], lab_r.at[1], (c, up_l)),
    ]
    chunk = plan.chunk

    def own_copies(i):
        start = jnp.where(lower, i * chunk, planes - (i + 1) * chunk)
        source, at = pl.ds(start, chunk), pl.ds(base + start, chunk)
        return [
            remote(fiedler.at[:, source, lo], field.at[:, at, nxt], own_s.at[i, 0], own_r.at[i, 0], (c, down_l)),
            remote(fiedler.at[:, source, hi], field.at[:, at, prv], own_s.at[i, 1], own_r.at[i, 1], (c, up_l)),
        ]

    sends = ((0, up_count, up_side != side), (1, down_count, down_side != side))

    def spot_of(way, j):
        if way == 0:
            return planes - j, pad + up_slot - j, up_c
        return j - 1, pad + down_slot + planes - 1 + j, down_c

    def plane_copy(way, j):
        source, at, to = spot_of(way, j)
        return remote(
            fiedler.at[:, source], field.at[:, at, 0:lines], plane_s.at[way, j - 1], plane_r.at[way, j - 1], (to, l))

    def corner_copies(way, j):
        source, at, to = spot_of(way, j)
        return [
            remote(fiedler.at[:, source, lo], field.at[:, at, nxt], edge_s.at[way, j - 1, 0],
                   edge_r.at[way, j - 1, 0], (to, down_l)),
            remote(fiedler.at[:, source, hi], field.at[:, at, prv], edge_s.at[way, j - 1, 1],
                   edge_r.at[way, j - 1, 1], (to, up_l)),
        ]

    def passed_on(j, total):
        return (j >= 2) & (j <= total - 2)

    def pass_copies(j):
        at = near_edge + d * j
        return [
            remote(field.at[:, at, lo], field.at[:, at, nxt], pass_s.at[j - 1, 0], edge_r.at[near_way, j - 1, 0],
                   (c, down_l)),
            remote(field.at[:, at, hi], field.at[:, at, prv], pass_s.at[j - 1, 1], edge_r.at[near_way, j - 1, 1],
                   (c, up_l)),
        ]

    def send_plane(j, late):
        for way, total, across in sends:
            @pl.when((j <= total) & (across if late else (jnp.logical_not(across) | (j <= EARLY_PLANES))))
            def _():
                plane_copy(way, j).start()

                @pl.when(jnp.logical_not(across & passed_on(j, total)))
                def _():
                    for copy in corner_copies(way, j):
                        copy.start()

    def count_copies(way):
        to = (up_c, down_c)[way]
        return [
            remote(count.at[way], counted.at[way, 0:lines], cnt_s.at[way, 0], cnt_r.at[way, 0], (to, l)),
            remote(count.at[way, lo], counted.at[way, nxt], cnt_s.at[way, 1], cnt_r.at[way, 1], (to, down_l)),
            remote(count.at[way, hi], counted.at[way, prv], cnt_s.at[way, 2], cnt_r.at[way, 2], (to, up_l)),
        ]

    for way, total, _ in sends:
        @pl.when(total > 0)
        def _():
            for copy in count_copies(way):
                copy.start()
    for copy in lab_copies:
        copy.start()
    send_plane(1, False)
    for i in range(CHUNKS):
        for copy in own_copies(i):
            copy.start()
    for j in range(2, most + 1):
        send_plane(j, False)

    for copy in lab_copies:
        copy.wait_recv()
    acc[...] = jnp.zeros(acc.shape, jnp.float32)
    for p in range(planes):
        mark[base + p] = jnp.where(label[p] == side, 1.0, 0.0)

    @pl.when(is_end)
    def _():
        at = near_edge + d * (near + 1)
        mark[at] = jnp.zeros((tall, width), jnp.float32)

        def clear(k, _):
            moved[k, at] = jnp.zeros((tall, width), jnp.float32)
            once[k, at] = jnp.zeros((tall, width), jnp.float32)
            return 0

        lax.fori_loop(0, vectors, clear, 0)

    def take(at):
        keep = mark[at] > 0.5

        def one(k, _):
            moved[k, at] = jnp.where(keep, field[k, at], 0.0)
            return 0

        lax.fori_loop(0, vectors, one, 0, unroll=vectors)

    def weights(before, here, after):
        scale = here * jnp.float32(1.0 / 6.0)
        return scale * (before + after + two_sided(here)), scale

    def apply_once(s):
        degree, scale = weights(mark[s - 1], mark[s], mark[s + 1])

        def one(k, _):
            here = moved[k, s]
            once[k, s] = degree * here - scale * (moved[k, s - 1] + moved[k, s + 1] + two_sided(here))
            return 0

        lax.fori_loop(0, vectors, one, 0, unroll=vectors)

    def apply_twice(s):
        degree, scale = weights(mark[s - 1], mark[s], mark[s + 1])

        def one(k, _):
            here = once[k, s]
            value = degree * here - scale * (once[k, s - 1] + once[k, s + 1] + two_sided(here))
            image[k, s - pad - REACH] = value[0:lines]
            return 0

        @pl.when(in_band(s))
        def _():
            lax.fori_loop(0, vectors, one, 0, unroll=vectors)

    def add_gram(read, which):
        block = jnp.concatenate(
            [read(g).reshape(8 * vectors, width) for g in range(lines // 8)], axis=1)
        high = block.astype(jnp.bfloat16)
        low = (block - high.astype(jnp.float32)).astype(jnp.bfloat16)
        dot = functools.partial(
            lax.dot_general, dimension_numbers=(((1,), (1,)), ((), ())), preferred_element_type=jnp.float32)
        acc[which, 0] += dot(high, high)
        acc[which, 1] += dot(high, low)

    def gram_of(s):
        add_gram(lambda g: once[:, s, 8 * g : 8 * g + 8, :], 0)

    def in_band(s):
        return (s >= pad + REACH) & (s < pad + window - REACH)

    def wait_plane(way, j, at):
        remote(fiedler.at[:, 0], field.at[:, at, 0:lines], plane_s.at[way, j - 1], plane_r.at[way, j - 1],
               (c, l)).wait_recv()

    def wait_edges(way, j, at):
        remote(fiedler.at[:, 0, lo], field.at[:, at, nxt], edge_s.at[way, j - 1, 0], edge_r.at[way, j - 1, 0],
               (c, l)).wait_recv()
        remote(fiedler.at[:, 0, hi], field.at[:, at, prv], edge_s.at[way, j - 1, 1], edge_r.at[way, j - 1, 1],
               (c, l)).wait_recv()

    def near_use(j, _):
        at = near_edge + d * j

        @pl.when(j <= near)
        def _():
            wait_edges(near_way, j, at)
            mark[at] = jnp.where(counted[near_way] >= j.astype(jnp.float32) - 0.5, 1.0, 0.0)
            take(at)

        @pl.when(j <= near + 1)
        def _():
            apply_once(at - d)

        @pl.when(in_band(at - d) & (jnp.logical_not(is_end) | (j == 1)))
        def _():
            gram_of(at - d)

        apply_twice(at - 2 * d)
        return 0

    def near_step(j, _):
        goes_on = is_end & passed_on(j, near)

        @pl.when(j <= near)
        def _():
            wait_plane(near_way, j, near_edge + d * j)

        @pl.when(goes_on)
        def _():
            for copy in pass_copies(j):
                copy.start()

        begin = jnp.where(is_end & passed_on(j - 1, near), j - 1, j)
        lax.fori_loop(begin, jnp.where(goes_on, j, j + 1), near_use, 0)
        return 0

    def far_step(j, _):
        at = far_edge - d * j
        wait_plane(far_way, j, at)
        wait_edges(far_way, j, at)
        mark[at] = jnp.where(counted[far_way] >= (far - j + 1).astype(jnp.float32) - 0.5, 1.0, 0.0)
        take(at)
        apply_once(at + d)

        @pl.when(in_band(at + d))
        def _():
            gram_of(at + d)

        apply_twice(at + 2 * d)
        return 0

    def other_step(j, _):
        at = near_edge - d * (j - 1)
        toward, away = 1.0 - mark[at + d], jnp.where(j < near, 1.0 - mark[at - d], 0.0)
        here = 1.0 - mark[at]
        degree, scale = weights(toward, here, away)

        def one(k, _):
            def part(keep, index):
                return jnp.where(keep > 0.5, field[k, index], 0.0)

            value = part(here, at)
            value = degree * value - scale * (part(toward, at + d) + part(away, at - d) + two_sided(value))
            spare[k] = value[0:lines]
            return 0

        lax.fori_loop(0, vectors, one, 0, unroll=vectors)
        add_gram(lambda g: spare[:, 8 * g : 8 * g + 8, :], 1)
        return 0

    def take_own(m, _):
        take(near_edge - d * m)
        return 0

    def inner_once(m, _):
        s = near_edge - d * m

        @pl.when((s > pad) & (s < pad + window - 1))
        def _():
            apply_once(s)

        @pl.when(in_band(s))
        def _():
            gram_of(s)
        return 0

    def inner_twice(m, _):
        apply_twice(near_edge - d * m)
        return 0

    def end_gram():
        @pl.when(is_end)
        def _():
            lax.fori_loop(1, 2, near_step, 0)
            lax.fori_loop(1, near + 1, other_step, 0)

    load_field.wait()
    ready = min(CHUNKS - 1, plan.end_near // chunk)
    for i in range(CHUNKS):
        for copy in own_copies(i):
            copy.wait_recv()
        lax.fori_loop(i * chunk, (i + 1) * chunk, take_own, 0)
        lax.fori_loop(max(1, i * chunk - 1), (i + 1) * chunk - 1, inner_once, 0)
        if i == 0:
            for way, total in ((0, below), (1, above)):
                @pl.when(total > 0)
                def _():
                    for copy in count_copies(way):
                        copy.wait_recv()
        if i == ready:
            end_gram()

    @pl.when(jnp.logical_not(is_end))
    def _():
        lax.fori_loop(2, planes - 2, inner_twice, 0)
        lax.fori_loop(1, near + 1, near_step, 0)

    lax.fori_loop(1, far + 1, far_step, 0)

    me = c * lanes + l
    lane_of = functools.partial(lax.broadcasted_iota, jnp.int32)
    for which in range(2):
        total = acc[which, 0] + (acc[which, 1] + acc[which, 1].T)
        shape = (vectors, 8, width)
        diagonal = lane_of(shape, 1) == lax.rem(lane_of(shape, 2), 8)
        rows = jnp.sum(jnp.where(diagonal, total.reshape(shape), 0.0), axis=1)
        ones = jnp.where(lax.div(lane_of((width, width), 0), 8) == lax.div(lane_of((width, width), 1), 8), 1.0, 0.0)
        rows = jnp.dot(rows, ones, precision=lax.Precision.HIGHEST, preferred_element_type=jnp.float32)
        half = (8, width)
        pick = lane_of(half, 0) == lax.rem(lane_of(half, 1), 8)
        for h in range(vectors // 8):
            row = jnp.sum(jnp.where(pick, rows[8 * h : 8 * h + 8], 0.0), axis=0, keepdims=True)
            for place in range(2):
                @pl.when((side if which == 0 else 1 - side) == place)
                def _():
                    packed[place * (vectors // 8) + h : place * (vectors // 8) + h + 1, :] = row
    count_rows = 2 * (vectors // 8)
    body = packed.at[0:count_rows]
    for dc in range(chain):
        for dl in range(lanes):
            if dc or dl:
                remote(body, got.at[me, 0:count_rows], gram_s.at[0], gram_r.at[0],
                       (lax.rem(c + dc, chain), lax.rem(l + dl, lanes))).start()
    got[me, 0:count_rows] = packed[0:count_rows]

    for j in range(EARLY_PLANES + 1, most + 1):
        send_plane(j, True)

    @pl.when(is_end)
    def _():
        lax.fori_loop(2, planes - 2, inner_twice, 0)
        lax.fori_loop(2, near, near_step, 0)

    everyone = got.at[0 : chain * lanes - 1, 0:count_rows]
    remote(everyone, everyone, gram_s.at[0], gram_r.at[0], (c, l)).wait_recv()

    def sum_one(i, total):
        return total + got[i, 0:count_rows]

    total = lax.fori_loop(1, chain * lanes, sum_one, got[0, 0:count_rows], unroll=True)
    tall_shape = (vectors, width)
    inside = lax.div(lane_of(tall_shape, 1), 8) == lane_of(tall_shape, 0)
    choose = jnp.where(
        lax.rem(lane_of((width, width), 0), 8) == lax.rem(lane_of((width, width), 1), 8), 1.0, 0.0)
    for place in range(2):
        result = jnp.zeros(tall_shape, jnp.float32)
        for h in range(vectors // 8):
            i = place * (vectors // 8) + h
            spread = jnp.where(inside, jnp.broadcast_to(total[i : i + 1], tall_shape), 0.0)
            spread = jnp.dot(spread, choose, precision=lax.Precision.HIGHEST, preferred_element_type=jnp.float32)
            result = jnp.where(lax.div(lane_of(tall_shape, 1), 8) == h, spread, result)
        gram[place] = result[:, 0:vectors] / scale_of

    @pl.when(is_end)
    def _():
        lax.fori_loop(near, near + 3, near_step, 0)

    remote(everyone, everyone, gram_s.at[0], gram_r.at[0], (c, l)).wait_send()
    for i in range(CHUNKS):
        for copy in own_copies(i):
            copy.wait_send()
    for copy in lab_copies:
        copy.wait_send()
    for way, total, across in sends:
        @pl.when(total > 0)
        def _():
            for copy in count_copies(way):
                copy.wait_send()
        for j in range(1, most + 1):
            @pl.when(j <= total)
            def _():
                plane_copy(way, j).wait_send()

                @pl.when(jnp.logical_not(across & passed_on(j, total)))
                def _():
                    for copy in corner_copies(way, j):
                        copy.wait_send()
    for j in range(1, most + 1):
        @pl.when(is_end & passed_on(j, near))
        def _():
            for copy in pass_copies(j):
                copy.wait_send()


def store_kernel(image, gram, image_out, gram_out, sems):
    part = image.shape[0] // STORES
    copies = [pltpu.make_async_copy(gram, gram_out, sems.at[STORES])]
    for i in range(STORES):
        rows = pl.ds(i * part, part)
        copies.append(pltpu.make_async_copy(image.at[rows], image_out.at[rows], sems.at[i]))
    for copy in copies:
        copy.start()
    for copy in copies:
        copy.wait()


def per_device(fiedler, side_labels):
    chain, lanes = lax.axis_size("chain"), lax.axis_size("lane")
    vectors, planes, lines, width = fiedler.shape
    plan = Plan(chain, lanes, vectors, planes, lines, width)
    slots = plan.band * plan.half * lines * lanes * width
    tall, frames, most = lines + 8, plan.frames, plan.most
    f32, dma = jnp.float32, pltpu.SemaphoreType.DMA
    anywhere, vmem = pl.BlockSpec(memory_space=pl.ANY), pl.BlockSpec(memory_space=pltpu.VMEM)
    image, gram = pl.pallas_call(
        functools.partial(kernel, plan, float(slots)),
        in_specs=[anywhere, anywhere],
        out_specs=[vmem, vmem],
        out_shape=[
            pltpu.VMEM((vectors, plan.band, lines, width), f32),
            pltpu.VMEM((2, vectors, vectors), f32),
        ],
        scratch_shapes=[
            pltpu.VMEM((vectors, frames, tall, width), f32),
            pltpu.VMEM((vectors, frames, tall, width), f32),
            pltpu.VMEM((vectors, frames, tall, width), f32),
            pltpu.VMEM((frames, tall, width), f32),
            pltpu.VMEM((planes, tall, width), jnp.int32),
            pltpu.VMEM((2, lines, width), f32),
            pltpu.VMEM((2, tall, width), f32),
            pltpu.VMEM((vectors, lines, width), f32),
            pltpu.VMEM((2, 2, 8 * vectors, 8 * vectors), f32),
            pltpu.VMEM((8, width), f32),
            pltpu.VMEM((chain * lanes, 8, width), f32),
            dma((2,)), dma((2,)), dma((2,)), dma((CHUNKS, 2)), dma((CHUNKS, 2)),
            dma((2, most)), dma((2, most)), dma((2, most, 2)), dma((2, most, 2)), dma((most, 2)),
            dma((2, 3)), dma((2, 3)), dma((1,)), dma((1,)),
        ],
        compiler_params=pltpu.CompilerParams(
            collective_id=0, has_side_effects=True, vmem_limit_bytes=56 * 1024 * 1024),
        name="laplace",
    )(fiedler, side_labels)
    return pl.pallas_call(
        store_kernel,
        in_specs=[vmem, vmem],
        out_specs=[anywhere, anywhere],
        out_shape=[jax.ShapeDtypeStruct(a.shape, a.dtype) for a in (image, gram)],
        scratch_shapes=[dma((STORES + 1,))],
        compiler_params=pltpu.CompilerParams(vmem_limit_bytes=1024 * 1024),
        name="store",
    )(*(pltpu.with_memory_space_constraint(a, pltpu.VMEM) for a in (image, gram)))


def solution(mesh):
    return jax.shard_map(
        per_device,
        mesh=mesh,
        in_specs=(P(None, "chain", "lane", None), P("chain", "lane", None)),
        out_specs=(P(None, "chain", "lane", None), P()),
        check_vma=False,
    )
```

```python
import functools

import jax
import jax.numpy as jnp
from jax import lax
from jax.experimental import pallas as pl
from jax.experimental.pallas import tpu as pltpu
from jax.sharding import PartitionSpec as P

REACH = 2
CHUNKS = 3
PARTS = 2
STORES = 4
MESH = pl.DeviceIdType.MESH


def two_sided(field):
    return (
        pltpu.roll(field, 1, 0) + pltpu.roll(field, field.shape[0] - 1, 0)
        + pltpu.roll(field, 1, 1) + pltpu.roll(field, field.shape[1] - 1, 1)
    )


class Plan:
    def __init__(self, chain, lanes, vectors, planes, lines, width):
        self.chain, self.lanes, self.vectors, self.planes, self.lines, self.width = (
            chain, lanes, vectors, planes, lines, width)
        self.half = chain // 2
        self.band = planes + planes // 4
        self.grow = self.band - planes
        self.margin = self.grow * self.half // 2
        self.window = self.band + 2 * REACH
        spots = [self.spot(w, max_of=max) for w in range(self.half)]
        self.most = max(max(below, above) for _, below, above in spots)
        assert self.most <= planes and 8 * vectors == width
        assert spots[0][1] == spots[-1][2] > 4 and spots[0][2] == spots[-1][1] == 0
        self.end_near = spots[0][1]
        self.most_far = max(min(below, above) for _, below, above in spots)
        self.chunk = planes // CHUNKS
        assert self.chunk * CHUNKS == planes and self.chunk > 2 and vectors % PARTS == 0
        self.pad = 1 + max(max(0, -slot) for slot, _, _ in spots)
        tail = 1 + max(max(0, slot + planes - self.window) for slot, _, _ in spots)
        self.frames = self.pad + self.window + tail

    def spot(self, w, max_of=jnp.maximum):
        first, last = (w == 0), (w == self.half - 1)
        if not isinstance(w, int):
            first, last = first.astype(jnp.int32), last.astype(jnp.int32)
        slot = self.margin + REACH - self.grow * w
        below = max_of(0, slot - REACH * first)
        above = max_of(0, self.window - REACH * last - slot - self.planes)
        return slot, below, above

    def is_end(self, c):
        within = self.place(c)[1]
        return (within == 0) | (within == self.half - 1)

    def place(self, c):
        relative = lax.rem(c + (self.chain - self.chain // 4), self.chain)
        side = lax.div(relative, self.half)
        within = relative - side * self.half
        return side, within


def kernel(plan, scale_of, fiedler, labels, image, gram, field, moved, once, mark, label, count, counted, spare, acc,
           weight, packed, handed, got, local_sem, lab_s, lab_r, own_s, own_r, plane_s, plane_r, last_s, last_r, edge_s, edge_r, pass_s, cnt_s, cnt_r,
           hand_s, hand_r, gram_s, gram_r):
    chain, lanes, vectors, planes, lines, width = (
        plan.chain, plan.lanes, plan.vectors, plan.planes, plan.lines, plan.width)
    window, pad, most = plan.window, plan.pad, plan.most
    c, l = lax.axis_index("chain"), lax.axis_index("lane")
    up_c, down_c = lax.rem(c + 1, chain), lax.rem(c + chain - 1, chain)
    up_l, down_l = lax.rem(l + 1, lanes), lax.rem(l + lanes - 1, lanes)
    side, within = plan.place(c)
    slot, below, above = plan.spot(within)
    up_side, up_within = plan.place(up_c)
    down_side, down_within = plan.place(down_c)
    up_slot, up_count, _ = plan.spot(up_within)
    down_slot, _, down_count = plan.spot(down_within)
    tall = lines + 8
    lo, hi = slice(0, REACH), slice(lines - REACH, lines)
    nxt, prv = slice(lines, lines + REACH), slice(tall - REACH, tall)

    def remote(src, dst, send, recv, device):
        return pltpu.make_async_remote_copy(
            src_ref=src, dst_ref=dst, send_sem=send, recv_sem=recv, device_id=device, device_id_type=MESH)

    base = pad + slot
    is_end = (within == 0) | (within == plan.half - 1)
    lower = within < plan.half // 2
    d = jnp.where(lower, -1, 1)
    near_way, far_way = jnp.where(lower, 0, 1), jnp.where(lower, 1, 0)
    near, far = jnp.where(lower, below, above), jnp.where(lower, above, below)
    near_edge = jnp.where(lower, base, base + planes - 1)
    far_edge = jnp.where(lower, base + planes - 1, base)

    load_field = pltpu.make_async_copy(fiedler, field.at[:, pl.ds(base, planes), 0:lines], local_sem.at[0])
    load_label = pltpu.make_async_copy(labels, label.at[:, 0:lines], local_sem.at[1])
    load_label.start()
    load_field.start()

    barrier = pltpu.get_barrier_semaphore()
    for dc in range(chain):
        for dl in range(lanes):
            if dc or dl:
                pl.semaphore_signal(barrier, inc=1, device_id=(lax.rem(c + dc, chain), lax.rem(l + dl, lanes)),
                                    device_id_type=MESH)
    load_label.wait()
    totals = [jnp.zeros((lines, width), jnp.float32) for _ in range(2)]
    for p in range(planes):
        here = label[p, 0:lines]
        totals[0] += jnp.where((here == up_side) & (p >= planes - up_count), 1.0, 0.0)
        totals[1] += jnp.where((here == down_side) & (p < down_count), 1.0, 0.0)
    for way in range(2):
        count[way] = totals[way]
    pl.semaphore_wait(barrier, chain * lanes - 1)

    lab_copies = [
        remote(label.at[:, lo], label.at[:, nxt], lab_s.at[0], lab_r.at[0], (c, down_l)),
        remote(label.at[:, hi], label.at[:, prv], lab_s.at[1], lab_r.at[1], (c, up_l)),
    ]
    chunk = plan.chunk

    def own_copies(i):
        start = jnp.where(lower, i * chunk, planes - (i + 1) * chunk)
        at = pl.ds(base + start, chunk)
        return [
            remote(field.at[:, at, lo], field.at[:, at, nxt], own_s.at[i, 0], own_r.at[i, 0], (c, down_l)),
            remote(field.at[:, at, hi], field.at[:, at, prv], own_s.at[i, 1], own_r.at[i, 1], (c, up_l)),
        ]

    sends = ((0, up_count, up_side != side), (1, down_count, down_side != side))

    def spot_of(way, j):
        if way == 0:
            return base + planes - j, pad + up_slot - j, up_c
        return base + j - 1, pad + down_slot + planes - 1 + j, down_c

    def plane_copy(way, j):
        source, at, to = spot_of(way, j)
        return remote(
            field.at[:, source, 0:lines], field.at[:, at, 0:lines], plane_s.at[way, j - 1], plane_r.at[way, j - 1], (to, l))

    def part_copies(way, j):
        source, at, to = spot_of(way, j)
        share = vectors // PARTS
        return [
            remote(field.at[i * share : (i + 1) * share, source, 0:lines],
                   field.at[i * share : (i + 1) * share, at, 0:lines], last_s.at[way, i], last_r.at[way, i], (to, l))
            for i in range(PARTS)
        ]

    def corner_copies(way, j):
        source, at, to = spot_of(way, j)
        return [
            remote(field.at[:, source, lo], field.at[:, at, nxt], edge_s.at[way, j - 1, 0],
                   edge_r.at[way, j - 1, 0], (to, down_l)),
            remote(field.at[:, source, hi], field.at[:, at, prv], edge_s.at[way, j - 1, 1],
                   edge_r.at[way, j - 1, 1], (to, up_l)),
        ]

    def passed_on(j, total):
        return (j >= 2) & (j <= total - 2)

    def pass_copies(j):
        at = near_edge + d * j
        return [
            remote(field.at[:, at, lo], field.at[:, at, nxt], pass_s.at[j - 1, 0], edge_r.at[near_way, j - 1, 0],
                   (c, down_l)),
            remote(field.at[:, at, hi], field.at[:, at, prv], pass_s.at[j - 1, 1], edge_r.at[near_way, j - 1, 1],
                   (c, up_l)),
        ]

    def each_send(j, act):
        for way, total, across in sends:
            @pl.when((j <= total) & jnp.logical_not(across & passed_on(j, total)))
            def _():
                for copy in corner_copies(way, j):
                    act(copy)

            @pl.when((j < total) | ((j == total) & jnp.logical_not(across)))
            def _():
                act(plane_copy(way, j))

            @pl.when((j == total) & across)
            def _():
                for copy in part_copies(way, j):
                    act(copy)

    def send_plane(j):
        each_send(j, lambda copy: copy.start())

    def count_copies(way):
        to = (up_c, down_c)[way]
        return [
            remote(count.at[way], counted.at[way, 0:lines], cnt_s.at[way, 0], cnt_r.at[way, 0], (to, l)),
            remote(count.at[way, lo], counted.at[way, nxt], cnt_s.at[way, 1], cnt_r.at[way, 1], (to, down_l)),
            remote(count.at[way, hi], counted.at[way, prv], cnt_s.at[way, 2], cnt_r.at[way, 2], (to, up_l)),
        ]

    load_field.wait()
    for way, total, _ in sends:
        @pl.when(total > 0)
        def _():
            for copy in count_copies(way):
                copy.start()
    for copy in lab_copies:
        copy.start()
    send_plane(1)
    for i in range(CHUNKS):
        for copy in own_copies(i):
            copy.start()
    for j in range(2, most + 1):
        send_plane(j)

    for copy in lab_copies:
        copy.wait_recv()
    acc[...] = jnp.zeros(acc.shape, jnp.float32)
    for p in range(planes):
        mark[base + p] = jnp.where(label[p] == side, 1.0, 0.0)

    @pl.when(is_end)
    def _():
        mark[near_edge + d * (near + 1)] = jnp.zeros((tall, width), jnp.float32)

    def take(at):
        keep = mark[at] > 0.5

        def one(k, _):
            moved[k, at] = jnp.where(keep, field[k, at], 0.0)
            return 0

        lax.fori_loop(0, vectors, one, 0, unroll=vectors)

    def weights(before, here, after):
        scale = here * jnp.float32(1.0 / 6.0)
        return scale * (before + after + two_sided(here)), scale

    def apply_once(s):
        degree, scale = weights(mark[s - 1], mark[s], mark[s + 1])

        def one(k, _):
            here = moved[k, s]
            once[k, s] = degree * here - scale * (moved[k, s - 1] + moved[k, s + 1] + two_sided(here))
            return 0

        lax.fori_loop(0, vectors, one, 0, unroll=vectors)

    def apply_twice(s):
        degree, scale = weights(mark[s - 1], mark[s], mark[s + 1])

        def one(k, _):
            here = once[k, s]
            value = degree * here - scale * (once[k, s - 1] + once[k, s + 1] + two_sided(here))
            image[k, s - pad - REACH] = value[0:lines]
            return 0

        @pl.when(in_band(s))
        def _():
            lax.fori_loop(0, vectors, one, 0, unroll=vectors)

    def add_gram(reads, which):
        block = jnp.concatenate(
            [read(g).reshape(8 * vectors, width) for read in reads for g in range(lines // 8)], axis=1)
        high = block.astype(jnp.bfloat16)
        low = (block - high.astype(jnp.float32)).astype(jnp.bfloat16)
        dot = functools.partial(
            lax.dot_general, dimension_numbers=(((1,), (1,)), ((), ())), preferred_element_type=jnp.float32)
        acc[which, 0] += dot(high, high)
        acc[which, 1] += dot(high, low)

    def gram_of(spots):
        def reader(s, counts):
            def read(g):
                return jnp.where(counts & in_band(s), once[:, s, 8 * g : 8 * g + 8, :], 0.0)

            return read

        add_gram([reader(s, counts) for s, counts in spots], 0)

    def in_band(s):
        return (s >= pad + REACH) & (s < pad + window - REACH)

    def wait_plane(way, j, at):
        remote(fiedler.at[:, 0], field.at[:, at, 0:lines], plane_s.at[way, j - 1], plane_r.at[way, j - 1],
               (c, l)).wait_recv()

    def wait_edges(way, j, at):
        remote(fiedler.at[:, 0, lo], field.at[:, at, nxt], edge_s.at[way, j - 1, 0], edge_r.at[way, j - 1, 0],
               (c, l)).wait_recv()
        remote(fiedler.at[:, 0, hi], field.at[:, at, prv], edge_s.at[way, j - 1, 1], edge_r.at[way, j - 1, 1],
               (c, l)).wait_recv()

    def near_mark(j):
        at = near_edge + d * j
        wait_edges(near_way, j, at)
        mark[at] = jnp.where(counted[near_way] >= (j + 0.0) - 0.5, 1.0, 0.0)

    def near_use(j, _):
        at = near_edge + d * j
        near_mark(j)
        take(at)
        apply_once(at - d)
        apply_twice(at - 2 * d)
        return 0

    def last_use():
        at = near_edge + d * near
        near_mark(near)
        for i in range(3):
            s = at - d * i
            degree, scale = weights(mark[s - 1], mark[s], mark[s + 1])
            weight[i, 0], weight[i, 1] = degree, scale

        def step(i, here, beside):
            return weight[i, 0] * here - weight[i, 1] * (beside + two_sided(here))

        def one(k, _):
            moved_0 = jnp.where(mark[at] > 0.5, field[k, at], 0.0)
            moved_1 = moved[k, at - d]
            once_0 = step(0, moved_0, moved_1)
            once_1 = step(1, moved_1, moved_0 + moved[k, at - 2 * d])
            once_2 = once[k, at - 2 * d]
            values = (
                step(0, once_0, once_1), step(1, once_1, once_0 + once_2),
                step(2, once_2, once_1 + once[k, at - 3 * d]))
            for i in range(3):
                image[k, at - d * i - pad - REACH] = values[i][0:lines]
            return 0

        share = vectors // PARTS
        for i in range(PARTS):
            part = field.at[i * share : (i + 1) * share, at, 0:lines]
            remote(part, part, last_s.at[near_way, i], last_r.at[near_way, i], (c, l)).wait_recv()
            lax.fori_loop(i * share, (i + 1) * share, one, 0, unroll=share)

    def arrive(j):
        wait_plane(near_way, j, near_edge + d * j)

        @pl.when(is_end & passed_on(j, near))
        def _():
            for copy in pass_copies(j):
                copy.start()

    def near_step(j, _):
        arrive(j)
        begin = jnp.where(is_end & passed_on(j - 1, near), j - 1, j)
        lax.fori_loop(begin, jnp.where(is_end & passed_on(j, near), j, j + 1), near_use, 0)
        return 0

    def far_step(j, _):
        at = far_edge - d * j
        wait_plane(far_way, j, at)
        wait_edges(far_way, j, at)
        mark[at] = jnp.where(counted[far_way] >= (far - j + 1).astype(jnp.float32) - 0.5, 1.0, 0.0)
        take(at)
        apply_once(at + d)

        apply_twice(at + 2 * d)
        return 0

    def other_step(j, _):
        at = near_edge - d * (j - 1)
        toward, away = 1.0 - mark[at + d], jnp.where(j < near, 1.0 - mark[at - d], 0.0)
        here = 1.0 - mark[at]
        degree, scale = weights(toward, here, away)

        def one(k, _):
            def part(keep, index):
                return jnp.where(keep > 0.5, field[k, index], 0.0)

            value = part(here, at)
            value = degree * value - scale * (part(toward, at + d) + part(away, at - d) + two_sided(value))
            spare[k, j - 1] = value[0:lines]
            return 0

        lax.fori_loop(0, vectors, one, 0, unroll=vectors)
        return 0

    def take_own(m, _):
        take(near_edge - d * m)
        return 0

    def inner_once(m, _):
        s = near_edge - d * m

        @pl.when((s > pad) & (s < pad + window - 1))
        def _():
            apply_once(s)
        return 0

    def inner_twice(m, _):
        apply_twice(near_edge - d * m)
        return 0

    def end_gram():
        @pl.when(is_end)
        def _():
            lax.fori_loop(1, 2, near_step, 0)
            lax.fori_loop(1, near + 1, other_step, 0)
            add_gram([lambda g, p=p: spare[:, p, 8 * g : 8 * g + 8, :] for p in range(plan.end_near)], 1)

    ready = min(CHUNKS - 1, plan.end_near // chunk)
    for i in range(CHUNKS):
        for copy in own_copies(i):
            copy.wait_recv()
        lax.fori_loop(i * chunk, (i + 1) * chunk, take_own, 0)
        inner = max(1, i * chunk - 1), (i + 1) * chunk - 1
        lax.fori_loop(*inner, inner_once, 0)
        gram_of([(near_edge - d * m, True) for m in range(*inner)])
        if i == 0:
            for way, total in ((0, below), (1, above)):
                @pl.when(total > 0)
                def _():
                    for copy in count_copies(way):
                        copy.wait_recv()
        if i == ready:
            end_gram()

            @pl.when(is_end)
            def _():
                arrive(2)

    @pl.when(jnp.logical_not(is_end))
    def _():
        lax.fori_loop(1, near + 1, near_step, 0)
        gram_of([(near_edge + d * (j - 1), j <= near) for j in range(1, most + 1)])

    lax.fori_loop(1, far + 1, far_step, 0)
    gram_of([(near_edge, is_end)] + [(far_edge - d * (j - 1), j <= far) for j in range(1, plan.most_far + 1)])

    lane_of = functools.partial(lax.broadcasted_iota, jnp.int32)
    ones = jnp.where(lax.div(lane_of((width, width), 0), 8) == lax.div(lane_of((width, width), 1), 8), 1.0, 0.0)
    pick = lane_of((8, width), 0) == lax.rem(lane_of((8, width), 1), 8)
    shape = (vectors, 8, width)
    diagonal = lane_of(shape, 1) == lax.rem(lane_of(shape, 2), 8)
    rows = []
    for which in range(2):
        total = acc[which, 0] + (acc[which, 1] + acc[which, 1].T)
        rows.append(jnp.sum(jnp.where(diagonal, total.reshape(shape), 0.0), axis=1))
    folded = jnp.dot(jnp.concatenate(rows, axis=0), ones, precision=lax.Precision.HIGHEST,
                     preferred_element_type=jnp.float32)
    parts = vectors // 8
    terms = [jnp.sum(jnp.where(pick, folded[8 * h : 8 * h + 8], 0.0), axis=0, keepdims=True) for h in range(2 * parts)]
    for h in range(parts):
        packed[h : h + 1, :] = jnp.where(side == 0, terms[h], terms[parts + h])
        packed[parts + h : parts + h + 1, :] = jnp.where(side == 0, terms[parts + h], terms[h])
    count_rows = 2 * parts
    body = packed.at[0:count_rows]
    chips = chain // 2 * lanes
    slot_of = lax.div(c, 2) * lanes + l
    partner = c + 1 - 2 * lax.rem(c, 2)
    leads = jnp.logical_not(is_end) & (plan.is_end(partner) | (lax.rem(c, 2) == 0))
    hand_over = remote(body, handed.at[0:count_rows], hand_s.at[0], hand_r.at[0], (partner, l))

    def broadcast(dc, dl):
        return remote(got.at[slot_of, 0:count_rows], got.at[slot_of, 0:count_rows], gram_s.at[0], gram_r.at[0],
                      (lax.rem(c + dc, chain), lax.rem(l + dl, lanes)))

    @pl.when(jnp.logical_not(leads))
    def _():
        hand_over.start()

    @pl.when(leads)
    def _():
        hand_over.wait_recv()
        got[slot_of, 0:count_rows] = packed[0:count_rows] + handed[0:count_rows]
        for dc in range(chain):
            for dl in range(lanes):
                if dc or dl:
                    broadcast(dc, dl).start()

    @pl.when(is_end)
    def _():
        arrive(3)

    lax.fori_loop(2, planes - 2, inner_twice, 0)

    @pl.when(is_end)
    def _():
        lax.fori_loop(2, 3, near_use, 0)
        lax.fori_loop(4, near, near_step, 0)

    def many(total):
        return remote(got.at[0:total, 0:count_rows], got.at[0:total, 0:count_rows], gram_s.at[0], gram_r.at[0], (c, l))

    @pl.when(leads)
    def _():
        many(chips - 1).wait_recv()

    @pl.when(jnp.logical_not(leads))
    def _():
        many(chips).wait_recv()

    def sum_one(i, total):
        return total + got[i, 0:count_rows]

    total = lax.fori_loop(1, chips, sum_one, got[0, 0:count_rows], unroll=True)
    tall_shape = (vectors, width)
    inside = lax.div(lane_of(tall_shape, 1), 8) == lane_of(tall_shape, 0)
    choose = jnp.where(
        lax.rem(lane_of((width, width), 0), 8) == lax.rem(lane_of((width, width), 1), 8), 1.0, 0.0)
    for place in range(2):
        result = jnp.zeros(tall_shape, jnp.float32)
        for h in range(vectors // 8):
            i = place * (vectors // 8) + h
            spread = jnp.where(inside, jnp.broadcast_to(total[i : i + 1], tall_shape), 0.0)
            spread = jnp.dot(spread, choose, precision=lax.Precision.HIGHEST, preferred_element_type=jnp.float32)
            result = jnp.where(lax.div(lane_of(tall_shape, 1), 8) == h, spread, result)
        gram[place] = result[:, 0:vectors] / scale_of

    def finish(copy):
        copy.wait_send()

    @pl.when(leads)
    def _():
        sent = got.at[0 : chain * lanes - 1, 0:count_rows]
        remote(sent, sent, gram_s.at[0], gram_r.at[0], (c, l)).wait_send()

    @pl.when(jnp.logical_not(leads))
    def _():
        hand_over.wait_send()

    for i in range(CHUNKS):
        for copy in own_copies(i):
            copy.wait_send()
    for copy in lab_copies:
        copy.wait_send()
    for way, total, _ in sends:
        @pl.when(total > 0)
        def _():
            for copy in count_copies(way):
                copy.wait_send()
    for j in range(1, most + 1):
        @pl.when(is_end & passed_on(j, near))
        def _():
            for copy in pass_copies(j):
                copy.wait_send()
    for j in range(1, most - 1):
        each_send(j, finish)

    @pl.when(is_end)
    def _():
        last_use()

    for j in range(max(1, most - 1), most + 1):
        each_send(j, finish)


def store_kernel(image, gram, image_out, gram_out, sems):
    part = image.shape[0] // STORES
    copies = [pltpu.make_async_copy(gram, gram_out, sems.at[STORES])]
    for i in range(STORES):
        rows = pl.ds(i * part, part)
        copies.append(pltpu.make_async_copy(image.at[rows], image_out.at[rows], sems.at[i]))
    for copy in copies:
        copy.start()
    for copy in copies:
        copy.wait()


def per_device(fiedler, side_labels):
    chain, lanes = lax.axis_size("chain"), lax.axis_size("lane")
    vectors, planes, lines, width = fiedler.shape
    plan = Plan(chain, lanes, vectors, planes, lines, width)
    slots = plan.band * plan.half * lines * lanes * width
    tall, frames, most = lines + 8, plan.frames, plan.most
    f32, dma = jnp.float32, pltpu.SemaphoreType.DMA
    anywhere, vmem = pl.BlockSpec(memory_space=pl.ANY), pl.BlockSpec(memory_space=pltpu.VMEM)
    image, gram = pl.pallas_call(
        functools.partial(kernel, plan, float(slots)),
        in_specs=[anywhere, anywhere],
        out_specs=[vmem, vmem],
        out_shape=[
            pltpu.VMEM((vectors, plan.band, lines, width), f32),
            pltpu.VMEM((2, vectors, vectors), f32),
        ],
        scratch_shapes=[
            pltpu.VMEM((vectors, frames, tall, width), f32),
            pltpu.VMEM((vectors, frames, tall, width), f32),
            pltpu.VMEM((vectors, frames, tall, width), f32),
            pltpu.VMEM((frames, tall, width), f32),
            pltpu.VMEM((planes, tall, width), jnp.int32),
            pltpu.VMEM((2, lines, width), f32),
            pltpu.VMEM((2, tall, width), f32),
            pltpu.VMEM((vectors, plan.end_near, lines, width), f32),
            pltpu.VMEM((2, 2, 8 * vectors, 8 * vectors), f32),
            pltpu.VMEM((3, 2, tall, width), f32),
            pltpu.VMEM((8, width), f32),
            pltpu.VMEM((8, width), f32),
            pltpu.VMEM((chain * lanes, 8, width), f32),
            dma((2,)), dma((2,)), dma((2,)), dma((CHUNKS, 2)), dma((CHUNKS, 2)),
            dma((2, most)), dma((2, most)), dma((2, PARTS)), dma((2, PARTS)), dma((2, most, 2)), dma((2, most, 2)), dma((most, 2)),
            dma((2, 3)), dma((2, 3)), dma((1,)), dma((1,)), dma((1,)), dma((1,)),
        ],
        compiler_params=pltpu.CompilerParams(
            collective_id=0, has_side_effects=True, vmem_limit_bytes=56 * 1024 * 1024),
        name="laplace",
    )(fiedler, side_labels)
    return pl.pallas_call(
        store_kernel,
        in_specs=[vmem, vmem],
        out_specs=[anywhere, anywhere],
        out_shape=[jax.ShapeDtypeStruct(a.shape, a.dtype) for a in (image, gram)],
        scratch_shapes=[dma((STORES + 1,))],
        compiler_params=pltpu.CompilerParams(vmem_limit_bytes=1024 * 1024),
        name="store",
    )(*(pltpu.with_memory_space_constraint(a, pltpu.VMEM) for a in (image, gram)))


def solution(mesh):
    return jax.shard_map(
        per_device,
        mesh=mesh,
        in_specs=(P(None, "chain", "lane", None), P("chain", "lane", None)),
        out_specs=(P(None, "chain", "lane", None), P()),
        check_vma=False,
    )
```

```python
import functools

import jax
import jax.numpy as jnp
from jax import lax
from jax.experimental import pallas as pl
from jax.experimental.pallas import tpu as pltpu
from jax.sharding import PartitionSpec as P

REACH = 2
CHUNKS = 3
PARTS = 2
STORES = 4
MESH = pl.DeviceIdType.MESH


def two_sided(field):
    return (
        pltpu.roll(field, 1, 0) + pltpu.roll(field, field.shape[0] - 1, 0)
        + pltpu.roll(field, 1, 1) + pltpu.roll(field, field.shape[1] - 1, 1)
    )


class Plan:
    def __init__(self, chain, lanes, vectors, planes, lines, width):
        self.chain, self.lanes, self.vectors, self.planes, self.lines, self.width = (
            chain, lanes, vectors, planes, lines, width)
        self.half = chain // 2
        self.band = planes + planes // 4
        self.grow = self.band - planes
        self.margin = self.grow * self.half // 2
        self.window = self.band + 2 * REACH
        spots = [self.spot(w, max_of=max) for w in range(self.half)]
        self.most = max(max(below, above) for _, below, above in spots)
        assert self.most <= planes and 8 * vectors == width
        assert spots[0][1] == spots[-1][2] > 4 and spots[0][2] == spots[-1][1] == 0
        self.end_near = spots[0][1]
        self.most_far = max(min(below, above) for _, below, above in spots)
        self.totals = sorted({count for _, below, above in spots for count in (below, above)} - {0})
        self.rounds = chain // 2
        assert self.rounds % 4 == 0 and lanes % 2 == 0 and lanes > 2
        self.chunk = planes // CHUNKS
        assert self.chunk * CHUNKS == planes and self.chunk > 2 and vectors % PARTS == 0
        self.pad = 1 + max(max(0, -slot) for slot, _, _ in spots)
        tail = 1 + max(max(0, slot + planes - self.window) for slot, _, _ in spots)
        self.frames = self.pad + self.window + tail

    def spot(self, w, max_of=jnp.maximum):
        first, last = (w == 0), (w == self.half - 1)
        if not isinstance(w, int):
            first, last = first.astype(jnp.int32), last.astype(jnp.int32)
        slot = self.margin + REACH - self.grow * w
        below = max_of(0, slot - REACH * first)
        above = max_of(0, self.window - REACH * last - slot - self.planes)
        return slot, below, above

    def is_end(self, c):
        within = self.place(c)[1]
        return (within == 0) | (within == self.half - 1)

    def place(self, c):
        relative = lax.rem(c + (self.chain - self.chain // 4), self.chain)
        side = lax.div(relative, self.half)
        within = relative - side * self.half
        return side, within


def kernel(plan, scale_of, fiedler, labels, image, gram, field, moved, once, mark, label, count, counted, spare, acc,
           weight, packed, handed, got, local_sem, lab_s, lab_r, own_s, own_r, plane_s, plane_r, last_r, corner_s, edge_r,
           pass_s, cnt_s, cnt_r, hand_s, hand_r, gram_s, gram_r, lane_told, tell, cross, chain_told):
    chain, lanes, vectors, planes, lines, width = (
        plan.chain, plan.lanes, plan.vectors, plan.planes, plan.lines, plan.width)
    window, pad, most = plan.window, plan.pad, plan.most
    c, l = lax.axis_index("chain"), lax.axis_index("lane")
    up_c, down_c = lax.rem(c + 1, chain), lax.rem(c + chain - 1, chain)
    up_l, down_l = lax.rem(l + 1, lanes), lax.rem(l + lanes - 1, lanes)
    side, within = plan.place(c)
    slot, below, above = plan.spot(within)
    up_side, up_within = plan.place(up_c)
    down_side, down_within = plan.place(down_c)
    up_slot, up_count, _ = plan.spot(up_within)
    down_slot, _, down_count = plan.spot(down_within)
    tall = lines + 8
    lo, hi = slice(0, REACH), slice(lines - REACH, lines)
    nxt, prv = slice(lines, lines + REACH), slice(tall - REACH, tall)

    def remote(src, dst, send, recv, device):
        return pltpu.make_async_remote_copy(
            src_ref=src, dst_ref=dst, send_sem=send, recv_sem=recv, device_id=device, device_id_type=MESH)

    base = pad + slot
    is_end = (within == 0) | (within == plan.half - 1)
    lower = within < plan.half // 2
    d = jnp.where(lower, -1, 1)
    near_way, far_way = jnp.where(lower, 0, 1), jnp.where(lower, 1, 0)
    near, far = jnp.where(lower, below, above), jnp.where(lower, above, below)
    near_edge = jnp.where(lower, base, base + planes - 1)
    far_edge = jnp.where(lower, base + planes - 1, base)

    load_field = pltpu.make_async_copy(fiedler, field.at[:, pl.ds(base, planes), 0:lines], local_sem.at[0])
    load_label = pltpu.make_async_copy(labels, label.at[:, 0:lines], local_sem.at[1])
    load_label.start()
    load_field.start()

    barrier = pltpu.get_barrier_semaphore()
    def signal(sem, device):
        pl.semaphore_signal(sem, inc=1, device_id=device, device_id_type=MESH)

    signal(barrier, (up_c, l))
    signal(barrier, (down_c, l))

    @pl.when(jnp.logical_not(is_end))
    def _():
        signal(barrier, (c, up_l))
        signal(barrier, (c, down_l))

    load_label.wait()
    totals = [jnp.zeros((lines, width), jnp.float32) for _ in range(2)]
    for p in range(planes):
        here = label[p, 0:lines]
        totals[0] += jnp.where((here == up_side) & (p >= planes - up_count), 1.0, 0.0)
        totals[1] += jnp.where((here == down_side) & (p < down_count), 1.0, 0.0)
    for way in range(2):
        count[way] = totals[way]

    @pl.when(is_end)
    def _():
        pl.semaphore_wait(barrier, 2)

    @pl.when(jnp.logical_not(is_end))
    def _():
        pl.semaphore_wait(barrier, 4)
        signal(lane_told.at[0], (c, up_l))
        signal(lane_told.at[0], (c, down_l))

    lab_copies = [
        remote(label.at[:, lo], label.at[:, nxt], lab_s.at[0], lab_r.at[0], (c, down_l)),
        remote(label.at[:, hi], label.at[:, prv], lab_s.at[0], lab_r.at[0], (c, up_l)),
    ]
    chunk = plan.chunk

    def own_copies(i):
        start = jnp.where(lower, i * chunk, planes - (i + 1) * chunk)
        at = pl.ds(base + start, chunk)
        return [
            remote(field.at[:, at, lo], field.at[:, at, nxt], own_s.at[0], own_r.at[i], (c, down_l)),
            remote(field.at[:, at, hi], field.at[:, at, prv], own_s.at[0], own_r.at[i], (c, up_l)),
        ]

    sends = ((0, up_count, up_side != side), (1, down_count, down_side != side))
    up_near, down_near = up_within < plan.half // 2, down_within >= plan.half // 2
    first_sem = (jnp.where(up_near, 0, most), jnp.where(down_near, 0, most))
    count_sem = (jnp.where(up_near, 0, 1), jnp.where(down_near, 0, 1))

    def spot_of(way, j):
        if way == 0:
            return base + planes - j, pad + up_slot - j, up_c
        return base + j - 1, pad + down_slot + planes - 1 + j, down_c

    def plane_copy(way, j):
        source, at, to = spot_of(way, j)
        return remote(
            field.at[:, source, 0:lines], field.at[:, at, 0:lines], plane_s.at[way],
            plane_r.at[first_sem[way] + j - 1], (to, l))

    def part_copies(way, j):
        source, at, to = spot_of(way, j)
        share = vectors // PARTS
        return [
            remote(field.at[i * share : (i + 1) * share, source, 0:lines],
                   field.at[i * share : (i + 1) * share, at, 0:lines], plane_s.at[way], last_r.at[i], (to, l))
            for i in range(PARTS)
        ]

    def corner_copies(way, j):
        source, at, to = spot_of(way, j)
        return [
            remote(field.at[:, source, lo], field.at[:, at, nxt], corner_s.at[way],
                   edge_r.at[first_sem[way] + j - 1], (to, down_l)),
            remote(field.at[:, source, hi], field.at[:, at, prv], corner_s.at[way],
                   edge_r.at[first_sem[way] + j - 1], (to, up_l)),
        ]

    def passed_on(j, total):
        return (j >= 2) & (j <= total - 2)

    def pass_copies(j):
        at = near_edge + d * j
        return [
            remote(field.at[:, at, lo], field.at[:, at, nxt], pass_s.at[0], edge_r.at[j - 1],
                   (c, down_l)),
            remote(field.at[:, at, hi], field.at[:, at, prv], pass_s.at[0], edge_r.at[j - 1],
                   (c, up_l)),
        ]

    def send_plane(j):
        for way, total, across in sends:
            @pl.when((j < total) | ((j == total) & jnp.logical_not(across)))
            def _():
                plane_copy(way, j).start()

            @pl.when((j == total) & across)
            def _():
                for copy in part_copies(way, j):
                    copy.start()

    def send_corners(j):
        for way, total, across in sends:
            @pl.when((j <= total) & jnp.logical_not(across & passed_on(j, total)))
            def _():
                for copy in corner_copies(way, j):
                    copy.start()

    def count_copies(way, corners):
        to = (up_c, down_c)[way]
        send, recv = cnt_s.at[way], cnt_r.at[count_sem[way]]
        if not corners:
            return [remote(count.at[way], counted.at[way, 0:lines], send, recv, (to, l))]
        return [
            remote(count.at[way, lo], counted.at[way, nxt], send, recv, (to, down_l)),
            remote(count.at[way, hi], counted.at[way, prv], send, recv, (to, up_l)),
        ]

    def start_counts(corners):
        for way, total, _ in sends:
            @pl.when(total > 0)
            def _():
                for copy in count_copies(way, corners):
                    copy.start()

    partner = c + 1 - 2 * lax.rem(c, 2)
    partner_end = plan.is_end(partner)
    cross_c = lax.rem(c + d + chain, chain)

    def start_lanes():
        for copy in lab_copies:
            copy.start()
        for i in range(CHUNKS):
            for copy in own_copies(i):
                copy.start()

    load_field.wait()
    start_counts(False)
    send_plane(1)

    @pl.when(is_end)
    def _():
        pl.semaphore_wait(tell.at[0], 1)
        signal(cross.at[0], (cross_c, l))
        start_lanes()
        pl.semaphore_wait(cross.at[0], 1)

    @pl.when(jnp.logical_not(is_end))
    def _():
        start_lanes()
        pl.semaphore_wait(lane_told.at[0], 2)

        @pl.when(partner_end)
        def _():
            signal(tell.at[0], (partner, l))

        signal(lane_told.at[1], (c, up_l))
        signal(lane_told.at[1], (c, down_l))

    start_counts(True)
    send_corners(1)
    for j in range(2, most + 1):
        send_corners(j)
        send_plane(j)

    @pl.when(jnp.logical_not(is_end))
    def _():
        for r in range(1, lanes // 2):
            pl.semaphore_wait(lane_told.at[r], 2)
            if r + 1 < lanes // 2:
                signal(lane_told.at[r + 1], (c, up_l))
                signal(lane_told.at[r + 1], (c, down_l))

    def tell_chain(r):
        signal(chain_told.at[r], (up_c, l))
        signal(chain_told.at[r], (down_c, l))

    def chain_rounds(point):
        each = plan.rounds // 4
        for r in range(point * each, (point + 1) * each):
            pl.semaphore_wait(chain_told.at[r], 2)
            if r + 1 < plan.rounds:
                tell_chain(r + 1)

    tell_chain(0)

    def drain(ref, recv):
        remote(ref, ref, lab_s.at[0], recv, (c, l)).wait_recv()

    def flush(ref, send):
        remote(ref, ref, send, lab_r.at[0], (c, l)).wait_send()

    both = slice(0, 2 * REACH)
    drain(label.at[:, both], lab_r.at[0])
    acc[...] = jnp.zeros(acc.shape, jnp.float32)
    for p in range(planes):
        mark[base + p] = jnp.where(label[p] == side, 1.0, 0.0)

    @pl.when(is_end)
    def _():
        mark[near_edge + d * (near + 1)] = jnp.zeros((tall, width), jnp.float32)

    def take(at):
        keep = mark[at] > 0.5

        def one(k, _):
            moved[k, at] = jnp.where(keep, field[k, at], 0.0)
            return 0

        lax.fori_loop(0, vectors, one, 0, unroll=vectors)

    def weights(before, here, after):
        scale = here * jnp.float32(1.0 / 6.0)
        return scale * (before + after + two_sided(here)), scale

    def apply_once(s):
        degree, scale = weights(mark[s - 1], mark[s], mark[s + 1])

        def one(k, _):
            here = moved[k, s]
            once[k, s] = degree * here - scale * (moved[k, s - 1] + moved[k, s + 1] + two_sided(here))
            return 0

        lax.fori_loop(0, vectors, one, 0, unroll=vectors)

    def apply_twice(s):
        degree, scale = weights(mark[s - 1], mark[s], mark[s + 1])

        def one(k, _):
            here = once[k, s]
            value = degree * here - scale * (once[k, s - 1] + once[k, s + 1] + two_sided(here))
            image[k, s - pad - REACH] = value[0:lines]
            return 0

        @pl.when(in_band(s))
        def _():
            lax.fori_loop(0, vectors, one, 0, unroll=vectors)

    def add_gram(reads, which):
        block = jnp.concatenate(
            [read(g).reshape(8 * vectors, width) for read in reads for g in range(lines // 8)], axis=1)
        high = block.astype(jnp.bfloat16)
        low = (block - high.astype(jnp.float32)).astype(jnp.bfloat16)
        dot = functools.partial(
            lax.dot_general, dimension_numbers=(((1,), (1,)), ((), ())), preferred_element_type=jnp.float32)
        acc[which, 0] += dot(high, high)
        acc[which, 1] += dot(high, low)

    def gram_of(spots):
        def reader(s, counts):
            def read(g):
                return jnp.where(counts & in_band(s), once[:, s, 8 * g : 8 * g + 8, :], 0.0)

            return read

        add_gram([reader(s, counts) for s, counts in spots], 0)

    def in_band(s):
        return (s >= pad + REACH) & (s < pad + window - REACH)

    def wait_plane(index, at):
        drain(field.at[:, at, 0:lines], plane_r.at[index])

    def wait_edges(index, at):
        drain(field.at[:, at, both], edge_r.at[index])

    def near_mark(j):
        at = near_edge + d * j
        wait_edges(j - 1, at)
        mark[at] = jnp.where(counted[near_way] >= (j + 0.0) - 0.5, 1.0, 0.0)

    def near_use(j, _):
        at = near_edge + d * j
        near_mark(j)
        take(at)
        apply_once(at - d)
        apply_twice(at - 2 * d)
        return 0

    def last_use():
        at = near_edge + d * near
        near_mark(near)
        for i in range(3):
            s = at - d * i
            degree, scale = weights(mark[s - 1], mark[s], mark[s + 1])
            weight[i, 0], weight[i, 1] = degree, scale

        def step(i, here, beside):
            return weight[i, 0] * here - weight[i, 1] * (beside + two_sided(here))

        def one(k, _):
            moved_0 = jnp.where(mark[at] > 0.5, field[k, at], 0.0)
            moved_1 = moved[k, at - d]
            once_0 = step(0, moved_0, moved_1)
            once_1 = step(1, moved_1, moved_0 + moved[k, at - 2 * d])
            once_2 = once[k, at - 2 * d]
            values = (
                step(0, once_0, once_1), step(1, once_1, once_0 + once_2),
                step(2, once_2, once_1 + once[k, at - 3 * d]))
            for i in range(3):
                image[k, at - d * i - pad - REACH] = values[i][0:lines]
            return 0

        share = vectors // PARTS
        for i in range(PARTS):
            drain(field.at[i * share : (i + 1) * share, at, 0:lines], last_r.at[i])
            lax.fori_loop(i * share, (i + 1) * share, one, 0, unroll=share)

    def arrive(j):
        wait_plane(j - 1, near_edge + d * j)

        @pl.when(is_end & passed_on(j, near))
        def _():
            for copy in pass_copies(j):
                copy.start()

    def near_step(j, _):
        arrive(j)
        begin = jnp.where(is_end & passed_on(j - 1, near), j - 1, j)
        lax.fori_loop(begin, jnp.where(is_end & passed_on(j, near), j, j + 1), near_use, 0)
        return 0

    def far_step(j, _):
        at = far_edge - d * j
        wait_plane(most + j - 1, at)
        wait_edges(most + j - 1, at)
        mark[at] = jnp.where(counted[far_way] >= (far - j + 1).astype(jnp.float32) - 0.5, 1.0, 0.0)
        take(at)
        apply_once(at + d)

        apply_twice(at + 2 * d)
        return 0

    def other_step(j, _):
        at = near_edge - d * (j - 1)
        toward, away = 1.0 - mark[at + d], jnp.where(j < near, 1.0 - mark[at - d], 0.0)
        here = 1.0 - mark[at]
        degree, scale = weights(toward, here, away)

        def one(k, _):
            def part(keep, index):
                return jnp.where(keep > 0.5, field[k, index], 0.0)

            value = part(here, at)
            value = degree * value - scale * (part(toward, at + d) + part(away, at - d) + two_sided(value))
            spare[k, j - 1] = value[0:lines]
            return 0

        lax.fori_loop(0, vectors, one, 0, unroll=vectors)
        return 0

    def take_own(m, _):
        take(near_edge - d * m)
        return 0

    def inner_once(m, _):
        s = near_edge - d * m

        @pl.when((s > pad) & (s < pad + window - 1))
        def _():
            apply_once(s)
        return 0

    def inner_twice(m, _):
        apply_twice(near_edge - d * m)
        return 0

    def end_gram():
        @pl.when(is_end)
        def _():
            lax.fori_loop(1, 2, near_step, 0)
            lax.fori_loop(1, near + 1, other_step, 0)
            add_gram([lambda g, p=p: spare[:, p, 8 * g : 8 * g + 8, :] for p in range(plan.end_near)], 1)

    ready = min(CHUNKS - 1, plan.end_near // chunk)
    for i in range(CHUNKS):
        drain(field.at[:, 0:chunk, both], own_r.at[i])
        chain_rounds(i)
        lax.fori_loop(i * chunk, (i + 1) * chunk, take_own, 0)
        inner = max(1, i * chunk - 1), (i + 1) * chunk - 1
        lax.fori_loop(*inner, inner_once, 0)
        gram_of([(near_edge - d * m, True) for m in range(*inner)])
        if i == ready:
            for way, total in ((near_way, near), (far_way, far)):
                @pl.when(total > 0)
                def _():
                    drain(counted.at[way, 0 : lines + 2 * REACH], cnt_r.at[0 if way is near_way else 1])
            end_gram()

            @pl.when(is_end)
            def _():
                arrive(2)

    @pl.when(jnp.logical_not(is_end))
    def _():
        lax.fori_loop(1, near + 1, near_step, 0)
        gram_of([(near_edge + d * (j - 1), j <= near) for j in range(1, most + 1)])

    lax.fori_loop(1, far + 1, far_step, 0)
    gram_of([(near_edge, is_end)] + [(far_edge - d * (j - 1), j <= far) for j in range(1, plan.most_far + 1)])

    lane_of = functools.partial(lax.broadcasted_iota, jnp.int32)
    ones = jnp.where(lax.div(lane_of((width, width), 0), 8) == lax.div(lane_of((width, width), 1), 8), 1.0, 0.0)
    pick = lane_of((8, width), 0) == lax.rem(lane_of((8, width), 1), 8)
    shape = (vectors, 8, width)
    diagonal = lane_of(shape, 1) == lax.rem(lane_of(shape, 2), 8)
    rows = []
    for which in range(2):
        total = acc[which, 0] + (acc[which, 1] + acc[which, 1].T)
        rows.append(jnp.sum(jnp.where(diagonal, total.reshape(shape), 0.0), axis=1))
    folded = jnp.dot(jnp.concatenate(rows, axis=0), ones, precision=lax.Precision.HIGHEST,
                     preferred_element_type=jnp.float32)
    parts = vectors // 8
    terms = [jnp.sum(jnp.where(pick, folded[8 * h : 8 * h + 8], 0.0), axis=0, keepdims=True) for h in range(2 * parts)]
    for h in range(parts):
        packed[h : h + 1, :] = jnp.where(side == 0, terms[h], terms[parts + h])
        packed[parts + h : parts + h + 1, :] = jnp.where(side == 0, terms[parts + h], terms[h])
    count_rows = 2 * parts
    body = packed.at[0:count_rows]
    chips = chain // 2 * lanes
    slot_of = lax.div(c, 2) * lanes + l
    leads = jnp.logical_not(is_end) & (partner_end | (lax.rem(c, 2) == 0))
    hand_over = remote(body, handed.at[0:count_rows], hand_s.at[0], hand_r.at[0], (partner, l))

    def broadcast(dc, dl):
        return remote(got.at[slot_of, 0:count_rows], got.at[slot_of, 0:count_rows], gram_s.at[0], gram_r.at[0],
                      (lax.rem(c + dc, chain), lax.rem(l + dl, lanes)))

    @pl.when(jnp.logical_not(leads))
    def _():
        hand_over.start()

    @pl.when(leads)
    def _():
        chain_rounds(3)
        hand_over.wait_recv()
        got[slot_of, 0:count_rows] = packed[0:count_rows] + handed[0:count_rows]
        for dc in range(chain):
            for dl in range(lanes):
                if dc or dl:
                    broadcast(dc, dl).start()

    @pl.when(is_end)
    def _():
        arrive(3)

    lax.fori_loop(2, planes - 2, inner_twice, 0)

    @pl.when(is_end)
    def _():
        lax.fori_loop(2, 3, near_use, 0)
        lax.fori_loop(4, near, near_step, 0)

    def many(total):
        return remote(got.at[0:total, 0:count_rows], got.at[0:total, 0:count_rows], gram_s.at[0], gram_r.at[0], (c, l))

    @pl.when(leads)
    def _():
        many(chips - 1).wait_recv()

    @pl.when(jnp.logical_not(leads))
    def _():
        chain_rounds(3)
        many(chips).wait_recv()

    def sum_one(i, total):
        return total + got[i, 0:count_rows]

    total = lax.fori_loop(1, chips, sum_one, got[0, 0:count_rows], unroll=True)
    tall_shape = (vectors, width)
    inside = lax.div(lane_of(tall_shape, 1), 8) == lane_of(tall_shape, 0)
    choose = jnp.where(
        lax.rem(lane_of((width, width), 0), 8) == lax.rem(lane_of((width, width), 1), 8), 1.0, 0.0)
    for place in range(2):
        result = jnp.zeros(tall_shape, jnp.float32)
        for h in range(vectors // 8):
            i = place * (vectors // 8) + h
            spread = jnp.where(inside, jnp.broadcast_to(total[i : i + 1], tall_shape), 0.0)
            spread = jnp.dot(spread, choose, precision=lax.Precision.HIGHEST, preferred_element_type=jnp.float32)
            result = jnp.where(lax.div(lane_of(tall_shape, 1), 8) == h, spread, result)
        gram[place] = result[:, 0:vectors] / scale_of

    @pl.when(leads)
    def _():
        sent = got.at[0 : chain * lanes - 1, 0:count_rows]
        remote(sent, sent, gram_s.at[0], gram_r.at[0], (c, l)).wait_send()

    @pl.when(jnp.logical_not(leads))
    def _():
        hand_over.wait_send()

    flush(field.at[:, 0:planes, both], own_s.at[0])
    flush(label.at[:, both], lab_s.at[0])

    @pl.when(is_end)
    def _():
        flush(field.at[:, 0 : plan.end_near - 3, both], pass_s.at[0])
        last_use()

    for way, total, across in sends:
        @pl.when(total > 0)
        def _():
            flush(counted.at[way, 0 : lines + 2 * REACH], cnt_s.at[way])

        @pl.when(across)
        def _():
            flush(field.at[:, 0:3, both], corner_s.at[way])

        for t in plan.totals:
            @pl.when(total == t)
            def _():
                flush(field.at[:, 0:t, 0:lines], plane_s.at[way])

            @pl.when((total == t) & jnp.logical_not(across))
            def _():
                flush(field.at[:, 0:t, both], corner_s.at[way])


def store_kernel(image, gram, image_out, gram_out, sems):
    part = image.shape[0] // STORES
    copies = [pltpu.make_async_copy(gram, gram_out, sems.at[STORES])]
    for i in range(STORES):
        rows = pl.ds(i * part, part)
        copies.append(pltpu.make_async_copy(image.at[rows], image_out.at[rows], sems.at[i]))
    for copy in copies:
        copy.start()
    for copy in copies:
        copy.wait()


def per_device(fiedler, side_labels):
    chain, lanes = lax.axis_size("chain"), lax.axis_size("lane")
    vectors, planes, lines, width = fiedler.shape
    plan = Plan(chain, lanes, vectors, planes, lines, width)
    slots = plan.band * plan.half * lines * lanes * width
    tall, frames, most = lines + 8, plan.frames, plan.most
    f32, dma, regular = jnp.float32, pltpu.SemaphoreType.DMA, pltpu.SemaphoreType.REGULAR
    anywhere, vmem = pl.BlockSpec(memory_space=pl.ANY), pl.BlockSpec(memory_space=pltpu.VMEM)
    image, gram = pl.pallas_call(
        functools.partial(kernel, plan, float(slots)),
        in_specs=[anywhere, anywhere],
        out_specs=[vmem, vmem],
        out_shape=[
            pltpu.VMEM((vectors, plan.band, lines, width), f32),
            pltpu.VMEM((2, vectors, vectors), f32),
        ],
        scratch_shapes=[
            pltpu.VMEM((vectors, frames, tall, width), f32),
            pltpu.VMEM((vectors, frames, tall, width), f32),
            pltpu.VMEM((vectors, frames, tall, width), f32),
            pltpu.VMEM((frames, tall, width), f32),
            pltpu.VMEM((planes, tall, width), jnp.int32),
            pltpu.VMEM((2, lines, width), f32),
            pltpu.VMEM((2, tall, width), f32),
            pltpu.VMEM((vectors, plan.end_near, lines, width), f32),
            pltpu.VMEM((2, 2, 8 * vectors, 8 * vectors), f32),
            pltpu.VMEM((3, 2, tall, width), f32),
            pltpu.VMEM((8, width), f32),
            pltpu.VMEM((8, width), f32),
            pltpu.VMEM((chain * lanes, 8, width), f32),
            dma((2,)), dma((1,)), dma((1,)), dma((1,)), dma((CHUNKS,)),
            dma((2,)), dma((most + plan.most_far,)), dma((PARTS,)), dma((2,)), dma((most + plan.most_far,)),
            dma((1,)), dma((2,)), dma((2,)), dma((1,)), dma((1,)), dma((1,)), dma((1,)),
            regular((lanes // 2,)), regular((1,)), regular((1,)), regular((plan.rounds,)),
        ],
        compiler_params=pltpu.CompilerParams(
            collective_id=0, has_side_effects=True, vmem_limit_bytes=56 * 1024 * 1024),
        name="laplace",
    )(fiedler, side_labels)
    return pl.pallas_call(
        store_kernel,
        in_specs=[vmem, vmem],
        out_specs=[anywhere, anywhere],
        out_shape=[jax.ShapeDtypeStruct(a.shape, a.dtype) for a in (image, gram)],
        scratch_shapes=[dma((STORES + 1,))],
        compiler_params=pltpu.CompilerParams(vmem_limit_bytes=1024 * 1024),
        name="store",
    )(*(pltpu.with_memory_space_constraint(a, pltpu.VMEM) for a in (image, gram)))


def solution(mesh):
    return jax.shard_map(
        per_device,
        mesh=mesh,
        in_specs=(P(None, "chain", "lane", None), P("chain", "lane", None)),
        out_specs=(P(None, "chain", "lane", None), P()),
        check_vma=False,
    )
```

```python
import functools

import jax
import jax.numpy as jnp
from jax import lax
from jax.experimental import pallas as pl
from jax.experimental.pallas import tpu as pltpu
from jax.sharding import PartitionSpec as P

REACH = 2
CHUNKS = 3
PARTS = 4
DIRECT = 3
STORES = 4
MESH = pl.DeviceIdType.MESH


def two_sided(field):
    return (
        pltpu.roll(field, 1, 0) + pltpu.roll(field, field.shape[0] - 1, 0)
        + pltpu.roll(field, 1, 1) + pltpu.roll(field, field.shape[1] - 1, 1)
    )


class Plan:
    def __init__(self, chain, lanes, vectors, planes, lines, width):
        self.chain, self.lanes, self.vectors, self.planes, self.lines, self.width = (
            chain, lanes, vectors, planes, lines, width)
        self.half = chain // 2
        self.band = planes + planes // 4
        self.grow = self.band - planes
        self.margin = self.grow * self.half // 2
        self.window = self.band + 2 * REACH
        spots = [self.spot(w, max_of=max) for w in range(self.half)]
        self.most = max(max(below, above) for _, below, above in spots)
        assert self.most <= planes and 8 * vectors == width
        assert spots[0][1] == spots[-1][2] > 3 + DIRECT - 1 and spots[0][2] == spots[-1][1] == 0
        self.end_near = spots[0][1]
        self.most_far = max(min(below, above) for _, below, above in spots)
        self.totals = sorted({count for _, below, above in spots for count in (below, above)} - {0})
        self.rounds = chain // 2
        assert self.rounds % 4 == 0 and lanes % 2 == 0 and lanes > 2
        self.chunk = planes // CHUNKS
        assert self.chunk * CHUNKS == planes and self.chunk > 2 and vectors % PARTS == 0
        self.pad = 1 + max(max(0, -slot) for slot, _, _ in spots)
        tail = 1 + max(max(0, slot + planes - self.window) for slot, _, _ in spots)
        self.frames = self.pad + self.window + tail

    def spot(self, w, max_of=jnp.maximum):
        first, last = (w == 0), (w == self.half - 1)
        if not isinstance(w, int):
            first, last = first.astype(jnp.int32), last.astype(jnp.int32)
        slot = self.margin + REACH - self.grow * w
        below = max_of(0, slot - REACH * first)
        above = max_of(0, self.window - REACH * last - slot - self.planes)
        return slot, below, above

    def is_end(self, c):
        within = self.place(c)[1]
        return (within == 0) | (within == self.half - 1)

    def place(self, c):
        relative = lax.rem(c + (self.chain - self.chain // 4), self.chain)
        side = lax.div(relative, self.half)
        within = relative - side * self.half
        return side, within


def kernel(plan, scale_of, fiedler, labels, image, gram, field, moved, once, mark, label, count, counted, spare, acc,
           weight, packed, handed, got, local_sem, lab_s, lab_r, own_s, own_r, plane_s, plane_r, last_r, corner_s, edge_r,
           pass_s, cnt_s, cnt_r, hand_s, hand_r, gram_s, gram_r, lane_told, tell, cross, chain_told):
    chain, lanes, vectors, planes, lines, width = (
        plan.chain, plan.lanes, plan.vectors, plan.planes, plan.lines, plan.width)
    window, pad, most = plan.window, plan.pad, plan.most
    c, l = lax.axis_index("chain"), lax.axis_index("lane")
    up_c, down_c = lax.rem(c + 1, chain), lax.rem(c + chain - 1, chain)
    up_l, down_l = lax.rem(l + 1, lanes), lax.rem(l + lanes - 1, lanes)
    side, within = plan.place(c)
    slot, below, above = plan.spot(within)
    up_side, up_within = plan.place(up_c)
    down_side, down_within = plan.place(down_c)
    up_slot, up_count, _ = plan.spot(up_within)
    down_slot, _, down_count = plan.spot(down_within)
    tall = lines + 8
    lo, hi = slice(0, REACH), slice(lines - REACH, lines)
    nxt, prv = slice(lines, lines + REACH), slice(tall - REACH, tall)

    def remote(src, dst, send, recv, device):
        return pltpu.make_async_remote_copy(
            src_ref=src, dst_ref=dst, send_sem=send, recv_sem=recv, device_id=device, device_id_type=MESH)

    base = pad + slot
    is_end = (within == 0) | (within == plan.half - 1)
    lower = within < plan.half // 2
    d = jnp.where(lower, -1, 1)
    near_way, far_way = jnp.where(lower, 0, 1), jnp.where(lower, 1, 0)
    near, far = jnp.where(lower, below, above), jnp.where(lower, above, below)
    near_edge = jnp.where(lower, base, base + planes - 1)
    far_edge = jnp.where(lower, base + planes - 1, base)

    chunk = plan.chunk
    near_start, far_start = jnp.where(lower, 0, planes - chunk), jnp.where(lower, planes - chunk, 0)
    rest = planes - 2 * chunk
    loads = []
    for i, (start, size) in enumerate((
            (jnp.where(is_end, near_start, far_start), chunk), (jnp.where(is_end, far_start, near_start), chunk),
            (chunk, rest))):
        loads.append(pltpu.make_async_copy(
            fiedler.at[:, pl.ds(start, size)], field.at[:, pl.ds(base + start, size), 0:lines], local_sem.at[i]))
    load_label = pltpu.make_async_copy(labels, label.at[:, 0:lines], local_sem.at[3])
    load_label.start()
    for load in loads:
        load.start()

    barrier = pltpu.get_barrier_semaphore()
    def signal(sem, device):
        pl.semaphore_signal(sem, inc=1, device_id=device, device_id_type=MESH)

    signal(barrier, (up_c, l))
    signal(barrier, (down_c, l))

    @pl.when(jnp.logical_not(is_end))
    def _():
        signal(barrier, (c, up_l))
        signal(barrier, (c, down_l))

    load_label.wait()
    totals = [jnp.zeros((lines, width), jnp.float32) for _ in range(2)]
    for p in range(planes):
        here = label[p, 0:lines]
        totals[0] += jnp.where((here == up_side) & (p >= planes - up_count), 1.0, 0.0)
        totals[1] += jnp.where((here == down_side) & (p < down_count), 1.0, 0.0)
    for way in range(2):
        count[way] = totals[way]

    @pl.when(is_end)
    def _():
        pl.semaphore_wait(barrier, 2)

    @pl.when(jnp.logical_not(is_end))
    def _():
        pl.semaphore_wait(barrier, 4)
        signal(lane_told.at[0], (c, up_l))
        signal(lane_told.at[0], (c, down_l))

    lab_copies = [
        remote(label.at[:, lo], label.at[:, nxt], lab_s.at[0], lab_r.at[0], (c, down_l)),
        remote(label.at[:, hi], label.at[:, prv], lab_s.at[0], lab_r.at[0], (c, up_l)),
    ]
    def own_copies(i):
        start = jnp.where(lower, i * chunk, planes - (i + 1) * chunk)
        at = pl.ds(base + start, chunk)
        return [
            remote(field.at[:, at, lo], field.at[:, at, nxt], own_s.at[0], own_r.at[i], (c, down_l)),
            remote(field.at[:, at, hi], field.at[:, at, prv], own_s.at[0], own_r.at[i], (c, up_l)),
        ]

    sends = ((0, up_count, up_side != side), (1, down_count, down_side != side))
    up_near, down_near = up_within < plan.half // 2, down_within >= plan.half // 2
    first_sem = (jnp.where(up_near, 0, most), jnp.where(down_near, 0, most))
    count_sem = (jnp.where(up_near, 0, 1), jnp.where(down_near, 0, 1))

    def spot_of(way, j):
        if way == 0:
            return base + planes - j, pad + up_slot - j, up_c
        return base + j - 1, pad + down_slot + planes - 1 + j, down_c

    def plane_copy(way, j):
        source, at, to = spot_of(way, j)
        return remote(
            field.at[:, source, 0:lines], field.at[:, at, 0:lines], plane_s.at[way],
            plane_r.at[first_sem[way] + j - 1], (to, l))

    def part_copies(way, j):
        source, at, to = spot_of(way, j)
        share = vectors // PARTS
        return [
            remote(field.at[i * share : (i + 1) * share, source, 0:lines],
                   field.at[i * share : (i + 1) * share, at, 0:lines], plane_s.at[way], last_r.at[i], (to, l))
            for i in range(PARTS)
        ]

    def corner_copies(way, j):
        source, at, to = spot_of(way, j)
        return [
            remote(field.at[:, source, lo], field.at[:, at, nxt], corner_s.at[way],
                   edge_r.at[first_sem[way] + j - 1], (to, down_l)),
            remote(field.at[:, source, hi], field.at[:, at, prv], corner_s.at[way],
                   edge_r.at[first_sem[way] + j - 1], (to, up_l)),
        ]

    def passed_on(j, total):
        return j <= total - DIRECT

    def pass_along(ref, send, recv):
        remote(ref(lo), ref(nxt), send, recv, (c, down_l)).start()
        remote(ref(hi), ref(prv), send, recv, (c, up_l)).start()

    def pass_plane(index, at):
        pass_along(lambda rows: field.at[:, at, rows], pass_s.at[0], edge_r.at[index])

    def send_plane(j, only=(True, True)):
        for way, total, across in sends:
            @pl.when(((j < total) | ((j == total) & jnp.logical_not(across))) & only[way])
            def _():
                plane_copy(way, j).start()

            @pl.when((j == total) & across & only[way])
            def _():
                for copy in part_copies(way, j):
                    copy.start()

    def send_corners(j):
        for way, total, across in sends:
            target_near = (up_near, down_near)[way]

            direct = jnp.where(target_near, jnp.logical_not(across & passed_on(j, total)), j == total)

            @pl.when((j <= total) & direct)
            def _():
                for copy in corner_copies(way, j):
                    copy.start()

    def start_counts(only):
        for way, total, _ in sends:
            @pl.when((total > 0) & only[way])
            def _():
                remote(count.at[way], counted.at[way, 0:lines], cnt_s.at[way], cnt_r.at[count_sem[way]],
                       ((up_c, down_c)[way], l)).start()

    def drain(ref, recv):
        remote(ref, ref, lab_s.at[0], recv, (c, l)).wait_recv()

    def flush(ref, send):
        remote(ref, ref, send, lab_r.at[0], (c, l)).wait_send()

    both = slice(0, 2 * REACH)
    incoming = ((near_way, near, 0), (far_way, far, 1))
    partner = c + 1 - 2 * lax.rem(c, 2)
    partner_end = plan.is_end(partner)
    cross_c = lax.rem(c + d + chain, chain)

    def start_chunk(i):
        for copy in own_copies(i):
            copy.start()

    def start_lanes():
        for copy in lab_copies:
            copy.start()
        start_chunk(0)

    def pass_counts():
        for way, total, index in incoming:
            @pl.when(total > 0)
            def _():
                drain(counted.at[way, 0:lines], cnt_r.at[index])
                pass_along(lambda rows: counted.at[way, rows], cnt_s.at[2 + index], cnt_r.at[2 + index])

    down_first = lower == is_end
    ahead = min(chunk, most - DIRECT)
    for load, only in zip(loads, ((jnp.logical_not(down_first), down_first), (down_first, jnp.logical_not(down_first)))):
        load.wait()
        start_counts(only)
        for j in range(1, ahead + 1):
            send_plane(j, only)
    loads[2].wait()
    for j in range(ahead + 1, most - DIRECT + 1):
        send_plane(j)

    @pl.when(is_end)
    def _():
        pl.semaphore_wait(tell.at[0], 1)
        signal(cross.at[0], (cross_c, l))
        start_lanes()
        pl.semaphore_wait(cross.at[0], 1)
        pass_counts()
        start_chunk(1)

    @pl.when(jnp.logical_not(is_end))
    def _():
        start_lanes()
        pl.semaphore_wait(lane_told.at[0], 2)

        @pl.when(partner_end)
        def _():
            signal(tell.at[0], (partner, l))

        signal(lane_told.at[1], (c, up_l))
        signal(lane_told.at[1], (c, down_l))
        pass_counts()
        start_chunk(1)

    def send_rest():
        for j in range(1, most + 1):
            send_corners(j)
            if j > most - DIRECT:
                send_plane(j)

    @pl.when(jnp.logical_not(is_end))
    def _():
        for r in range(1, lanes // 2):
            pl.semaphore_wait(lane_told.at[r], 2)
            if r + 1 < lanes // 2:
                signal(lane_told.at[r + 1], (c, up_l))
                signal(lane_told.at[r + 1], (c, down_l))

    def tell_chain(r):
        signal(chain_told.at[r], (up_c, l))
        signal(chain_told.at[r], (down_c, l))

    def chain_rounds(point):
        each = plan.rounds // 4
        for r in range(point * each, (point + 1) * each):
            pl.semaphore_wait(chain_told.at[r], 2)
            if r + 1 < plan.rounds:
                tell_chain(r + 1)

    tell_chain(0)

    drain(label.at[:, both], lab_r.at[0])
    acc[...] = jnp.zeros(acc.shape, jnp.float32)
    for p in range(planes):
        mark[base + p] = jnp.where(label[p] == side, 1.0, 0.0)

    @pl.when(is_end)
    def _():
        mark[near_edge + d * (near + 1)] = jnp.zeros((tall, width), jnp.float32)

    def take(at):
        keep = mark[at] > 0.5

        def one(k, _):
            moved[k, at] = jnp.where(keep, field[k, at], 0.0)
            return 0

        lax.fori_loop(0, vectors, one, 0, unroll=vectors)

    def weights(before, here, after):
        scale = here * jnp.float32(1.0 / 6.0)
        return scale * (before + after + two_sided(here)), scale

    def apply_once(s):
        degree, scale = weights(mark[s - 1], mark[s], mark[s + 1])

        def one(k, _):
            here = moved[k, s]
            once[k, s] = degree * here - scale * (moved[k, s - 1] + moved[k, s + 1] + two_sided(here))
            return 0

        lax.fori_loop(0, vectors, one, 0, unroll=vectors)

    def apply_twice(s):
        degree, scale = weights(mark[s - 1], mark[s], mark[s + 1])

        def one(k, _):
            here = once[k, s]
            value = degree * here - scale * (once[k, s - 1] + once[k, s + 1] + two_sided(here))
            image[k, s - pad - REACH] = value[0:lines]
            return 0

        @pl.when(in_band(s))
        def _():
            lax.fori_loop(0, vectors, one, 0, unroll=vectors)

    def add_gram(reads, which):
        block = jnp.concatenate(
            [read(g).reshape(8 * vectors, width) for read in reads for g in range(lines // 8)], axis=1)
        high = block.astype(jnp.bfloat16)
        low = (block - high.astype(jnp.float32)).astype(jnp.bfloat16)
        dot = functools.partial(
            lax.dot_general, dimension_numbers=(((1,), (1,)), ((), ())), preferred_element_type=jnp.float32)
        acc[which, 0] += dot(high, high)
        acc[which, 1] += dot(high, low)

    def gram_of(spots):
        def reader(s, counts):
            def read(g):
                return jnp.where(counts & in_band(s), once[:, s, 8 * g : 8 * g + 8, :], 0.0)

            return read

        add_gram([reader(s, counts) for s, counts in spots], 0)

    def in_band(s):
        return (s >= pad + REACH) & (s < pad + window - REACH)

    def wait_plane(index, at):
        drain(field.at[:, at, 0:lines], plane_r.at[index])

    def wait_edges(index, at):
        drain(field.at[:, at, both], edge_r.at[index])

    def near_mark(j):
        at = near_edge + d * j
        wait_edges(j - 1, at)
        mark[at] = jnp.where(counted[near_way] >= (j + 0.0) - 0.5, 1.0, 0.0)

    def near_use(j, _):
        at = near_edge + d * j
        near_mark(j)
        take(at)
        apply_once(at - d)
        apply_twice(at - 2 * d)
        return 0

    def last_use():
        at = near_edge + d * near
        near_mark(near)
        for i in range(3):
            s = at - d * i
            degree, scale = weights(mark[s - 1], mark[s], mark[s + 1])
            weight[i, 0], weight[i, 1] = degree, scale

        def step(i, here, beside):
            return weight[i, 0] * here - weight[i, 1] * (beside + two_sided(here))

        def one(k, _):
            moved_0 = jnp.where(mark[at] > 0.5, field[k, at], 0.0)
            moved_1 = moved[k, at - d]
            once_0 = step(0, moved_0, moved_1)
            once_1 = step(1, moved_1, moved_0 + moved[k, at - 2 * d])
            once_2 = once[k, at - 2 * d]
            values = (
                step(0, once_0, once_1), step(1, once_1, once_0 + once_2),
                step(2, once_2, once_1 + once[k, at - 3 * d]))
            for i in range(3):
                image[k, at - d * i - pad - REACH] = values[i][0:lines]
            return 0

        share = vectors // PARTS
        for i in range(PARTS):
            drain(field.at[i * share : (i + 1) * share, at, 0:lines], last_r.at[i])
            lax.fori_loop(i * share, (i + 1) * share, one, 0, unroll=share)

    def arrive(j):
        wait_plane(j - 1, near_edge + d * j)

        @pl.when(is_end & passed_on(j, near))
        def _():
            pass_plane(j - 1, near_edge + d * j)

    def near_use_now(j):
        lax.fori_loop(j, j + 1, near_use, 0)

    def near_step(j, _):
        wait_plane(j - 1, near_edge + d * j)
        near_use(j, 0)
        return 0

    def far_step(j, _):
        at = far_edge - d * j
        @pl.when(j == far)
        def _():
            wait_plane(most + j - 1, at)

        wait_edges(most + j - 1, at)
        mark[at] = jnp.where(counted[far_way] >= (far - j + 1).astype(jnp.float32) - 0.5, 1.0, 0.0)
        take(at)
        apply_once(at + d)

        apply_twice(at + 2 * d)
        return 0

    def other_step(j, _):
        at = near_edge - d * (j - 1)
        toward, away = 1.0 - mark[at + d], jnp.where(j < near, 1.0 - mark[at - d], 0.0)
        here = 1.0 - mark[at]
        degree, scale = weights(toward, here, away)

        def one(k, _):
            def part(keep, index):
                return jnp.where(keep > 0.5, field[k, index], 0.0)

            value = part(here, at)
            value = degree * value - scale * (part(toward, at + d) + part(away, at - d) + two_sided(value))
            spare[k, j - 1] = value[0:lines]
            return 0

        lax.fori_loop(0, vectors, one, 0, unroll=vectors)
        return 0

    def take_own(m, _):
        take(near_edge - d * m)
        return 0

    def inner_once(m, _):
        s = near_edge - d * m

        @pl.when((s > pad) & (s < pad + window - 1))
        def _():
            apply_once(s)
        return 0

    def inner_twice(m, _):
        apply_twice(near_edge - d * m)
        return 0

    def end_gram():
        @pl.when(is_end)
        def _():
            near_use_now(1)
            lax.fori_loop(1, near + 1, other_step, 0)
            add_gram([lambda g, p=p: spare[:, p, 8 * g : 8 * g + 8, :] for p in range(plan.end_near)], 1)

    ready = min(CHUNKS - 1, plan.end_near // chunk)
    for i in range(CHUNKS):
        drain(field.at[:, 0:chunk, both], own_r.at[i])
        chain_rounds(i)
        if i == 0:
            @pl.when(is_end)
            def _():
                arrive(1)

            for more in range(2, CHUNKS):
                start_chunk(more)
            send_rest()
        lax.fori_loop(i * chunk, (i + 1) * chunk, take_own, 0)
        inner = max(1, i * chunk - 1), (i + 1) * chunk - 1
        lax.fori_loop(*inner, inner_once, 0)
        gram_of([(near_edge - d * m, True) for m in range(*inner)])
        if i == ready:
            for way, total, index in incoming:
                @pl.when(total > 0)
                def _():
                    drain(counted.at[way, both], cnt_r.at[2 + index])
            end_gram()

            @pl.when(is_end)
            def _():
                arrive(2)

    @pl.when(jnp.logical_not(is_end))
    def _():
        def far_arrive(j, _):
            at = far_edge - d * j
            wait_plane(most + j - 1, at)
            pass_plane(most + j - 1, at)
            return 0

        lax.fori_loop(1, far, far_arrive, 0)
        lax.fori_loop(1, near + 1, near_step, 0)
        gram_of([(near_edge + d * (j - 1), j <= near) for j in range(1, most + 1)])

    lax.fori_loop(1, far + 1, far_step, 0)
    gram_of([(near_edge, is_end)] + [(far_edge - d * (j - 1), j <= far) for j in range(1, plan.most_far + 1)])

    lane_of = functools.partial(lax.broadcasted_iota, jnp.int32)
    ones = jnp.where(lax.div(lane_of((width, width), 0), 8) == lax.div(lane_of((width, width), 1), 8), 1.0, 0.0)
    pick = lane_of((8, width), 0) == lax.rem(lane_of((8, width), 1), 8)
    shape = (vectors, 8, width)
    diagonal = lane_of(shape, 1) == lax.rem(lane_of(shape, 2), 8)
    rows = []
    for which in range(2):
        total = acc[which, 0] + (acc[which, 1] + acc[which, 1].T)
        rows.append(jnp.sum(jnp.where(diagonal, total.reshape(shape), 0.0), axis=1))
    folded = jnp.dot(jnp.concatenate(rows, axis=0), ones, precision=lax.Precision.HIGHEST,
                     preferred_element_type=jnp.float32)
    parts = vectors // 8
    terms = [jnp.sum(jnp.where(pick, folded[8 * h : 8 * h + 8], 0.0), axis=0, keepdims=True) for h in range(2 * parts)]
    for h in range(parts):
        packed[h : h + 1, :] = jnp.where(side == 0, terms[h], terms[parts + h])
        packed[parts + h : parts + h + 1, :] = jnp.where(side == 0, terms[parts + h], terms[h])
    count_rows = 2 * parts
    body = packed.at[0:count_rows]
    chips = chain // 2 * lanes
    slot_of = lax.div(c, 2) * lanes + l
    leads = jnp.logical_not(is_end) & (partner_end | (lax.rem(c, 2) == 0))
    hand_over = remote(body, handed.at[0:count_rows], hand_s.at[0], hand_r.at[0], (partner, l))

    def broadcast(dc, dl):
        return remote(got.at[slot_of, 0:count_rows], got.at[slot_of, 0:count_rows], gram_s.at[0], gram_r.at[0],
                      (lax.rem(c + dc, chain), lax.rem(l + dl, lanes)))

    @pl.when(jnp.logical_not(leads))
    def _():
        hand_over.start()

    @pl.when(leads)
    def _():
        chain_rounds(3)
        hand_over.wait_recv()
        got[slot_of, 0:count_rows] = packed[0:count_rows] + handed[0:count_rows]
        for dc in range(chain):
            for dl in range(lanes):
                if dc or dl:
                    broadcast(dc, dl).start()

    @pl.when(is_end)
    def _():
        arrive(3)

    lax.fori_loop(2, planes - 2, inner_twice, 0)

    @pl.when(is_end)
    def _():
        for j in range(4, plan.end_near - DIRECT + 1):
            arrive(j)
        lax.fori_loop(2, near - DIRECT + 1, near_use, 0)
        lax.fori_loop(near - DIRECT + 1, near, near_step, 0)

    @pl.when(is_end)
    def _():
        last_use()

    def many(total):
        return remote(got.at[0:total, 0:count_rows], got.at[0:total, 0:count_rows], gram_s.at[0], gram_r.at[0], (c, l))

    @pl.when(leads)
    def _():
        many(chips - 1).wait_recv()

    @pl.when(jnp.logical_not(leads))
    def _():
        chain_rounds(3)
        many(chips).wait_recv()

    def sum_one(i, total):
        return total + got[i, 0:count_rows]

    total = lax.fori_loop(1, chips, sum_one, got[0, 0:count_rows], unroll=True)
    tall_shape = (vectors, width)
    inside = lax.div(lane_of(tall_shape, 1), 8) == lane_of(tall_shape, 0)
    choose = jnp.where(
        lax.rem(lane_of((width, width), 0), 8) == lax.rem(lane_of((width, width), 1), 8), 1.0, 0.0)
    for place in range(2):
        result = jnp.zeros(tall_shape, jnp.float32)
        for h in range(vectors // 8):
            i = place * (vectors // 8) + h
            spread = jnp.where(inside, jnp.broadcast_to(total[i : i + 1], tall_shape), 0.0)
            spread = jnp.dot(spread, choose, precision=lax.Precision.HIGHEST, preferred_element_type=jnp.float32)
            result = jnp.where(lax.div(lane_of(tall_shape, 1), 8) == h, spread, result)
        gram[place] = result[:, 0:vectors] / scale_of

    @pl.when(leads)
    def _():
        sent = got.at[0 : chain * lanes - 1, 0:count_rows]
        remote(sent, sent, gram_s.at[0], gram_r.at[0], (c, l)).wait_send()

    @pl.when(jnp.logical_not(leads))
    def _():
        hand_over.wait_send()

    flush(field.at[:, 0:planes, both], own_s.at[0])
    flush(label.at[:, both], lab_s.at[0])

    @pl.when(is_end)
    def _():
        flush(field.at[:, 0 : plan.end_near - DIRECT, both], pass_s.at[0])

    for index, total in enumerate((near, far)):
        @pl.when(total > 0)
        def _():
            flush(counted.at[0, both], cnt_s.at[2 + index])

    for t in range(1, plan.most_far):
        @pl.when(far == t + 1)
        def _():
            flush(field.at[:, 0:t, both], pass_s.at[0])

    for way, total, across in sends:
        target_near = (up_near, down_near)[way]

        @pl.when(total > 0)
        def _():
            flush(counted.at[way, 0:lines], cnt_s.at[way])

        @pl.when(across)
        def _():
            flush(field.at[:, 0:DIRECT, both], corner_s.at[way])

        @pl.when((total > 0) & jnp.logical_not(target_near))
        def _():
            flush(field.at[:, 0:1, both], corner_s.at[way])

        for t in plan.totals:
            @pl.when(total == t)
            def _():
                flush(field.at[:, 0:t, 0:lines], plane_s.at[way])

            @pl.when((total == t) & target_near & jnp.logical_not(across))
            def _():
                flush(field.at[:, 0:t, both], corner_s.at[way])


def store_kernel(image, gram, image_out, gram_out, sems):
    part = image.shape[0] // STORES
    copies = [pltpu.make_async_copy(gram, gram_out, sems.at[STORES])]
    for i in range(STORES):
        rows = pl.ds(i * part, part)
        copies.append(pltpu.make_async_copy(image.at[rows], image_out.at[rows], sems.at[i]))
    for copy in copies:
        copy.start()
    for copy in copies:
        copy.wait()


def per_device(fiedler, side_labels):
    chain, lanes = lax.axis_size("chain"), lax.axis_size("lane")
    vectors, planes, lines, width = fiedler.shape
    plan = Plan(chain, lanes, vectors, planes, lines, width)
    slots = plan.band * plan.half * lines * lanes * width
    tall, frames, most = lines + 8, plan.frames, plan.most
    f32, dma, regular = jnp.float32, pltpu.SemaphoreType.DMA, pltpu.SemaphoreType.REGULAR
    anywhere, vmem = pl.BlockSpec(memory_space=pl.ANY), pl.BlockSpec(memory_space=pltpu.VMEM)
    image, gram = pl.pallas_call(
        functools.partial(kernel, plan, float(slots)),
        in_specs=[anywhere, anywhere],
        out_specs=[vmem, vmem],
        out_shape=[
            pltpu.VMEM((vectors, plan.band, lines, width), f32),
            pltpu.VMEM((2, vectors, vectors), f32),
        ],
        scratch_shapes=[
            pltpu.VMEM((vectors, frames, tall, width), f32),
            pltpu.VMEM((vectors, frames, tall, width), f32),
            pltpu.VMEM((vectors, frames, tall, width), f32),
            pltpu.VMEM((frames, tall, width), f32),
            pltpu.VMEM((planes, tall, width), jnp.int32),
            pltpu.VMEM((2, lines, width), f32),
            pltpu.VMEM((2, tall, width), f32),
            pltpu.VMEM((vectors, plan.end_near, lines, width), f32),
            pltpu.VMEM((2, 2, 8 * vectors, 8 * vectors), f32),
            pltpu.VMEM((3, 2, tall, width), f32),
            pltpu.VMEM((8, width), f32),
            pltpu.VMEM((8, width), f32),
            pltpu.VMEM((chain * lanes, 8, width), f32),
            dma((4,)), dma((1,)), dma((1,)), dma((1,)), dma((CHUNKS,)),
            dma((2,)), dma((most + plan.most_far,)), dma((PARTS,)), dma((2,)), dma((most + plan.most_far,)),
            dma((1,)), dma((4,)), dma((4,)), dma((1,)), dma((1,)), dma((1,)), dma((1,)),
            regular((lanes // 2,)), regular((1,)), regular((1,)), regular((plan.rounds,)),
        ],
        compiler_params=pltpu.CompilerParams(
            collective_id=0, has_side_effects=True, vmem_limit_bytes=56 * 1024 * 1024),
        name="laplace",
    )(fiedler, side_labels)
    return pl.pallas_call(
        store_kernel,
        in_specs=[vmem, vmem],
        out_specs=[anywhere, anywhere],
        out_shape=[jax.ShapeDtypeStruct(a.shape, a.dtype) for a in (image, gram)],
        scratch_shapes=[dma((STORES + 1,))],
        compiler_params=pltpu.CompilerParams(vmem_limit_bytes=1024 * 1024),
        name="store",
    )(*(pltpu.with_memory_space_constraint(a, pltpu.VMEM) for a in (image, gram)))


def solution(mesh):
    return jax.shard_map(
        per_device,
        mesh=mesh,
        in_specs=(P(None, "chain", "lane", None), P("chain", "lane", None)),
        out_specs=(P(None, "chain", "lane", None), P()),
        check_vma=False,
    )
```

```python
import functools

import jax
import jax.numpy as jnp
from jax import lax
from jax.experimental import pallas as pl
from jax.experimental.pallas import tpu as pltpu
from jax.sharding import PartitionSpec as P

REACH = 2
CHUNKS = 3
PARTS = 4
DIRECT = 3
EARLY = 4
STORES = 4
MESH = pl.DeviceIdType.MESH


def two_sided(field):
    return (
        pltpu.roll(field, 1, 0) + pltpu.roll(field, field.shape[0] - 1, 0)
        + pltpu.roll(field, 1, 1) + pltpu.roll(field, field.shape[1] - 1, 1)
    )


class Plan:
    def __init__(self, chain, lanes, vectors, planes, lines, width):
        self.chain, self.lanes, self.vectors, self.planes, self.lines, self.width = (
            chain, lanes, vectors, planes, lines, width)
        self.half = chain // 2
        self.band = planes + planes // 4
        self.grow = self.band - planes
        self.margin = self.grow * self.half // 2
        self.window = self.band + 2 * REACH
        spots = [self.spot(w, max_of=max) for w in range(self.half)]
        self.most = max(max(below, above) for _, below, above in spots)
        assert self.most <= planes and 8 * vectors == width and spots[0][1] == self.most
        assert spots[0][1] == spots[-1][2] > 3 + DIRECT - 1 and spots[0][2] == spots[-1][1] == 0
        self.end_near = spots[0][1]
        self.most_far = max(min(below, above) for _, below, above in spots)
        self.totals = sorted({count for _, below, above in spots for count in (below, above)} - {0})
        self.rounds = chain // 2
        assert self.rounds % 4 == 0 and lanes % 2 == 0 and lanes > 2
        self.chunk = planes // CHUNKS
        assert self.chunk * CHUNKS == planes and self.chunk > 2 and vectors % PARTS == 0
        self.pad = 1 + max(max(0, -slot) for slot, _, _ in spots)
        tail = 1 + max(max(0, slot + planes - self.window) for slot, _, _ in spots)
        self.frames = self.pad + self.window + tail

    def spot(self, w, max_of=jnp.maximum):
        first, last = (w == 0), (w == self.half - 1)
        if not isinstance(w, int):
            first, last = first.astype(jnp.int32), last.astype(jnp.int32)
        slot = self.margin + REACH - self.grow * w
        below = max_of(0, slot - REACH * first)
        above = max_of(0, self.window - REACH * last - slot - self.planes)
        return slot, below, above

    def is_end(self, c):
        within = self.place(c)[1]
        return (within == 0) | (within == self.half - 1)

    def place(self, c):
        relative = lax.rem(c + (self.chain - self.chain // 4), self.chain)
        side = lax.div(relative, self.half)
        within = relative - side * self.half
        return side, within


def kernel(plan, scale_of, fiedler, labels, image, gram, field, moved, once, mark, label, count, counted, spare, acc,
           weight, packed, handed, got, local_sem, lab_s, lab_r, own_s, own_r, plane_s, plane_r, last_r, corner_s, edge_r,
           pass_s, cnt_s, cnt_r, hand_s, hand_r, gram_s, gram_r, lane_told, tell, cross, chain_told):
    chain, lanes, vectors, planes, lines, width = (
        plan.chain, plan.lanes, plan.vectors, plan.planes, plan.lines, plan.width)
    window, pad, most = plan.window, plan.pad, plan.most
    c, l = lax.axis_index("chain"), lax.axis_index("lane")
    up_c, down_c = lax.rem(c + 1, chain), lax.rem(c + chain - 1, chain)
    up_l, down_l = lax.rem(l + 1, lanes), lax.rem(l + lanes - 1, lanes)
    side, within = plan.place(c)
    slot, below, above = plan.spot(within)
    up_side, up_within = plan.place(up_c)
    down_side, down_within = plan.place(down_c)
    up_slot, up_count, _ = plan.spot(up_within)
    down_slot, _, down_count = plan.spot(down_within)
    tall = lines + 8
    lo, hi = slice(0, REACH), slice(lines - REACH, lines)
    nxt, prv = slice(lines, lines + REACH), slice(tall - REACH, tall)

    def remote(src, dst, send, recv, device):
        return pltpu.make_async_remote_copy(
            src_ref=src, dst_ref=dst, send_sem=send, recv_sem=recv, device_id=device, device_id_type=MESH)

    base = pad + slot
    is_end = (within == 0) | (within == plan.half - 1)
    lower = within < plan.half // 2
    d = jnp.where(lower, -1, 1)
    near_way, far_way = jnp.where(lower, 0, 1), jnp.where(lower, 1, 0)
    near, far = jnp.where(lower, below, above), jnp.where(lower, above, below)
    near_edge = jnp.where(lower, base, base + planes - 1)
    far_edge = jnp.where(lower, base + planes - 1, base)

    chunk = plan.chunk
    near_start, far_start = jnp.where(lower, 0, planes - chunk), jnp.where(lower, planes - chunk, 0)
    rest = planes - 2 * chunk
    loads = []
    for i, (start, size) in enumerate((
            (jnp.where(is_end, near_start, far_start), chunk), (jnp.where(is_end, far_start, near_start), chunk),
            (chunk, rest))):
        loads.append(pltpu.make_async_copy(
            fiedler.at[:, pl.ds(start, size)], field.at[:, pl.ds(base + start, size), 0:lines], local_sem.at[i]))
    load_label = pltpu.make_async_copy(labels, label.at[:, 0:lines], local_sem.at[3])
    load_label.start()
    for load in loads:
        load.start()

    barrier = pltpu.get_barrier_semaphore()
    def signal(sem, device):
        pl.semaphore_signal(sem, inc=1, device_id=device, device_id_type=MESH)

    signal(barrier, (up_c, l))
    signal(barrier, (down_c, l))

    @pl.when(jnp.logical_not(is_end))
    def _():
        signal(barrier, (c, up_l))
        signal(barrier, (c, down_l))

    load_label.wait()
    totals = [jnp.zeros((lines, width), jnp.float32) for _ in range(2)]
    for p in range(planes):
        here = label[p, 0:lines]
        totals[0] += jnp.where((here == up_side) & (p >= planes - up_count), 1.0, 0.0)
        totals[1] += jnp.where((here == down_side) & (p < down_count), 1.0, 0.0)
    for way in range(2):
        count[way] = totals[way]

    @pl.when(is_end)
    def _():
        pl.semaphore_wait(barrier, 2)

    @pl.when(jnp.logical_not(is_end))
    def _():
        pl.semaphore_wait(barrier, 4)
        signal(lane_told.at[0], (c, up_l))
        signal(lane_told.at[0], (c, down_l))

    lab_copies = [
        remote(label.at[:, lo], label.at[:, nxt], lab_s.at[0], lab_r.at[0], (c, down_l)),
        remote(label.at[:, hi], label.at[:, prv], lab_s.at[0], lab_r.at[0], (c, up_l)),
    ]
    def own_copies(i):
        start = jnp.where(lower, i * chunk, planes - (i + 1) * chunk)
        at = pl.ds(base + start, chunk)
        return [
            remote(field.at[:, at, lo], field.at[:, at, nxt], own_s.at[0], own_r.at[i], (c, down_l)),
            remote(field.at[:, at, hi], field.at[:, at, prv], own_s.at[0], own_r.at[i], (c, up_l)),
        ]

    sends = ((0, up_count, up_side != side), (1, down_count, down_side != side))
    up_near, down_near = up_within < plan.half // 2, down_within >= plan.half // 2
    first_sem = (jnp.where(up_near, 0, most), jnp.where(down_near, 0, most))
    count_sem = (jnp.where(up_near, 0, 1), jnp.where(down_near, 0, 1))

    def spot_of(way, j):
        if way == 0:
            return base + planes - j, pad + up_slot - j, up_c
        return base + j - 1, pad + down_slot + planes - 1 + j, down_c

    def plane_copy(way, j):
        source, at, to = spot_of(way, j)
        return remote(
            field.at[:, source, 0:lines], field.at[:, at, 0:lines], plane_s.at[way],
            plane_r.at[first_sem[way] + j - 1], (to, l))

    def part_copies(way, j):
        source, at, to = spot_of(way, j)
        share = vectors // PARTS
        return [
            remote(field.at[i * share : (i + 1) * share, source, 0:lines],
                   field.at[i * share : (i + 1) * share, at, 0:lines], plane_s.at[way], last_r.at[i], (to, l))
            for i in range(PARTS)
        ]

    def corner_copies(way, j):
        source, at, to = spot_of(way, j)
        return [
            remote(field.at[:, source, lo], field.at[:, at, nxt], corner_s.at[way],
                   edge_r.at[first_sem[way] + j - 1], (to, down_l)),
            remote(field.at[:, source, hi], field.at[:, at, prv], corner_s.at[way],
                   edge_r.at[first_sem[way] + j - 1], (to, up_l)),
        ]

    def passed_on(j, total):
        return j <= total - DIRECT

    def pass_along(ref, send, recv):
        remote(ref(lo), ref(nxt), send, recv, (c, down_l)).start()
        remote(ref(hi), ref(prv), send, recv, (c, up_l)).start()

    def pass_plane(index, at):
        pass_along(lambda rows: field.at[:, at, rows], pass_s.at[0], edge_r.at[index])

    def send_plane(j, only=(True, True)):
        for way, total, across in sends:
            @pl.when(((j < total) | ((j == total) & jnp.logical_not(across))) & only[way])
            def _():
                plane_copy(way, j).start()

            @pl.when((j == total) & across & only[way])
            def _():
                for copy in part_copies(way, j):
                    copy.start()

    def send_corners(j):
        for way, total, across in sends:
            target_near = (up_near, down_near)[way]

            direct = jnp.where(target_near, jnp.logical_not(across & passed_on(j, total)), j == total)

            @pl.when((j <= total) & direct)
            def _():
                for copy in corner_copies(way, j):
                    copy.start()

    def start_counts(only):
        for way, total, _ in sends:
            @pl.when((total > 0) & only[way])
            def _():
                remote(count.at[way], counted.at[way, 0:lines], cnt_s.at[way], cnt_r.at[count_sem[way]],
                       ((up_c, down_c)[way], l)).start()

    def drain(ref, recv):
        remote(ref, ref, lab_s.at[0], recv, (c, l)).wait_recv()

    def flush(ref, send):
        remote(ref, ref, send, lab_r.at[0], (c, l)).wait_send()

    both = slice(0, 2 * REACH)
    incoming = ((near_way, near, 0), (far_way, far, 1))
    partner = c + 1 - 2 * lax.rem(c, 2)
    partner_end = plan.is_end(partner)
    cross_c = lax.rem(c + d + chain, chain)

    def start_chunk(i):
        for copy in own_copies(i):
            copy.start()

    def start_lanes():
        for copy in lab_copies:
            copy.start()
        start_chunk(0)

    def pass_counts():
        for way, total, index in incoming:
            @pl.when(total > 0)
            def _():
                drain(counted.at[way, 0:lines], cnt_r.at[index])
                pass_along(lambda rows: counted.at[way, rows], cnt_s.at[2 + index], cnt_r.at[2 + index])

    down_first = lower == is_end
    ahead = min(chunk, EARLY)
    for load, only in zip(loads, ((jnp.logical_not(down_first), down_first), (down_first, jnp.logical_not(down_first)))):
        load.wait()
        start_counts(only)
        for j in range(1, ahead + 1):
            send_plane(j, only)
    loads[2].wait()
    for j in range(ahead + 1, EARLY + 1):
        send_plane(j)

    @pl.when(is_end)
    def _():
        pl.semaphore_wait(tell.at[0], 1)
        signal(cross.at[0], (cross_c, l))
        start_lanes()
        pl.semaphore_wait(cross.at[0], 1)
        pass_counts()
        start_chunk(1)

    @pl.when(jnp.logical_not(is_end))
    def _():
        start_lanes()
        pl.semaphore_wait(lane_told.at[0], 2)

        @pl.when(partner_end)
        def _():
            signal(tell.at[0], (partner, l))

        signal(lane_told.at[1], (c, up_l))
        signal(lane_told.at[1], (c, down_l))
        pass_counts()
        start_chunk(1)

    def send_rest():
        for j in range(1, most + 1):
            send_corners(j)
            if j > EARLY:
                send_plane(j)

    @pl.when(jnp.logical_not(is_end))
    def _():
        for r in range(1, lanes // 2):
            pl.semaphore_wait(lane_told.at[r], 2)
            if r + 1 < lanes // 2:
                signal(lane_told.at[r + 1], (c, up_l))
                signal(lane_told.at[r + 1], (c, down_l))

    def tell_chain(r):
        signal(chain_told.at[r], (up_c, l))
        signal(chain_told.at[r], (down_c, l))

    def chain_rounds(point):
        each = plan.rounds // 4
        for r in range(point * each, (point + 1) * each):
            pl.semaphore_wait(chain_told.at[r], 2)
            if r + 1 < plan.rounds:
                tell_chain(r + 1)

    tell_chain(0)

    drain(label.at[:, both], lab_r.at[0])
    acc[...] = jnp.zeros(acc.shape, jnp.float32)
    for p in range(planes):
        mark[base + p] = jnp.where(label[p] == side, 1.0, 0.0)

    @pl.when(is_end)
    def _():
        mark[near_edge + d * (near + 1)] = jnp.zeros((tall, width), jnp.float32)

    def take(at):
        keep = mark[at] > 0.5

        def one(k, _):
            moved[k, at] = jnp.where(keep, field[k, at], 0.0)
            return 0

        lax.fori_loop(0, vectors, one, 0, unroll=vectors)

    def weights(before, here, after):
        scale = here * jnp.float32(1.0 / 6.0)
        return scale * (before + after + two_sided(here)), scale

    def apply_once(s):
        degree, scale = weights(mark[s - 1], mark[s], mark[s + 1])

        def one(k, _):
            here = moved[k, s]
            once[k, s] = degree * here - scale * (moved[k, s - 1] + moved[k, s + 1] + two_sided(here))
            return 0

        lax.fori_loop(0, vectors, one, 0, unroll=vectors)

    def apply_twice(s):
        degree, scale = weights(mark[s - 1], mark[s], mark[s + 1])

        def one(k, _):
            here = once[k, s]
            value = degree * here - scale * (once[k, s - 1] + once[k, s + 1] + two_sided(here))
            image[k, s - pad - REACH] = value[0:lines]
            return 0

        @pl.when(in_band(s))
        def _():
            lax.fori_loop(0, vectors, one, 0, unroll=vectors)

    def add_gram(reads, which):
        block = jnp.concatenate(
            [read(g).reshape(8 * vectors, width) for read in reads for g in range(lines // 8)], axis=1)
        high = block.astype(jnp.bfloat16)
        low = (block - high.astype(jnp.float32)).astype(jnp.bfloat16)
        dot = functools.partial(
            lax.dot_general, dimension_numbers=(((1,), (1,)), ((), ())), preferred_element_type=jnp.float32)
        acc[which, 0] += dot(high, high)
        acc[which, 1] += dot(high, low)

    def gram_of(spots):
        def reader(s, counts):
            def read(g):
                return jnp.where(counts & in_band(s), once[:, s, 8 * g : 8 * g + 8, :], 0.0)

            return read

        add_gram([reader(s, counts) for s, counts in spots], 0)

    def in_band(s):
        return (s >= pad + REACH) & (s < pad + window - REACH)

    def wait_plane(index, at):
        drain(field.at[:, at, 0:lines], plane_r.at[index])

    def wait_edges(index, at):
        drain(field.at[:, at, both], edge_r.at[index])

    def near_mark(j):
        at = near_edge + d * j
        wait_edges(j - 1, at)
        mark[at] = jnp.where(counted[near_way] >= (j + 0.0) - 0.5, 1.0, 0.0)

    def near_use(j, _):
        at = near_edge + d * j
        near_mark(j)
        take(at)
        apply_once(at - d)
        apply_twice(at - 2 * d)
        return 0

    def last_use(before_last):
        at = near_edge + d * near
        near_mark(near)
        for i in range(3):
            s = at - d * i
            degree, scale = weights(mark[s - 1], mark[s], mark[s + 1])
            weight[i, 0], weight[i, 1] = degree, scale

        def step(i, here, beside):
            return weight[i, 0] * here - weight[i, 1] * (beside + two_sided(here))

        def one(k, _):
            moved_0 = jnp.where(mark[at] > 0.5, field[k, at], 0.0)
            moved_1 = moved[k, at - d]
            once_0 = step(0, moved_0, moved_1)
            once_1 = step(1, moved_1, moved_0 + moved[k, at - 2 * d])
            once_2 = once[k, at - 2 * d]
            values = (
                step(0, once_0, once_1), step(1, once_1, once_0 + once_2),
                step(2, once_2, once_1 + once[k, at - 3 * d]))
            for i in range(3):
                image[k, at - d * i - pad - REACH] = values[i][0:lines]
            return 0

        share = vectors // PARTS
        for i in range(PARTS):
            if i == PARTS - 1:
                before_last()
            drain(field.at[i * share : (i + 1) * share, at, 0:lines], last_r.at[i])
            lax.fori_loop(i * share, (i + 1) * share, one, 0, unroll=share)

    def arrive(j):
        wait_plane(j - 1, near_edge + d * j)

        @pl.when(is_end & passed_on(j, near))
        def _():
            pass_plane(j - 1, near_edge + d * j)

    def near_use_now(j):
        lax.fori_loop(j, j + 1, near_use, 0)

    def near_step(j, _):
        wait_plane(j - 1, near_edge + d * j)
        near_use(j, 0)
        return 0

    def far_step(j, _):
        at = far_edge - d * j
        @pl.when(j == far)
        def _():
            wait_plane(most + j - 1, at)

        wait_edges(most + j - 1, at)
        mark[at] = jnp.where(counted[far_way] >= (far - j + 1).astype(jnp.float32) - 0.5, 1.0, 0.0)
        take(at)
        apply_once(at + d)

        apply_twice(at + 2 * d)
        return 0

    def other_step(j, _):
        at = near_edge - d * (j - 1)
        toward, away = 1.0 - mark[at + d], jnp.where(j < near, 1.0 - mark[at - d], 0.0)
        here = 1.0 - mark[at]
        degree, scale = weights(toward, here, away)

        def one(k, _):
            def part(keep, index):
                return jnp.where(keep > 0.5, field[k, index], 0.0)

            value = part(here, at)
            value = degree * value - scale * (part(toward, at + d) + part(away, at - d) + two_sided(value))
            spare[k, j - 1] = value[0:lines]
            return 0

        lax.fori_loop(0, vectors, one, 0, unroll=vectors)
        return 0

    def take_own(m, _):
        take(near_edge - d * m)
        return 0

    def inner_once(m, _):
        s = near_edge - d * m

        @pl.when((s > pad) & (s < pad + window - 1))
        def _():
            apply_once(s)
        return 0

    def inner_twice(m, _):
        apply_twice(near_edge - d * m)
        return 0

    def end_gram():
        @pl.when(is_end)
        def _():
            near_use_now(1)
            lax.fori_loop(1, near + 1, other_step, 0)
            add_gram([lambda g, p=p: spare[:, p, 8 * g : 8 * g + 8, :] for p in range(plan.end_near)], 1)

    ready = min(CHUNKS - 1, plan.end_near // chunk)
    for i in range(CHUNKS):
        drain(field.at[:, 0:chunk, both], own_r.at[i])
        chain_rounds(i)
        if i == 0:
            @pl.when(is_end)
            def _():
                arrive(1)

            for more in range(2, CHUNKS):
                start_chunk(more)
            send_rest()
        lax.fori_loop(i * chunk, (i + 1) * chunk, take_own, 0)
        inner = max(1, i * chunk - 1), (i + 1) * chunk - 1
        lax.fori_loop(*inner, inner_once, 0)
        gram_of([(near_edge - d * m, True) for m in range(*inner)])
        if i == ready:
            for way, total, index in incoming:
                @pl.when(total > 0)
                def _():
                    drain(counted.at[way, both], cnt_r.at[2 + index])
            end_gram()

            @pl.when(is_end)
            def _():
                arrive(2)

    @pl.when(jnp.logical_not(is_end))
    def _():
        def far_arrive(j, _):
            at = far_edge - d * j
            wait_plane(most + j - 1, at)
            pass_plane(most + j - 1, at)
            return 0

        lax.fori_loop(1, far, far_arrive, 0)
        lax.fori_loop(1, near + 1, near_step, 0)
        gram_of([(near_edge + d * (j - 1), j <= near) for j in range(1, most + 1)])

    lax.fori_loop(1, far + 1, far_step, 0)
    gram_of([(near_edge, is_end)] + [(far_edge - d * (j - 1), j <= far) for j in range(1, plan.most_far + 1)])

    lane_of = functools.partial(lax.broadcasted_iota, jnp.int32)
    ones = jnp.where(lax.div(lane_of((width, width), 0), 8) == lax.div(lane_of((width, width), 1), 8), 1.0, 0.0)
    pick = lane_of((8, width), 0) == lax.rem(lane_of((8, width), 1), 8)
    shape = (vectors, 8, width)
    diagonal = lane_of(shape, 1) == lax.rem(lane_of(shape, 2), 8)
    rows = []
    for which in range(2):
        total = acc[which, 0] + (acc[which, 1] + acc[which, 1].T)
        rows.append(jnp.sum(jnp.where(diagonal, total.reshape(shape), 0.0), axis=1))
    folded = jnp.dot(jnp.concatenate(rows, axis=0), ones, precision=lax.Precision.HIGHEST,
                     preferred_element_type=jnp.float32)
    parts = vectors // 8
    terms = [jnp.sum(jnp.where(pick, folded[8 * h : 8 * h + 8], 0.0), axis=0, keepdims=True) for h in range(2 * parts)]
    for h in range(parts):
        packed[h : h + 1, :] = jnp.where(side == 0, terms[h], terms[parts + h])
        packed[parts + h : parts + h + 1, :] = jnp.where(side == 0, terms[parts + h], terms[h])
    count_rows = 2 * parts
    body = packed.at[0:count_rows]
    chips = chain // 2 * lanes
    slot_of = lax.div(c, 2) * lanes + l
    leads = jnp.logical_not(is_end) & (partner_end | (lax.rem(c, 2) == 0))
    hand_over = remote(body, handed.at[0:count_rows], hand_s.at[0], hand_r.at[0], (partner, l))

    def broadcast(dc, dl):
        return remote(got.at[slot_of, 0:count_rows], got.at[slot_of, 0:count_rows], gram_s.at[0], gram_r.at[0],
                      (lax.rem(c + dc, chain), lax.rem(l + dl, lanes)))

    @pl.when(jnp.logical_not(leads))
    def _():
        hand_over.start()

    @pl.when(leads)
    def _():
        chain_rounds(3)
        hand_over.wait_recv()
        got[slot_of, 0:count_rows] = packed[0:count_rows] + handed[0:count_rows]
        for dc in range(chain):
            for dl in range(lanes):
                if dc or dl:
                    broadcast(dc, dl).start()

    @pl.when(is_end)
    def _():
        arrive(3)

    lax.fori_loop(2, planes - 2, inner_twice, 0)

    @pl.when(is_end)
    def _():
        for j in range(4, plan.end_near - DIRECT + 1):
            arrive(j)
        lax.fori_loop(2, near - DIRECT + 1, near_use, 0)
        lax.fori_loop(near - DIRECT + 1, near, near_step, 0)

    def many(total):
        return remote(got.at[0:total, 0:count_rows], got.at[0:total, 0:count_rows], gram_s.at[0], gram_r.at[0], (c, l))

    def finish_gram():
        @pl.when(leads)
        def _():
            many(chips - 1).wait_recv()

        @pl.when(jnp.logical_not(leads))
        def _():
            chain_rounds(3)
            many(chips).wait_recv()

        def sum_one(i, total):
            return total + got[i, 0:count_rows]

        total = lax.fori_loop(1, chips, sum_one, got[0, 0:count_rows], unroll=True)
        tall_shape = (vectors, width)
        inside = lax.div(lane_of(tall_shape, 1), 8) == lane_of(tall_shape, 0)
        choose = jnp.where(
            lax.rem(lane_of((width, width), 0), 8) == lax.rem(lane_of((width, width), 1), 8), 1.0, 0.0)
        for place in range(2):
            result = jnp.zeros(tall_shape, jnp.float32)
            for h in range(vectors // 8):
                i = place * (vectors // 8) + h
                spread = jnp.where(inside, jnp.broadcast_to(total[i : i + 1], tall_shape), 0.0)
                spread = jnp.dot(spread, choose, precision=lax.Precision.HIGHEST, preferred_element_type=jnp.float32)
                result = jnp.where(lax.div(lane_of(tall_shape, 1), 8) == h, spread, result)
            gram[place] = result[:, 0:vectors] / scale_of

    def flush_early():
        flush(field.at[:, 0:planes, both], own_s.at[0])
        flush(label.at[:, both], lab_s.at[0])
        for index, total in enumerate((near, far)):
            @pl.when(total > 0)
            def _():
                flush(counted.at[0, both], cnt_s.at[2 + index])

        for t in range(1, plan.most_far):
            @pl.when(far == t + 1)
            def _():
                flush(field.at[:, 0:t, both], pass_s.at[0])

        for way, total, across in sends:
            target_near = (up_near, down_near)[way]

            @pl.when(total > 0)
            def _():
                flush(counted.at[way, 0:lines], cnt_s.at[way])

            @pl.when((total > 0) & jnp.logical_not(target_near))
            def _():
                flush(field.at[:, 0:1, both], corner_s.at[way])

            for t in plan.totals:
                @pl.when((total == t) & jnp.logical_not(across))
                def _():
                    flush(field.at[:, 0:t, 0:lines], plane_s.at[way])

                @pl.when((total == t) & target_near & jnp.logical_not(across))
                def _():
                    flush(field.at[:, 0:t, both], corner_s.at[way])

    @pl.when(is_end)
    def _():
        flush(field.at[:, 0 : plan.end_near - DIRECT, both], pass_s.at[0])
        flush_early()
        last_use(finish_gram)

    @pl.when(jnp.logical_not(is_end))
    def _():
        finish_gram()

    @pl.when(leads)
    def _():
        sent = got.at[0 : chain * lanes - 1, 0:count_rows]
        remote(sent, sent, gram_s.at[0], gram_r.at[0], (c, l)).wait_send()

    @pl.when(jnp.logical_not(leads))
    def _():
        hand_over.wait_send()

    @pl.when(jnp.logical_not(is_end))
    def _():
        flush_early()

    for way, _, across in sends:
        @pl.when(across)
        def _():
            flush(field.at[:, 0:most, 0:lines], plane_s.at[way])
            flush(field.at[:, 0:DIRECT, both], corner_s.at[way])


def store_kernel(image, gram, image_out, gram_out, sems):
    part = image.shape[0] // STORES
    copies = [pltpu.make_async_copy(gram, gram_out, sems.at[STORES])]
    for i in range(STORES):
        rows = pl.ds(i * part, part)
        copies.append(pltpu.make_async_copy(image.at[rows], image_out.at[rows], sems.at[i]))
    for copy in copies:
        copy.start()
    for copy in copies:
        copy.wait()


def per_device(fiedler, side_labels):
    chain, lanes = lax.axis_size("chain"), lax.axis_size("lane")
    vectors, planes, lines, width = fiedler.shape
    plan = Plan(chain, lanes, vectors, planes, lines, width)
    slots = plan.band * plan.half * lines * lanes * width
    tall, frames, most = lines + 8, plan.frames, plan.most
    f32, dma, regular = jnp.float32, pltpu.SemaphoreType.DMA, pltpu.SemaphoreType.REGULAR
    anywhere, vmem = pl.BlockSpec(memory_space=pl.ANY), pl.BlockSpec(memory_space=pltpu.VMEM)
    image, gram = pl.pallas_call(
        functools.partial(kernel, plan, float(slots)),
        in_specs=[anywhere, anywhere],
        out_specs=[vmem, vmem],
        out_shape=[
            pltpu.VMEM((vectors, plan.band, lines, width), f32),
            pltpu.VMEM((2, vectors, vectors), f32),
        ],
        scratch_shapes=[
            pltpu.VMEM((vectors, frames, tall, width), f32),
            pltpu.VMEM((vectors, frames, tall, width), f32),
            pltpu.VMEM((vectors, frames, tall, width), f32),
            pltpu.VMEM((frames, tall, width), f32),
            pltpu.VMEM((planes, tall, width), jnp.int32),
            pltpu.VMEM((2, lines, width), f32),
            pltpu.VMEM((2, tall, width), f32),
            pltpu.VMEM((vectors, plan.end_near, lines, width), f32),
            pltpu.VMEM((2, 2, 8 * vectors, 8 * vectors), f32),
            pltpu.VMEM((3, 2, tall, width), f32),
            pltpu.VMEM((8, width), f32),
            pltpu.VMEM((8, width), f32),
            pltpu.VMEM((chain * lanes, 8, width), f32),
            dma((4,)), dma((1,)), dma((1,)), dma((1,)), dma((CHUNKS,)),
            dma((2,)), dma((most + plan.most_far,)), dma((PARTS,)), dma((2,)), dma((most + plan.most_far,)),
            dma((1,)), dma((4,)), dma((4,)), dma((1,)), dma((1,)), dma((1,)), dma((1,)),
            regular((lanes // 2,)), regular((1,)), regular((1,)), regular((plan.rounds,)),
        ],
        compiler_params=pltpu.CompilerParams(
            collective_id=0, has_side_effects=True, vmem_limit_bytes=56 * 1024 * 1024),
        name="laplace",
    )(fiedler, side_labels)
    return pl.pallas_call(
        store_kernel,
        in_specs=[vmem, vmem],
        out_specs=[anywhere, anywhere],
        out_shape=[jax.ShapeDtypeStruct(a.shape, a.dtype) for a in (image, gram)],
        scratch_shapes=[dma((STORES + 1,))],
        compiler_params=pltpu.CompilerParams(vmem_limit_bytes=1024 * 1024),
        name="store",
    )(*(pltpu.with_memory_space_constraint(a, pltpu.VMEM) for a in (image, gram)))


def solution(mesh):
    return jax.shard_map(
        per_device,
        mesh=mesh,
        in_specs=(P(None, "chain", "lane", None), P("chain", "lane", None)),
        out_specs=(P(None, "chain", "lane", None), P()),
        check_vma=False,
    )
```

```python
import functools

import jax
import jax.numpy as jnp
from jax import lax
from jax.experimental import pallas as pl
from jax.experimental.pallas import tpu as pltpu
from jax.sharding import PartitionSpec as P

REACH = 2
CHUNKS = 3
PARTS = 4
DIRECT = 3
EARLY = 4
STORES = 4
MESH = pl.DeviceIdType.MESH


def two_sided(field):
    return (
        pltpu.roll(field, 1, 0) + pltpu.roll(field, field.shape[0] - 1, 0)
        + pltpu.roll(field, 1, 1) + pltpu.roll(field, field.shape[1] - 1, 1)
    )


class Plan:
    def __init__(self, chain, lanes, vectors, planes, lines, width):
        self.chain, self.lanes, self.vectors, self.planes, self.lines, self.width = (
            chain, lanes, vectors, planes, lines, width)
        self.half = chain // 2
        self.band = planes + planes // 4
        self.grow = self.band - planes
        self.margin = self.grow * self.half // 2
        self.window = self.band + 2 * REACH
        spots = [self.spot(w, max_of=max) for w in range(self.half)]
        self.most = max(max(below, above) for _, below, above in spots)
        assert self.most <= planes and 8 * vectors == width and spots[0][1] == self.most
        assert spots[0][1] == spots[-1][2] > 3 + DIRECT - 1 and spots[0][2] == spots[-1][1] == 0
        self.end_near = spots[0][1]
        self.most_far = max(min(below, above) for _, below, above in spots)
        self.totals = sorted({count for _, below, above in spots for count in (below, above)} - {0})
        self.rounds = chain // 2
        assert self.rounds % 4 == 0 and lanes % 2 == 0 and lanes > 2
        self.chunk = planes // CHUNKS
        assert self.chunk * CHUNKS == planes and self.chunk > 2 and vectors % PARTS == 0
        self.pad = 1 + max(max(0, -slot) for slot, _, _ in spots)
        tail = 1 + max(max(0, slot + planes - self.window) for slot, _, _ in spots)
        self.frames = self.pad + self.window + tail

    def spot(self, w, max_of=jnp.maximum):
        first, last = (w == 0), (w == self.half - 1)
        if not isinstance(w, int):
            first, last = first.astype(jnp.int32), last.astype(jnp.int32)
        slot = self.margin + REACH - self.grow * w
        below = max_of(0, slot - REACH * first)
        above = max_of(0, self.window - REACH * last - slot - self.planes)
        return slot, below, above

    def is_end(self, c):
        within = self.place(c)[1]
        return (within == 0) | (within == self.half - 1)

    def place(self, c):
        relative = lax.rem(c + (self.chain - self.chain // 4), self.chain)
        side = lax.div(relative, self.half)
        within = relative - side * self.half
        return side, within


def kernel(plan, scale_of, fiedler, labels, image, gram, field, moved, once, mark, label, count, counted, spare, acc,
           weight, packed, handed, got, local_sem, lab_s, lab_r, own_s, own_r, plane_s, plane_r, last_r, corner_s, edge_r,
           pass_s, cnt_s, cnt_r, hand_s, hand_r, gram_s, gram_r, lane_told, tell, cross, chain_told):
    chain, lanes, vectors, planes, lines, width = (
        plan.chain, plan.lanes, plan.vectors, plan.planes, plan.lines, plan.width)
    window, pad, most = plan.window, plan.pad, plan.most
    c, l = lax.axis_index("chain"), lax.axis_index("lane")
    up_c, down_c = lax.rem(c + 1, chain), lax.rem(c + chain - 1, chain)
    up_l, down_l = lax.rem(l + 1, lanes), lax.rem(l + lanes - 1, lanes)
    side, within = plan.place(c)
    slot, below, above = plan.spot(within)
    up_side, up_within = plan.place(up_c)
    down_side, down_within = plan.place(down_c)
    up_slot, up_count, _ = plan.spot(up_within)
    down_slot, _, down_count = plan.spot(down_within)
    tall = lines + 8
    lo, hi = slice(0, REACH), slice(lines - REACH, lines)
    nxt, prv = slice(lines, lines + REACH), slice(tall - REACH, tall)

    def remote(src, dst, send, recv, device):
        return pltpu.make_async_remote_copy(
            src_ref=src, dst_ref=dst, send_sem=send, recv_sem=recv, device_id=device, device_id_type=MESH)

    base = pad + slot
    is_end = (within == 0) | (within == plan.half - 1)
    lower = within < plan.half // 2
    d = jnp.where(lower, -1, 1)
    near_way, far_way = jnp.where(lower, 0, 1), jnp.where(lower, 1, 0)
    near, far = jnp.where(lower, below, above), jnp.where(lower, above, below)
    near_edge = jnp.where(lower, base, base + planes - 1)
    far_edge = jnp.where(lower, base + planes - 1, base)

    chunk = plan.chunk
    near_start, far_start = jnp.where(lower, 0, planes - chunk), jnp.where(lower, planes - chunk, 0)
    rest = planes - 2 * chunk
    loads = []
    for i, (start, size) in enumerate((
            (jnp.where(is_end, near_start, far_start), chunk), (jnp.where(is_end, far_start, near_start), chunk),
            (chunk, rest))):
        loads.append(pltpu.make_async_copy(
            fiedler.at[:, pl.ds(start, size)], field.at[:, pl.ds(base + start, size), 0:lines], local_sem.at[i]))
    load_label = pltpu.make_async_copy(labels, label.at[:, 0:lines], local_sem.at[3])
    for load in (loads[0], load_label, loads[1], loads[2]):
        load.start()

    barrier = pltpu.get_barrier_semaphore()
    def signal(sem, device):
        pl.semaphore_signal(sem, inc=1, device_id=device, device_id_type=MESH)

    signal(barrier, (up_c, l))
    signal(barrier, (down_c, l))

    @pl.when(jnp.logical_not(is_end))
    def _():
        signal(barrier, (c, up_l))
        signal(barrier, (c, down_l))

    load_label.wait()
    totals = [jnp.zeros((lines, width), jnp.float32) for _ in range(2)]
    for p in range(planes):
        here = label[p, 0:lines]
        totals[0] += jnp.where((here == up_side) & (p >= planes - up_count), 1.0, 0.0)
        totals[1] += jnp.where((here == down_side) & (p < down_count), 1.0, 0.0)
    for way in range(2):
        count[way] = totals[way]

    @pl.when(is_end)
    def _():
        pl.semaphore_wait(barrier, 2)

    @pl.when(jnp.logical_not(is_end))
    def _():
        pl.semaphore_wait(barrier, 4)
        signal(lane_told.at[0], (c, up_l))
        signal(lane_told.at[0], (c, down_l))

    lab_copies = [
        remote(label.at[:, lo], label.at[:, nxt], lab_s.at[0], lab_r.at[0], (c, down_l)),
        remote(label.at[:, hi], label.at[:, prv], lab_s.at[0], lab_r.at[0], (c, up_l)),
    ]
    def own_copies(i):
        start = jnp.where(lower, i * chunk, planes - (i + 1) * chunk)
        at = pl.ds(base + start, chunk)
        return [
            remote(field.at[:, at, lo], field.at[:, at, nxt], own_s.at[0], own_r.at[i], (c, down_l)),
            remote(field.at[:, at, hi], field.at[:, at, prv], own_s.at[0], own_r.at[i], (c, up_l)),
        ]

    sends = ((0, up_count, up_side != side), (1, down_count, down_side != side))
    up_near, down_near = up_within < plan.half // 2, down_within >= plan.half // 2
    first_sem = (jnp.where(up_near, 0, most), jnp.where(down_near, 0, most))
    count_sem = (jnp.where(up_near, 0, 1), jnp.where(down_near, 0, 1))

    def spot_of(way, j):
        if way == 0:
            return base + planes - j, pad + up_slot - j, up_c
        return base + j - 1, pad + down_slot + planes - 1 + j, down_c

    def plane_copy(way, j):
        source, at, to = spot_of(way, j)
        return remote(
            field.at[:, source, 0:lines], field.at[:, at, 0:lines], plane_s.at[way],
            plane_r.at[first_sem[way] + j - 1], (to, l))

    def part_copies(way, j):
        source, at, to = spot_of(way, j)
        share = vectors // PARTS
        return [
            remote(field.at[i * share : (i + 1) * share, source, 0:lines],
                   field.at[i * share : (i + 1) * share, at, 0:lines], plane_s.at[way], last_r.at[i], (to, l))
            for i in range(PARTS)
        ]

    def corner_copies(way, j):
        source, at, to = spot_of(way, j)
        return [
            remote(field.at[:, source, lo], field.at[:, at, nxt], corner_s.at[way],
                   edge_r.at[first_sem[way] + j - 1], (to, down_l)),
            remote(field.at[:, source, hi], field.at[:, at, prv], corner_s.at[way],
                   edge_r.at[first_sem[way] + j - 1], (to, up_l)),
        ]

    def passed_on(j, total):
        return j <= total - DIRECT

    def pass_along(ref, send, recv):
        remote(ref(lo), ref(nxt), send, recv, (c, down_l)).start()
        remote(ref(hi), ref(prv), send, recv, (c, up_l)).start()

    def pass_plane(index, at):
        pass_along(lambda rows: field.at[:, at, rows], pass_s.at[0], edge_r.at[index])

    def send_plane(j, only=(True, True)):
        for way, total, across in sends:
            @pl.when(((j < total) | ((j == total) & jnp.logical_not(across))) & only[way])
            def _():
                plane_copy(way, j).start()

            @pl.when((j == total) & across & only[way])
            def _():
                for copy in part_copies(way, j):
                    copy.start()

    def send_corners(j):
        for way, total, across in sends:
            target_near = (up_near, down_near)[way]

            direct = jnp.where(target_near, jnp.logical_not(across & passed_on(j, total)), j == total)

            @pl.when((j <= total) & direct)
            def _():
                for copy in corner_copies(way, j):
                    copy.start()

    def start_counts(only):
        for way, total, _ in sends:
            @pl.when((total > 0) & only[way])
            def _():
                remote(count.at[way], counted.at[way, 0:lines], cnt_s.at[way], cnt_r.at[count_sem[way]],
                       ((up_c, down_c)[way], l)).start()

    def drain(ref, recv):
        remote(ref, ref, lab_s.at[0], recv, (c, l)).wait_recv()

    def flush(ref, send):
        remote(ref, ref, send, lab_r.at[0], (c, l)).wait_send()

    both = slice(0, 2 * REACH)
    incoming = ((near_way, near, 0), (far_way, far, 1))
    partner = c + 1 - 2 * lax.rem(c, 2)
    partner_end = plan.is_end(partner)
    cross_c = lax.rem(c + d + chain, chain)

    def start_chunk(i):
        for copy in own_copies(i):
            copy.start()

    def start_lanes():
        for copy in lab_copies:
            copy.start()
        start_chunk(0)

    def pass_counts():
        for way, total, index in incoming:
            @pl.when(total > 0)
            def _():
                drain(counted.at[way, 0:lines], cnt_r.at[index])
                pass_along(lambda rows: counted.at[way, rows], cnt_s.at[2 + index], cnt_r.at[2 + index])

    down_first = lower == is_end
    ahead = min(chunk, EARLY)
    for load, only in zip(loads, ((jnp.logical_not(down_first), down_first), (down_first, jnp.logical_not(down_first)))):
        load.wait()
        start_counts(only)
        for j in range(1, ahead + 1):
            send_plane(j, only)
    loads[2].wait()
    for j in range(ahead + 1, EARLY + 1):
        send_plane(j)

    @pl.when(is_end)
    def _():
        pl.semaphore_wait(tell.at[0], 1)
        signal(cross.at[0], (cross_c, l))
        start_lanes()
        pl.semaphore_wait(cross.at[0], 1)
        pass_counts()
        start_chunk(1)

    @pl.when(jnp.logical_not(is_end))
    def _():
        start_lanes()
        pl.semaphore_wait(lane_told.at[0], 2)

        @pl.when(partner_end)
        def _():
            signal(tell.at[0], (partner, l))

        signal(lane_told.at[1], (c, up_l))
        signal(lane_told.at[1], (c, down_l))
        pass_counts()
        start_chunk(1)

    def send_rest():
        for j in range(1, most + 1):
            send_corners(j)
            if j > EARLY:
                send_plane(j)

    @pl.when(jnp.logical_not(is_end))
    def _():
        for r in range(1, lanes // 2):
            pl.semaphore_wait(lane_told.at[r], 2)
            if r + 1 < lanes // 2:
                signal(lane_told.at[r + 1], (c, up_l))
                signal(lane_told.at[r + 1], (c, down_l))

    def tell_chain(r):
        signal(chain_told.at[r], (up_c, l))
        signal(chain_told.at[r], (down_c, l))

    def chain_rounds(point):
        each = plan.rounds // 4
        for r in range(point * each, (point + 1) * each):
            pl.semaphore_wait(chain_told.at[r], 2)
            if r + 1 < plan.rounds:
                tell_chain(r + 1)

    tell_chain(0)

    drain(label.at[:, both], lab_r.at[0])
    acc[...] = jnp.zeros(acc.shape, jnp.float32)
    for p in range(planes):
        mark[base + p] = jnp.where(label[p] == side, 1.0, 0.0)

    @pl.when(is_end)
    def _():
        mark[near_edge + d * (near + 1)] = jnp.zeros((tall, width), jnp.float32)

    def take(at):
        keep = mark[at] > 0.5

        def one(k, _):
            moved[k, at] = jnp.where(keep, field[k, at], 0.0)
            return 0

        lax.fori_loop(0, vectors, one, 0, unroll=vectors)

    def weights(before, here, after):
        scale = here * jnp.float32(1.0 / 6.0)
        return scale * (before + after + two_sided(here)), scale

    def apply_once(s):
        degree, scale = weights(mark[s - 1], mark[s], mark[s + 1])

        def one(k, _):
            here = moved[k, s]
            once[k, s] = degree * here - scale * (moved[k, s - 1] + moved[k, s + 1] + two_sided(here))
            return 0

        lax.fori_loop(0, vectors, one, 0, unroll=vectors)

    def apply_twice(s):
        degree, scale = weights(mark[s - 1], mark[s], mark[s + 1])

        def one(k, _):
            here = once[k, s]
            value = degree * here - scale * (once[k, s - 1] + once[k, s + 1] + two_sided(here))
            image[k, s - pad - REACH] = value[0:lines]
            return 0

        @pl.when(in_band(s))
        def _():
            lax.fori_loop(0, vectors, one, 0, unroll=vectors)

    def add_gram(reads, which):
        block = jnp.concatenate(
            [read(g).reshape(8 * vectors, width) for read in reads for g in range(lines // 8)], axis=1)
        high = block.astype(jnp.bfloat16)
        low = (block - high.astype(jnp.float32)).astype(jnp.bfloat16)
        dot = functools.partial(
            lax.dot_general, dimension_numbers=(((1,), (1,)), ((), ())), preferred_element_type=jnp.float32)
        acc[which, 0] += dot(high, high)
        acc[which, 1] += dot(high, low)

    def gram_of(spots):
        def reader(s, counts):
            def read(g):
                return jnp.where(counts & in_band(s), once[:, s, 8 * g : 8 * g + 8, :], 0.0)

            return read

        add_gram([reader(s, counts) for s, counts in spots], 0)

    def in_band(s):
        return (s >= pad + REACH) & (s < pad + window - REACH)

    def wait_plane(index, at):
        drain(field.at[:, at, 0:lines], plane_r.at[index])

    def wait_edges(index, at):
        drain(field.at[:, at, both], edge_r.at[index])

    def near_mark(j):
        at = near_edge + d * j
        wait_edges(j - 1, at)
        mark[at] = jnp.where(counted[near_way] >= (j + 0.0) - 0.5, 1.0, 0.0)

    def near_use(j, _):
        at = near_edge + d * j
        near_mark(j)
        take(at)
        apply_once(at - d)
        apply_twice(at - 2 * d)
        return 0

    def last_use(before_last):
        at = near_edge + d * near
        near_mark(near)
        for i in range(3):
            s = at - d * i
            degree, scale = weights(mark[s - 1], mark[s], mark[s + 1])
            weight[i, 0], weight[i, 1] = degree, scale

        def step(i, here, beside):
            return weight[i, 0] * here - weight[i, 1] * (beside + two_sided(here))

        def one(k, _):
            moved_0 = jnp.where(mark[at] > 0.5, field[k, at], 0.0)
            moved_1 = moved[k, at - d]
            once_0 = step(0, moved_0, moved_1)
            once_1 = step(1, moved_1, moved_0 + moved[k, at - 2 * d])
            once_2 = once[k, at - 2 * d]
            values = (
                step(0, once_0, once_1), step(1, once_1, once_0 + once_2),
                step(2, once_2, once_1 + once[k, at - 3 * d]))
            for i in range(3):
                image[k, at - d * i - pad - REACH] = values[i][0:lines]
            return 0

        share = vectors // PARTS
        for i in range(PARTS):
            if i == PARTS - 1:
                before_last()
            drain(field.at[i * share : (i + 1) * share, at, 0:lines], last_r.at[i])
            lax.fori_loop(i * share, (i + 1) * share, one, 0, unroll=share)

    def arrive(j):
        wait_plane(j - 1, near_edge + d * j)

        @pl.when(is_end & passed_on(j, near))
        def _():
            pass_plane(j - 1, near_edge + d * j)

    def near_use_now(j):
        lax.fori_loop(j, j + 1, near_use, 0)

    def near_step(j, _):
        wait_plane(j - 1, near_edge + d * j)
        near_use(j, 0)
        return 0

    def far_step(j, _):
        at = far_edge - d * j
        @pl.when(j == far)
        def _():
            wait_plane(most + j - 1, at)

        wait_edges(most + j - 1, at)
        mark[at] = jnp.where(counted[far_way] >= (far - j + 1).astype(jnp.float32) - 0.5, 1.0, 0.0)
        take(at)
        apply_once(at + d)

        apply_twice(at + 2 * d)
        return 0

    def other_step(j, _):
        at = near_edge - d * (j - 1)
        toward, away = 1.0 - mark[at + d], jnp.where(j < near, 1.0 - mark[at - d], 0.0)
        here = 1.0 - mark[at]
        degree, scale = weights(toward, here, away)

        def one(k, _):
            def part(keep, index):
                return jnp.where(keep > 0.5, field[k, index], 0.0)

            value = part(here, at)
            value = degree * value - scale * (part(toward, at + d) + part(away, at - d) + two_sided(value))
            spare[k, j - 1] = value[0:lines]
            return 0

        lax.fori_loop(0, vectors, one, 0, unroll=vectors)
        return 0

    def take_own(m, _):
        take(near_edge - d * m)
        return 0

    def inner_once(m, _):
        s = near_edge - d * m

        @pl.when((s > pad) & (s < pad + window - 1))
        def _():
            apply_once(s)
        return 0

    def inner_twice(m, _):
        apply_twice(near_edge - d * m)
        return 0

    def end_gram():
        @pl.when(is_end)
        def _():
            near_use_now(1)
            lax.fori_loop(1, near + 1, other_step, 0)
            add_gram([lambda g, p=p: spare[:, p, 8 * g : 8 * g + 8, :] for p in range(plan.end_near)], 1)

    ready = min(CHUNKS - 1, plan.end_near // chunk)
    for i in range(CHUNKS):
        drain(field.at[:, 0:chunk, both], own_r.at[i])
        chain_rounds(i)
        if i == 0:
            @pl.when(is_end)
            def _():
                arrive(1)

            for more in range(2, CHUNKS):
                start_chunk(more)
            send_rest()
        lax.fori_loop(i * chunk, (i + 1) * chunk, take_own, 0)
        inner = max(1, i * chunk - 1), (i + 1) * chunk - 1
        lax.fori_loop(*inner, inner_once, 0)
        gram_of([(near_edge - d * m, True) for m in range(*inner)])
        if i == ready:
            for way, total, index in incoming:
                @pl.when(total > 0)
                def _():
                    drain(counted.at[way, both], cnt_r.at[2 + index])
            end_gram()

            @pl.when(is_end)
            def _():
                arrive(2)

    @pl.when(jnp.logical_not(is_end))
    def _():
        def far_arrive(j, _):
            at = far_edge - d * j
            wait_plane(most + j - 1, at)
            pass_plane(most + j - 1, at)
            return 0

        lax.fori_loop(1, far, far_arrive, 0)
        lax.fori_loop(1, near + 1, near_step, 0)
        gram_of([(near_edge + d * (j - 1), j <= near) for j in range(1, most + 1)])

    lax.fori_loop(1, far + 1, far_step, 0)
    gram_of([(near_edge, is_end)] + [(far_edge - d * (j - 1), j <= far) for j in range(1, plan.most_far + 1)])

    lane_of = functools.partial(lax.broadcasted_iota, jnp.int32)
    ones = jnp.where(lax.div(lane_of((width, width), 0), 8) == lax.div(lane_of((width, width), 1), 8), 1.0, 0.0)
    pick = lane_of((8, width), 0) == lax.rem(lane_of((8, width), 1), 8)
    shape = (vectors, 8, width)
    diagonal = lane_of(shape, 1) == lax.rem(lane_of(shape, 2), 8)
    rows = []
    for which in range(2):
        total = acc[which, 0] + (acc[which, 1] + acc[which, 1].T)
        rows.append(jnp.sum(jnp.where(diagonal, total.reshape(shape), 0.0), axis=1))
    folded = jnp.dot(jnp.concatenate(rows, axis=0), ones, precision=lax.Precision.HIGHEST,
                     preferred_element_type=jnp.float32)
    parts = vectors // 8
    terms = [jnp.sum(jnp.where(pick, folded[8 * h : 8 * h + 8], 0.0), axis=0, keepdims=True) for h in range(2 * parts)]
    for h in range(parts):
        packed[h : h + 1, :] = jnp.where(side == 0, terms[h], terms[parts + h])
        packed[parts + h : parts + h + 1, :] = jnp.where(side == 0, terms[parts + h], terms[h])
    count_rows = 2 * parts
    body = packed.at[0:count_rows]
    chips = chain // 2 * lanes
    slot_of = lax.div(c, 2) * lanes + l
    leads = jnp.logical_not(is_end) & (partner_end | (lax.rem(c, 2) == 0))
    hand_over = remote(body, handed.at[0:count_rows], hand_s.at[0], hand_r.at[0], (partner, l))

    def broadcast(dc, dl):
        return remote(got.at[slot_of, 0:count_rows], got.at[slot_of, 0:count_rows], gram_s.at[0], gram_r.at[0],
                      (lax.rem(c + dc, chain), lax.rem(l + dl, lanes)))

    @pl.when(jnp.logical_not(leads))
    def _():
        hand_over.start()

    @pl.when(leads)
    def _():
        chain_rounds(3)
        hand_over.wait_recv()
        got[slot_of, 0:count_rows] = packed[0:count_rows] + handed[0:count_rows]
        for dc in range(chain):
            for dl in range(lanes):
                if dc or dl:
                    broadcast(dc, dl).start()

    @pl.when(is_end)
    def _():
        arrive(3)

    lax.fori_loop(2, planes - 2, inner_twice, 0)

    @pl.when(is_end)
    def _():
        for j in range(4, plan.end_near - DIRECT + 1):
            arrive(j)
        lax.fori_loop(2, near - DIRECT + 1, near_use, 0)
        lax.fori_loop(near - DIRECT + 1, near, near_step, 0)

    def many(total):
        return remote(got.at[0:total, 0:count_rows], got.at[0:total, 0:count_rows], gram_s.at[0], gram_r.at[0], (c, l))

    def finish_gram():
        @pl.when(leads)
        def _():
            many(chips - 1).wait_recv()

        @pl.when(jnp.logical_not(leads))
        def _():
            chain_rounds(3)
            many(chips).wait_recv()

        def sum_one(i, total):
            return total + got[i, 0:count_rows]

        total = lax.fori_loop(1, chips, sum_one, got[0, 0:count_rows], unroll=True)
        tall_shape = (vectors, width)
        inside = lax.div(lane_of(tall_shape, 1), 8) == lane_of(tall_shape, 0)
        choose = jnp.where(
            lax.rem(lane_of((width, width), 0), 8) == lax.rem(lane_of((width, width), 1), 8), 1.0, 0.0)
        for place in range(2):
            result = jnp.zeros(tall_shape, jnp.float32)
            for h in range(vectors // 8):
                i = place * (vectors // 8) + h
                spread = jnp.where(inside, jnp.broadcast_to(total[i : i + 1], tall_shape), 0.0)
                spread = jnp.dot(spread, choose, precision=lax.Precision.HIGHEST, preferred_element_type=jnp.float32)
                result = jnp.where(lax.div(lane_of(tall_shape, 1), 8) == h, spread, result)
            gram[place] = result[:, 0:vectors] / scale_of

    def flush_early():
        flush(field.at[:, 0:planes, both], own_s.at[0])
        flush(label.at[:, both], lab_s.at[0])
        for index, total in enumerate((near, far)):
            @pl.when(total > 0)
            def _():
                flush(counted.at[0, both], cnt_s.at[2 + index])

        for t in range(1, plan.most_far):
            @pl.when(far == t + 1)
            def _():
                flush(field.at[:, 0:t, both], pass_s.at[0])

        for way, total, across in sends:
            target_near = (up_near, down_near)[way]

            @pl.when(total > 0)
            def _():
                flush(counted.at[way, 0:lines], cnt_s.at[way])

            @pl.when((total > 0) & jnp.logical_not(target_near))
            def _():
                flush(field.at[:, 0:1, both], corner_s.at[way])

            for t in plan.totals:
                @pl.when((total == t) & jnp.logical_not(across))
                def _():
                    flush(field.at[:, 0:t, 0:lines], plane_s.at[way])

                @pl.when((total == t) & target_near & jnp.logical_not(across))
                def _():
                    flush(field.at[:, 0:t, both], corner_s.at[way])

    @pl.when(is_end)
    def _():
        flush(field.at[:, 0 : plan.end_near - DIRECT, both], pass_s.at[0])
        flush_early()
        last_use(finish_gram)

    @pl.when(jnp.logical_not(is_end))
    def _():
        finish_gram()

    @pl.when(leads)
    def _():
        sent = got.at[0 : chain * lanes - 1, 0:count_rows]
        remote(sent, sent, gram_s.at[0], gram_r.at[0], (c, l)).wait_send()

    @pl.when(jnp.logical_not(leads))
    def _():
        hand_over.wait_send()

    @pl.when(jnp.logical_not(is_end))
    def _():
        flush_early()

    for way, _, across in sends:
        @pl.when(across)
        def _():
            flush(field.at[:, 0:most, 0:lines], plane_s.at[way])
            flush(field.at[:, 0:DIRECT, both], corner_s.at[way])


def store_kernel(image, gram, image_out, gram_out, sems):
    part = image.shape[0] // STORES
    copies = [pltpu.make_async_copy(gram, gram_out, sems.at[STORES])]
    for i in range(STORES):
        rows = pl.ds(i * part, part)
        copies.append(pltpu.make_async_copy(image.at[rows], image_out.at[rows], sems.at[i]))
    for copy in copies:
        copy.start()
    for copy in copies:
        copy.wait()


def per_device(fiedler, side_labels):
    chain, lanes = lax.axis_size("chain"), lax.axis_size("lane")
    vectors, planes, lines, width = fiedler.shape
    plan = Plan(chain, lanes, vectors, planes, lines, width)
    slots = plan.band * plan.half * lines * lanes * width
    tall, frames, most = lines + 8, plan.frames, plan.most
    f32, dma, regular = jnp.float32, pltpu.SemaphoreType.DMA, pltpu.SemaphoreType.REGULAR
    anywhere, vmem = pl.BlockSpec(memory_space=pl.ANY), pl.BlockSpec(memory_space=pltpu.VMEM)
    image, gram = pl.pallas_call(
        functools.partial(kernel, plan, float(slots)),
        in_specs=[anywhere, anywhere],
        out_specs=[vmem, vmem],
        out_shape=[
            pltpu.VMEM((vectors, plan.band, lines, width), f32),
            pltpu.VMEM((2, vectors, vectors), f32),
        ],
        scratch_shapes=[
            pltpu.VMEM((vectors, frames, tall, width), f32),
            pltpu.VMEM((vectors, frames, tall, width), f32),
            pltpu.VMEM((vectors, frames, tall, width), f32),
            pltpu.VMEM((frames, tall, width), f32),
            pltpu.VMEM((planes, tall, width), jnp.int32),
            pltpu.VMEM((2, lines, width), f32),
            pltpu.VMEM((2, tall, width), f32),
            pltpu.VMEM((vectors, plan.end_near, lines, width), f32),
            pltpu.VMEM((2, 2, 8 * vectors, 8 * vectors), f32),
            pltpu.VMEM((3, 2, tall, width), f32),
            pltpu.VMEM((8, width), f32),
            pltpu.VMEM((8, width), f32),
            pltpu.VMEM((chain * lanes, 8, width), f32),
            dma((4,)), dma((1,)), dma((1,)), dma((1,)), dma((CHUNKS,)),
            dma((2,)), dma((most + plan.most_far,)), dma((PARTS,)), dma((2,)), dma((most + plan.most_far,)),
            dma((1,)), dma((4,)), dma((4,)), dma((1,)), dma((1,)), dma((1,)), dma((1,)),
            regular((lanes // 2,)), regular((1,)), regular((1,)), regular((plan.rounds,)),
        ],
        compiler_params=pltpu.CompilerParams(
            collective_id=0, has_side_effects=True, vmem_limit_bytes=56 * 1024 * 1024),
        name="laplace",
    )(fiedler, side_labels)
    return pl.pallas_call(
        store_kernel,
        in_specs=[vmem, vmem],
        out_specs=[anywhere, anywhere],
        out_shape=[jax.ShapeDtypeStruct(a.shape, a.dtype) for a in (image, gram)],
        scratch_shapes=[dma((STORES + 1,))],
        compiler_params=pltpu.CompilerParams(vmem_limit_bytes=1024 * 1024),
        name="store",
    )(*(pltpu.with_memory_space_constraint(a, pltpu.VMEM) for a in (image, gram)))


def solution(mesh):
    return jax.shard_map(
        per_device,
        mesh=mesh,
        in_specs=(P(None, "chain", "lane", None), P("chain", "lane", None)),
        out_specs=(P(None, "chain", "lane", None), P()),
        check_vma=False,
    )
```
